16 devices in a mesh: cp: 2 (over z), fsdp: 8 (over y, x, core).
Axes of the slice: x: 2, y: 2, z: 2, core: 2. Of those that a mesh axis runs over, the one named last changes fastest.
Arguments:
- hidden: bfloat16 [48, 512, 1536], P('fsdp', 'cp')
- tok_pos: int32 [48, 512], P('fsdp', 'cp')
- grad_out: bfloat16 [48, 512, 1536], P('fsdp', 'cp')
- norm_gain: float32 [1536], P(('fsdp', 'cp'))
- w_query: bfloat16 [1536, 1536], P(('fsdp', 'cp'))
- w_key: bfloat16 [1536, 256], P(('fsdp', 'cp'))
- w_value: bfloat16 [1536, 256], P(('fsdp', 'cp'))
- w_out: bfloat16 [1536, 1536], P(('fsdp', 'cp'))
Outputs:
- output 1: bfloat16 [48, 512, 1536], P('fsdp', 'cp')
- output 2: bfloat16 [48, 512, 1536], P('fsdp', 'cp')
- output 3: float32 [1536, 1536], P(('fsdp', 'cp'))
- output 4: float32 [1536, 256], P(('fsdp', 'cp'))
- output 5: float32 [1536, 256], P(('fsdp', 'cp'))
- output 6: float32 [1536, 1536], P(('fsdp', 'cp'))
- output 7: float32 [1536], P(('fsdp', 'cp'))
All inputs are finite; a program needn't handle non-finite values.
Results may differ from the reference program's by a relative error of at most 0.00682371.
Values are sent between devices in bfloat16 or wider.
A program may use at most 1 GiB of HBM per device.

```python
import jax
import jax.numpy as jnp
from jax import lax

SEQS_TOTAL = 48
SEQ_LEN = 512
MODEL_DIM = 1536
NUM_HEADS = 12
NUM_KV_HEADS = 2
HEAD_DIM = 128
Q_BLOCK = 32
ROPE_THETA = 1000000.0
RMS_EPS = 1e-5
NEG_BIG = -1e30
SCALE = HEAD_DIM ** -0.5
GROUP_SIZE = NUM_HEADS // NUM_KV_HEADS
N_QBLOCKS = SEQ_LEN // Q_BLOCK


def setup_inputs(seed: int = 0) -> dict:
    rand_keys = jax.random.split(jax.random.key(seed), 8)
    q_cols = NUM_HEADS * HEAD_DIM
    kv_cols = NUM_KV_HEADS * HEAD_DIM
    in_scale = MODEL_DIM ** -0.5
    hidden = jax.random.normal(rand_keys[0], (SEQS_TOTAL, SEQ_LEN, MODEL_DIM), jnp.float32)
    base_pos = jnp.broadcast_to(jnp.arange(SEQ_LEN, dtype=jnp.int32), (SEQS_TOTAL, SEQ_LEN))
    tok_pos = jax.random.permutation(rand_keys[1], base_pos, axis=1, independent=True)
    grad_out = jax.random.normal(rand_keys[2], (SEQS_TOTAL, SEQ_LEN, MODEL_DIM), jnp.float32)
    norm_gain = jax.random.uniform(rand_keys[3], (MODEL_DIM,), jnp.float32, 0.5, 1.5)
    w_query = jax.random.normal(rand_keys[4], (MODEL_DIM, q_cols), jnp.float32) * in_scale
    w_key = jax.random.normal(rand_keys[5], (MODEL_DIM, kv_cols), jnp.float32) * in_scale
    w_value = jax.random.normal(rand_keys[6], (MODEL_DIM, kv_cols), jnp.float32) * in_scale
    w_out = jax.random.normal(rand_keys[7], (q_cols, MODEL_DIM), jnp.float32) * q_cols ** -0.5
    return {'hidden': hidden.astype(jnp.bfloat16), 'tok_pos': tok_pos, 'grad_out': grad_out.astype(jnp.bfloat16), 'norm_gain': norm_gain, 'w_query': w_query.astype(jnp.bfloat16), 'w_key': w_key.astype(jnp.bfloat16), 'w_value': w_value.astype(jnp.bfloat16), 'w_out': w_out.astype(jnp.bfloat16)}


def rope_tables(positions):
    half_dim = HEAD_DIM // 2
    inv_freq = ROPE_THETA ** (-jnp.arange(half_dim, dtype=jnp.float32) / half_dim)
    angles = positions.astype(jnp.float32)[..., None] * inv_freq
    return jnp.cos(angles)[..., None, :], jnp.sin(angles)[..., None, :]


def rope_apply(values, cos_tab, sin_tab):
    half_dim = HEAD_DIM // 2
    first_half = values[..., :half_dim]
    second_half = values[..., half_dim:]
    return jnp.concatenate([first_half * cos_tab - second_half * sin_tab, second_half * cos_tab + first_half * sin_tab], axis=-1)


def rope_transpose(values, cos_tab, sin_tab):
    half_dim = HEAD_DIM // 2
    first_half = values[..., :half_dim]
    second_half = values[..., half_dim:]
    return jnp.concatenate([first_half * cos_tab + second_half * sin_tab, second_half * cos_tab - first_half * sin_tab], axis=-1)


def seq_pass(hidden, tok_pos, grad_out, norm_gain, w_query, w_key, w_value, w_out):
    x_f32 = hidden.astype(jnp.float32)
    inv_rms = lax.rsqrt(jnp.mean(x_f32 * x_f32, axis=-1) + RMS_EPS)
    x_hat = x_f32 * inv_rms[:, None]
    normed = (x_hat * norm_gain).astype(jnp.bfloat16)
    cos_tab, sin_tab = rope_tables(tok_pos)
    q_lin = jnp.dot(normed, w_query, preferred_element_type=jnp.float32).reshape(SEQ_LEN, NUM_HEADS, HEAD_DIM)
    k_lin = jnp.dot(normed, w_key, preferred_element_type=jnp.float32).reshape(SEQ_LEN, NUM_KV_HEADS, HEAD_DIM)
    q_rot = rope_apply(q_lin, cos_tab, sin_tab).astype(jnp.bfloat16)
    k_rot = rope_apply(k_lin, cos_tab, sin_tab).astype(jnp.bfloat16)
    v_val = jnp.dot(normed, w_value, preferred_element_type=jnp.float32).astype(jnp.bfloat16).reshape(SEQ_LEN, NUM_KV_HEADS, HEAD_DIM)
    k_f32 = k_rot.astype(jnp.float32)
    v_f32 = v_val.astype(jnp.float32)
    q_blocks = q_rot.reshape(N_QBLOCKS, Q_BLOCK, NUM_KV_HEADS, GROUP_SIZE, HEAD_DIM)
    pos_blocks = tok_pos.reshape(N_QBLOCKS, Q_BLOCK)

    def block_scores(q_blk, q_pos):
        scores = jnp.einsum('ikgd,jkd->kigj', q_blk.astype(jnp.float32), k_f32) * SCALE
        visible = tok_pos[None, None, None, :] <= q_pos[None, :, None, None]
        return jnp.where(visible, scores, NEG_BIG), visible

    def fwd_block(blk_args):
        q_blk, q_pos = blk_args
        scores, visible = block_scores(q_blk, q_pos)
        row_max = jnp.max(scores, axis=-1)
        att_probs = jnp.where(visible, jnp.exp(scores - row_max[..., None]), 0.0)
        row_sum = jnp.sum(att_probs, axis=-1)
        out_blk = jnp.einsum('kigj,jkd->ikgd', att_probs.astype(jnp.bfloat16).astype(jnp.float32), v_f32)
        out_blk = out_blk / jnp.transpose(row_sum, (1, 0, 2))[..., None]
        return out_blk.astype(jnp.bfloat16), row_max + jnp.log(row_sum)

    attn_out, log_sum = lax.map(fwd_block, (q_blocks, pos_blocks))
    attn_flat = attn_out.reshape(SEQ_LEN, NUM_HEADS * HEAD_DIM)
    result = (x_f32 + jnp.dot(attn_flat, w_out, preferred_element_type=jnp.float32)).astype(jnp.bfloat16)
    grad_w_out = jnp.dot(attn_flat.T, grad_out, preferred_element_type=jnp.float32)
    grad_attn = jnp.dot(grad_out, w_out.T, preferred_element_type=jnp.float32).astype(jnp.bfloat16)
    gout_blocks = grad_attn.reshape(N_QBLOCKS, Q_BLOCK, NUM_KV_HEADS, GROUP_SIZE, HEAD_DIM)
    row_delta = jnp.einsum('nikgd,nikgd->nkig', gout_blocks.astype(jnp.float32), attn_out.astype(jnp.float32))

    def bwd_block(kv_grads, blk_args):
        grad_k, grad_v = kv_grads
        q_blk, q_pos, gout_blk, lse_blk, delta_blk = blk_args
        scores, visible = block_scores(q_blk, q_pos)
        att_probs = jnp.where(visible, jnp.exp(scores - lse_blk[..., None]), 0.0)
        gout_f32 = gout_blk.astype(jnp.float32)
        grad_v = grad_v + jnp.einsum('kigj,ikgd->jkd', att_probs.astype(jnp.bfloat16).astype(jnp.float32), gout_f32)
        grad_probs = jnp.einsum('ikgd,jkd->kigj', gout_f32, v_f32)
        grad_scores = (att_probs * (grad_probs - delta_blk[..., None])).astype(jnp.bfloat16).astype(jnp.float32)
        grad_q = jnp.einsum('kigj,jkd->ikgd', grad_scores, k_f32)
        grad_k = grad_k + jnp.einsum('kigj,ikgd->jkd', grad_scores, q_blk.astype(jnp.float32))
        return (grad_k, grad_v), grad_q

    zero_kv = jnp.zeros((SEQ_LEN, NUM_KV_HEADS, HEAD_DIM), jnp.float32)
    kv_grads, grad_q = lax.scan(bwd_block, (zero_kv, zero_kv), (q_blocks, pos_blocks, gout_blocks, log_sum, row_delta))
    dq_pre = rope_transpose(grad_q.reshape(SEQ_LEN, NUM_HEADS, HEAD_DIM) * SCALE, cos_tab, sin_tab).astype(jnp.bfloat16).reshape(SEQ_LEN, NUM_HEADS * HEAD_DIM)
    dk_pre = rope_transpose(kv_grads[0] * SCALE, cos_tab, sin_tab).astype(jnp.bfloat16).reshape(SEQ_LEN, NUM_KV_HEADS * HEAD_DIM)
    dv_pre = kv_grads[1].astype(jnp.bfloat16).reshape(SEQ_LEN, NUM_KV_HEADS * HEAD_DIM)
    grad_w_query = jnp.dot(normed.T, dq_pre, preferred_element_type=jnp.float32)
    grad_w_key = jnp.dot(normed.T, dk_pre, preferred_element_type=jnp.float32)
    grad_w_value = jnp.dot(normed.T, dv_pre, preferred_element_type=jnp.float32)
    grad_normed = (jnp.dot(dq_pre, w_query.T, preferred_element_type=jnp.float32) + jnp.dot(dk_pre, w_key.T, preferred_element_type=jnp.float32) + jnp.dot(dv_pre, w_value.T, preferred_element_type=jnp.float32))
    grad_xhat = grad_normed * norm_gain
    grad_gain = jnp.sum(grad_normed * x_hat, axis=0)
    grad_x = inv_rms[:, None] * (grad_xhat - x_hat * jnp.mean(grad_xhat * x_hat, axis=-1, keepdims=True))
    grad_hidden = (grad_out.astype(jnp.float32) + grad_x).astype(jnp.bfloat16)
    return result, grad_hidden, (grad_w_query, grad_w_key, grad_w_value, grad_w_out, grad_gain)


def reference(hidden, tok_pos, grad_out, norm_gain, w_query, w_key, w_value, w_out):
    def per_seq(totals, seq_args):
        result, grad_hidden, seq_grads = seq_pass(seq_args[0], seq_args[1], seq_args[2], norm_gain, w_query, w_key, w_value, w_out)
        return jax.tree.map(jnp.add, totals, seq_grads), (result, grad_hidden)

    init_totals = (jnp.zeros(w_query.shape, jnp.float32), jnp.zeros(w_key.shape, jnp.float32), jnp.zeros(w_value.shape, jnp.float32), jnp.zeros(w_out.shape, jnp.float32), jnp.zeros(norm_gain.shape, jnp.float32))
    totals, seq_outs = lax.scan(per_seq, init_totals, (hidden, tok_pos, grad_out))
    return seq_outs[0], seq_outs[1], totals[0], totals[1], totals[2], totals[3], totals[4]
```

```python
import functools
import math

import jax
import jax.numpy as jnp
from jax import lax
from jax.experimental import pallas as pl
from jax.experimental.pallas import tpu as pltpu
from jax.sharding import PartitionSpec as P

HEAD = 128
THETA = 1000000.0
EPS = 1e-5
NEG = -1e30
SCALE = HEAD ** -0.5
LOG2E = math.log2(math.e)
AXES = ('fsdp', 'cp')
MESH = pl.DeviceIdType.MESH
F32 = jnp.float32
BF16 = jnp.bfloat16
NT = (((1,), (1,)), ((), ()))
TN = (((0,), (0,)), ((), ()))
NN = (((1,), (0,)), ((), ()))


def dot(a, b, dims=NN):
    return lax.dot_general(a, b, dims, preferred_element_type=F32)


def rope(v, cos2, sin2):
    return v * cos2 + pltpu.roll(v, HEAD // 2, 1) * sin2


def unrope(v, cos2, sin2):
    return v * cos2 - pltpu.roll(v, HEAD // 2, 1) * sin2


def attn_kernel(n_seq, rows, groups, gsize,
                q_ref, do_ref, kvo_ref, kvx_ref, pq_ref, pk_ref, px_ref, cos_ref, sin_ref,
                o_ref, dq_ref, dkv_ref,
                mask, p_s, ds_s, own, snd, rcv, send_sem, recv_sem):
    step = pl.program_id(0)
    n_steps = n_seq * groups
    seq = step // groups
    grp = step % groups
    cp = lax.axis_index('cp')
    peer = {'cp': 1 - cp}

    @pl.when(step == 0)
    def _():
        barrier = pltpu.get_barrier_semaphore()
        pl.semaphore_signal(barrier, inc=1, device_id=peer, device_id_type=MESH)
        pl.semaphore_wait(barrier, 1)

    @pl.when(grp == 0)
    def _():
        pq = pq_ref[...]
        mask[:, :rows] = jnp.where(pk_ref[0] <= pq, 0.0, NEG)
        mask[:, rows:] = jnp.where(px_ref[0] <= pq, 0.0, NEG)

    row0 = pl.multiple_of(seq * rows, rows)
    cos2 = cos_ref[pl.ds(row0, rows), :]
    sin2 = sin_ref[pl.ds(row0, rows), :]
    k = jnp.concatenate([kvo_ref[:, :HEAD], kvx_ref[:, :HEAD]], axis=0)
    v = jnp.concatenate([kvo_ref[:, HEAD:], kvx_ref[:, HEAD:]], axis=0)
    for h in range(gsize):
        cols = slice(h * HEAD, (h + 1) * HEAD)
        hrow = slice(h * rows, (h + 1) * rows)
        q = q_ref[:, cols]
        do = do_ref[:, cols]
        s = dot(q, k, NT) * (SCALE * LOG2E) + mask[...]
        m = jnp.max(s, axis=1, keepdims=True)
        e = jnp.exp2(s - m)
        l = jnp.sum(e, axis=1, keepdims=True)
        rl = 1.0 / l
        o = (dot(e.astype(BF16), v) * rl).astype(BF16)
        o_ref[:, cols] = o
        delta = jnp.sum(do.astype(F32) * o.astype(F32), axis=1, keepdims=True)
        p = e * rl
        p_s[hrow, :] = p.astype(BF16)
        ds = (p * (dot(do, v, NT) - delta)).astype(BF16)
        ds_s[hrow, :] = ds
        dq_ref[:, cols] = unrope(dot(ds, k) * SCALE, cos2, sin2).astype(BF16)
    do6 = jnp.concatenate([do_ref[:, h * HEAD:(h + 1) * HEAD] for h in range(gsize)], axis=0)
    q6 = jnp.concatenate([q_ref[:, h * HEAD:(h + 1) * HEAD] for h in range(gsize)], axis=0)
    dv = dot(p_s[...], do6, TN)
    dk = dot(ds_s[...], q6, TN) * SCALE
    own[step, :, :HEAD] = dk[:rows]
    own[step, :, HEAD:] = dv[:rows]
    snd[step, :, :HEAD] = dk[rows:]
    snd[step, :, HEAD:] = dv[rows:]

    def copy(i):
        return pltpu.make_async_remote_copy(snd.at[i], rcv.at[i], send_sem.at[i], recv_sem.at[i],
                                            device_id=peer, device_id_type=MESH)

    copy(step).start()

    @pl.when(step == n_steps - 1)
    def _():
        def fin(i, carry):
            copy(i).wait()
            r0 = pl.multiple_of((i // groups) * rows, rows)
            tot = own[i] + rcv[i]
            c2 = cos_ref[pl.ds(r0, rows), :]
            s2 = sin_ref[pl.ds(r0, rows), :]
            dkv_ref[i, :, :HEAD] = unrope(tot[:, :HEAD], c2, s2).astype(BF16)
            dkv_ref[i, :, HEAD:] = tot[:, HEAD:].astype(BF16)
            return carry
        lax.fori_loop(0, n_steps, fin, 0)


def attention(q, do, kv_own, kv_oth, pos, pos_oth, cos2, sin2):
    n_seq, rows = pos.shape
    groups = kv_own.shape[1] // (2 * HEAD)
    gsize = q.shape[1] // HEAD // groups
    steps = n_seq * groups
    gcols = gsize * HEAD
    tokens = n_seq * rows
    blk = lambda c: pl.BlockSpec((rows, c), lambda i: (i // groups, i % groups))
    row3 = pl.BlockSpec((1, 1, rows), lambda i: (i // groups, 0, 0))
    full = lambda *s: pl.BlockSpec(s, lambda i: (0,) * len(s))
    o, dq, dkv = pl.pallas_call(
        functools.partial(attn_kernel, n_seq, rows, groups, gsize),
        grid=(steps,),
        in_specs=[blk(gcols), blk(gcols), blk(2 * HEAD), blk(2 * HEAD),
                  pl.BlockSpec((rows, 1), lambda i: (i // groups, 0)), row3, row3,
                  full(tokens, HEAD), full(tokens, HEAD)],
        out_specs=[blk(gcols), blk(gcols), full(steps, rows, 2 * HEAD)],
        out_shape=[jax.ShapeDtypeStruct(q.shape, BF16), jax.ShapeDtypeStruct(q.shape, BF16),
                   jax.ShapeDtypeStruct((steps, rows, 2 * HEAD), BF16)],
        scratch_shapes=[
            pltpu.VMEM((rows, 2 * rows), F32),
            pltpu.VMEM((gsize * rows, 2 * rows), BF16),
            pltpu.VMEM((gsize * rows, 2 * rows), BF16),
            pltpu.VMEM((steps, rows, 2 * HEAD), F32),
            pltpu.VMEM((steps, rows, 2 * HEAD), F32),
            pltpu.VMEM((steps, rows, 2 * HEAD), F32),
            pltpu.SemaphoreType.DMA((steps,)),
            pltpu.SemaphoreType.DMA((steps,)),
        ],
        compiler_params=pltpu.CompilerParams(
            collective_id=0, has_side_effects=True, dimension_semantics=('arbitrary',),
            vmem_limit_bytes=60 * 2 ** 20),
        cost_estimate=pl.CostEstimate(flops=2 * 7 * tokens * 2 * rows * gcols * groups,
                                      bytes_accessed=24 * 2 ** 20, transcendentals=0),
    )(q, do, kv_own, kv_oth, pos.reshape(tokens, 1), pos[:, None, :], pos_oth[:, None, :], cos2, sin2)
    return o, dq, dkv.reshape(n_seq, groups, rows, 2, HEAD)


def solution(mesh):
    cp_size = mesh.shape['cp']
    perm = [(i, (i + 1) % cp_size) for i in range(cp_size)]

    def shard_fn(hidden, tok_pos, grad_out, norm_gain, w_query, w_key, w_value, w_out):
        n_seq, rows, dim = hidden.shape
        tokens = n_seq * rows
        n_q = w_query.shape[1]
        n_kv = w_key.shape[1]
        groups = n_kv // HEAD
        gather = lambda a: lax.all_gather(a, AXES, axis=0, tiled=True)
        w_kv = jnp.stack([w_key.reshape(-1, groups, HEAD), w_value.reshape(-1, groups, HEAD)], axis=2)
        w_kv = w_kv.reshape(-1, 2 * n_kv)
        w_in = gather(jnp.concatenate([w_query, w_kv], axis=1))
        w_o = gather(w_out)
        gain = gather(norm_gain)
        inv_freq = THETA ** (-jnp.arange(HEAD // 2, dtype=F32) / (HEAD // 2))
        ang = tok_pos.reshape(tokens, 1).astype(F32) * inv_freq
        cos, sin = jnp.cos(ang), jnp.sin(ang)
        cos2 = jnp.concatenate([cos, cos], axis=1)
        sin2 = jnp.concatenate([-sin, sin], axis=1)
        x = hidden.reshape(tokens, dim).astype(F32)
        dy = grad_out.reshape(tokens, dim)
        inv = lax.rsqrt(jnp.mean(x * x, axis=1, keepdims=True) + EPS)
        r = (x * inv * gain).astype(BF16)

        def rope_heads(lin):
            lin = lin.reshape(tokens, -1, HEAD)
            half = HEAD // 2
            rot = jnp.concatenate([lin[..., half:], lin[..., :half]], axis=-1)
            return (lin * cos2[:, None] + rot * sin2[:, None]).astype(BF16)

        q = rope_heads(dot(r, w_in[:, :n_q])).reshape(tokens, n_q)
        kv = dot(r, w_in[:, n_q:]).reshape(tokens, groups, 2, HEAD)
        k = rope_heads(kv[:, :, 0])
        kv = jnp.stack([k, kv[:, :, 1].astype(BF16)], axis=2).reshape(tokens, 2 * n_kv)
        kv_oth = lax.ppermute(kv, 'cp', perm)
        pos_oth = lax.ppermute(tok_pos, 'cp', perm)
        do = dot(dy, w_o, NT).astype(BF16)
        o, dq, dkv = attention(q, do, kv, kv_oth, tok_pos, pos_oth, cos2, sin2)
        result = (x + dot(o, w_o)).astype(BF16)
        g_wo = dot(o, dy, TN)
        dkv = jnp.transpose(dkv, (0, 2, 1, 3, 4)).reshape(tokens, 2 * n_kv)
        d_in = jnp.concatenate([dq, dkv], axis=1)
        g_in = dot(r, d_in, TN)
        dr = dot(d_in, w_in, NT)
        xh = x * inv
        g_gain = jnp.sum(dr * xh, axis=0)
        a = dr * gain
        gx = inv * (a - xh * jnp.mean(a * xh, axis=1, keepdims=True))
        grad_hidden = (dy.astype(F32) + gx).astype(BF16)
        scatter = lambda a: lax.psum_scatter(a, AXES, scatter_dimension=0, tiled=True)
        g_wo = scatter(g_wo)
        g_in = scatter(g_in)
        g_gain = scatter(g_gain)
        g_kv = g_in[:, n_q:].reshape(-1, groups, 2, HEAD)
        return (result.reshape(hidden.shape), grad_hidden.reshape(hidden.shape), g_in[:, :n_q],
                g_kv[:, :, 0].reshape(-1, n_kv), g_kv[:, :, 1].reshape(-1, n_kv), g_wo, g_gain)

    row = P('fsdp', 'cp', None)
    pos = P('fsdp', 'cp')
    w = P(AXES, None)
    g = P(AXES)
    return jax.shard_map(shard_fn, mesh=mesh, in_specs=(row, pos, row, g, w, w, w, w),
                         out_specs=(row, row, w, w, w, w, g), check_vma=False)
```

```python
import functools
import math

import jax
import jax.numpy as jnp
from jax import lax
from jax.experimental import pallas as pl
from jax.experimental.pallas import tpu as pltpu
from jax.sharding import PartitionSpec as P

HEAD = 128
THETA = 1000000.0
EPS = 1e-5
NEG = -1e30
SCALE = HEAD ** -0.5
LOG2E = math.log2(math.e)
AXES = ('fsdp', 'cp')
MESH = pl.DeviceIdType.MESH
F32 = jnp.float32
BF16 = jnp.bfloat16
NT = (((1,), (1,)), ((), ()))
TN = (((0,), (0,)), ((), ()))
NN = (((1,), (0,)), ((), ()))


def dot(a, b, dims=NN):
    return lax.dot_general(a, b, dims, preferred_element_type=F32)


def rope(v, cos2, sin2):
    return v * cos2 + pltpu.roll(v, HEAD // 2, 1) * sin2


def unrope(v, cos2, sin2):
    return v * cos2 - pltpu.roll(v, HEAD // 2, 1) * sin2


def attn_kernel(n_seq, rows, groups, gsize,
                q_ref, do_ref, kvo_ref, kvx_ref, pq_ref, pk_ref, px_ref, cos_ref, sin_ref,
                o_ref, dq_ref, dkv_ref,
                mask, p_s, ds_s, own, snd, rcv, send_sem, recv_sem):
    step = pl.program_id(0)
    n_steps = n_seq * groups
    seq = step // groups
    grp = step % groups
    cp = lax.axis_index('cp')
    peer = {'cp': 1 - cp}

    @pl.when(step == 0)
    def _():
        barrier = pltpu.get_barrier_semaphore()
        pl.semaphore_signal(barrier, inc=1, device_id=peer, device_id_type=MESH)
        pl.semaphore_wait(barrier, 1)

    @pl.when(grp == 0)
    def _():
        pq = pq_ref[...]
        mask[:, :rows] = jnp.where(pk_ref[0] <= pq, 0.0, NEG)
        mask[:, rows:] = jnp.where(px_ref[0] <= pq, 0.0, NEG)

    row0 = pl.multiple_of(seq * rows, rows)
    cos2 = cos_ref[pl.ds(row0, rows), :]
    sin2 = sin_ref[pl.ds(row0, rows), :]
    k = jnp.concatenate([kvo_ref[:, :HEAD], kvx_ref[:, :HEAD]], axis=0)
    v = jnp.concatenate([kvo_ref[:, HEAD:], kvx_ref[:, HEAD:]], axis=0)
    for h in range(gsize):
        cols = slice(h * HEAD, (h + 1) * HEAD)
        hrow = slice(h * rows, (h + 1) * rows)
        q = q_ref[:, cols]
        do = do_ref[:, cols]
        s = dot(q, k, NT) * (SCALE * LOG2E) + mask[...]
        m = jnp.max(s, axis=1, keepdims=True)
        e = jnp.exp2(s - m)
        l = jnp.sum(e, axis=1, keepdims=True)
        rl = 1.0 / l
        o = (dot(e.astype(BF16), v) * rl).astype(BF16)
        o_ref[:, cols] = o
        delta = jnp.sum(do.astype(F32) * o.astype(F32), axis=1, keepdims=True)
        p = e * rl
        p_s[hrow, :] = p.astype(BF16)
        ds = (p * (dot(do, v, NT) - delta)).astype(BF16)
        ds_s[hrow, :] = ds
        dq_ref[:, cols] = unrope(dot(ds, k) * SCALE, cos2, sin2).astype(BF16)
    do6 = jnp.concatenate([do_ref[:, h * HEAD:(h + 1) * HEAD] for h in range(gsize)], axis=0)
    q6 = jnp.concatenate([q_ref[:, h * HEAD:(h + 1) * HEAD] for h in range(gsize)], axis=0)
    dv = dot(p_s[...], do6, TN)
    dk = dot(ds_s[...], q6, TN) * SCALE
    own[step, :, :HEAD] = dk[:rows]
    own[step, :, HEAD:] = dv[:rows]
    snd[step, :, :HEAD] = dk[rows:]
    snd[step, :, HEAD:] = dv[rows:]

    def copy(i):
        return pltpu.make_async_remote_copy(snd.at[i], rcv.at[i], send_sem.at[i], recv_sem.at[i],
                                            device_id=peer, device_id_type=MESH)

    copy(step).start()

    @pl.when(step == n_steps - 1)
    def _():
        def fin(i, carry):
            copy(i).wait()
            r0 = pl.multiple_of((i // groups) * rows, rows)
            tot = own[i] + rcv[i]
            c2 = cos_ref[pl.ds(r0, rows), :]
            s2 = sin_ref[pl.ds(r0, rows), :]
            dkv_ref[i, :, :HEAD] = unrope(tot[:, :HEAD], c2, s2).astype(BF16)
            dkv_ref[i, :, HEAD:] = tot[:, HEAD:].astype(BF16)
            return carry
        lax.fori_loop(0, n_steps, fin, 0)


def attention(q, do, kv_own, kv_oth, pos, pos_oth, cos2, sin2):
    n_seq, rows = pos.shape
    groups = kv_own.shape[1] // (2 * HEAD)
    gsize = q.shape[1] // HEAD // groups
    steps = n_seq * groups
    gcols = gsize * HEAD
    tokens = n_seq * rows
    blk = lambda c: pl.BlockSpec((rows, c), lambda i: (i // groups, i % groups))
    row3 = pl.BlockSpec((1, 1, rows), lambda i: (i // groups, 0, 0))
    full = lambda *s: pl.BlockSpec(s, lambda i: (0,) * len(s))
    o, dq, dkv = pl.pallas_call(
        functools.partial(attn_kernel, n_seq, rows, groups, gsize),
        grid=(steps,),
        in_specs=[blk(gcols), blk(gcols), blk(2 * HEAD), blk(2 * HEAD),
                  pl.BlockSpec((rows, 1), lambda i: (i // groups, 0)), row3, row3,
                  full(tokens, HEAD), full(tokens, HEAD)],
        out_specs=[blk(gcols), blk(gcols), full(steps, rows, 2 * HEAD)],
        out_shape=[jax.ShapeDtypeStruct(q.shape, BF16), jax.ShapeDtypeStruct(q.shape, BF16),
                   jax.ShapeDtypeStruct((steps, rows, 2 * HEAD), BF16)],
        scratch_shapes=[
            pltpu.VMEM((rows, 2 * rows), F32),
            pltpu.VMEM((gsize * rows, 2 * rows), BF16),
            pltpu.VMEM((gsize * rows, 2 * rows), BF16),
            pltpu.VMEM((steps, rows, 2 * HEAD), F32),
            pltpu.VMEM((steps, rows, 2 * HEAD), F32),
            pltpu.VMEM((steps, rows, 2 * HEAD), F32),
            pltpu.SemaphoreType.DMA((steps,)),
            pltpu.SemaphoreType.DMA((steps,)),
        ],
        compiler_params=pltpu.CompilerParams(
            collective_id=0, has_side_effects=True, dimension_semantics=('arbitrary',),
            vmem_limit_bytes=60 * 2 ** 20),
        cost_estimate=pl.CostEstimate(flops=2 * 7 * tokens * 2 * rows * gcols * groups,
                                      bytes_accessed=24 * 2 ** 20, transcendentals=0),
    )(q, do, kv_own, kv_oth, pos.reshape(tokens, 1), pos[:, None, :], pos_oth[:, None, :], cos2, sin2)
    return o, dq, dkv.reshape(n_seq, groups, rows, 2, HEAD)

COLORS = ('xyz', 'yzx', 'zxy')


def place():
    f = lax.axis_index('fsdp')
    z = lax.axis_index('cp')
    bits = {'y': f // 4, 'x': (f // 2) % 2, 'c': f % 2, 'z': z}
    peers = {'y': {'fsdp': f + 4 - 8 * bits['y']}, 'x': {'fsdp': f + 2 - 4 * bits['x']},
             'c': {'fsdp': f + 1 - 2 * bits['c']}, 'z': {'cp': 1 - z}}
    return bits, peers


def meet(peers):
    barrier = pltpu.get_barrier_semaphore()
    for a in 'cxyz':
        pl.semaphore_signal(barrier, inc=1, device_id=peers[a], device_id_type=MESH)
    pl.semaphore_wait(barrier, 4)


def wgrad_kernel(shapes, o_hbm, dy_hbm, r_hbm, dq_hbm, dkv_hbm, gp_ref,
                 gin_ref, gwo_ref, gg_ref,
                 lhs, rhs, g, rcv_a, h, rcv1, rcv2, rcv3, gain_rcv,
                 load_sem, d2d_send, d2d_recv, ici_send, ici_recv, gain_send, gain_recv, credit):
    tokens, dim, width, sub = shapes
    bits, peers = place()
    core = bits['c']
    chunks = [(0, dy_hbm, j, gwo_ref, j) for j in range(dim // width)]
    chunks += [(1, dq_hbm, j, gin_ref, j) for j in range(dim // width)]
    chunks += [(1, dkv_hbm, 0, gin_ref, dim // width)]
    n = len(chunks)
    seg = dim // 4
    half = seg // 2

    def load_lhs(i):
        return pltpu.make_async_copy((o_hbm, r_hbm)[i], lhs.at[i], load_sem.at[i])

    def load_rhs(t):
        src, j = chunks[t][1], chunks[t][2]
        return pltpu.make_async_copy(src.at[:, pl.ds(j * width, width)], rhs.at[t % 2], load_sem.at[2 + t])

    load_lhs(0).start()
    load_rhs(0).start()
    load_lhs(1).start()
    load_rhs(1).start()
    meet(peers)

    def d2d(t):
        return pltpu.make_async_remote_copy(g.at[t % 2, :, 1 - core], rcv_a.at[t % 2], d2d_send.at[t], d2d_recv.at[t],
                                            device_id=peers['c'], device_id_type=MESH)

    def ici(t, c, p):
        b1, b2, b3 = (bits[a] for a in COLORS[c])
        if p == 0:
            src, dst = h.at[t, c, pl.ds((1 - b1) * 4, 4)], rcv1.at[t, c]
        elif p == 1:
            src, dst = h.at[t, c, pl.ds(b1 * 4 + (1 - b2) * 2, 2)], rcv2.at[t, c]
        else:
            src, dst = h.at[t, c, pl.ds(b1 * 4 + b2 * 2 + (1 - b3), 1)], rcv3.at[t, c]
        return pltpu.make_async_remote_copy(src, dst, ici_send.at[t, c, p], ici_recv.at[t, c, p],
                                            device_id=peers[COLORS[c][p]], device_id_type=MESH)

    def compute(t):
        li = chunks[t][0]
        if t == 0 or chunks[t - 1][0] != li:
            load_lhs(li).wait()
        load_rhs(t).wait()

        def body(yx, carry):
            cols = pl.ds(pl.multiple_of(yx * seg, HEAD), seg)
            res = dot(lhs[li, :, cols], rhs[t % 2], TN)
            g[t % 2, yx, 0] = res[:half]
            g[t % 2, yx, 1] = res[half:]
            return carry
        lax.fori_loop(0, 4, body, 0)
        if t + 2 < n:
            load_rhs(t + 2).start()
        if t >= 2:
            pl.semaphore_wait(credit, 1)
        d2d(t).start()

    def fold(t):
        d2d(t).wait()
        for y in range(2):
            for x in range(2):
                for z in range(2):
                    at = {'y': y, 'x': x, 'z': z}
                    for c in range(3):
                        a1, a2, a3 = (at[a] for a in COLORS[c])
                        rows = slice(z * 3 * sub + c * sub, z * 3 * sub + (c + 1) * sub)
                        h[t, c, a1 * 4 + a2 * 2 + a3] = g[t % 2, y * 2 + x, core, rows] + rcv_a[t % 2, y * 2 + x, rows]
        for c in range(3):
            ici(t, c, 0).start()
        if t + 2 < n:
            pl.semaphore_signal(credit, inc=1, device_id=peers['c'], device_id_type=MESH)

    def reduce(t, p):
        for c in range(3):
            b1, b2, b3 = (bits[a] for a in COLORS[c])
            ici(t, c, p).wait()
            if p == 0:
                for j in range(4):
                    h[t, c, b1 * 4 + j] = h[t, c, b1 * 4 + j] + rcv1[t, c, j]
                ici(t, c, 1).start()
            elif p == 1:
                for j in range(2):
                    k = b1 * 4 + b2 * 2 + j
                    h[t, c, k] = h[t, c, k] + rcv2[t, c, j]
                ici(t, c, 2).start()
            else:
                out, j = chunks[t][3], chunks[t][4]
                k = b1 * 4 + b2 * 2 + b3
                out[c * sub:(c + 1) * sub, j * width:(j + 1) * width] = h[t, c, k] + rcv3[t, c, 0]

    gg_ref[...] = gp_ref[...]

    def gain_copy(i):
        return pltpu.make_async_remote_copy(gg_ref, gain_rcv.at[i], gain_send.at[i], gain_recv.at[i],
                                            device_id=peers['cxyz'[i]], device_id_type=MESH)

    gain_copy(0).start()
    for i in range(n + 4):
        if i < n:
            compute(i)
        if 0 <= i - 1 < n:
            fold(i - 1)
        if i < 4:
            gain_copy(i).wait()
            gg_ref[...] = gg_ref[...] + gain_rcv[i]
            if i < 3:
                gain_copy(i + 1).start()
        for p in range(3):
            if 0 <= i - 2 - p < n:
                reduce(i - 2 - p, p)


def wgrad(o, dy, r, dq, dkv, gp):
    tokens, dim = o.shape
    width = dkv.shape[1]
    shard = dim // 16
    sub = shard // 3
    n = 2 * (dim // width) + 1
    hbm = pl.BlockSpec(memory_space=pl.ANY)
    vm = pl.BlockSpec(memory_space=pltpu.VMEM)
    dma = pltpu.SemaphoreType.DMA
    return pl.pallas_call(
        functools.partial(wgrad_kernel, (tokens, dim, width, sub)),
        in_specs=[hbm] * 5 + [vm],
        out_specs=[vm] * 3,
        out_shape=[jax.ShapeDtypeStruct((shard, dim + width), F32), jax.ShapeDtypeStruct((shard, dim), F32),
                   jax.ShapeDtypeStruct((1, dim), F32)],
        scratch_shapes=[
            pltpu.VMEM((2, tokens, dim), BF16),
            pltpu.VMEM((2, tokens, width), BF16),
            pltpu.VMEM((2, 4, 2, dim // 8, width), F32),
            pltpu.VMEM((2, 4, dim // 8, width), F32),
            pltpu.VMEM((n, 3, 8, sub, width), F32),
            pltpu.VMEM((n, 3, 4, sub, width), F32),
            pltpu.VMEM((n, 3, 2, sub, width), F32),
            pltpu.VMEM((n, 3, 1, sub, width), F32),
            pltpu.VMEM((4, 1, dim), F32),
            dma((2 + n,)), dma((n,)), dma((n,)), dma((n, 3, 3)), dma((n, 3, 3)), dma((4,)), dma((4,)),
            pltpu.SemaphoreType.REGULAR,
        ],
        compiler_params=pltpu.CompilerParams(collective_id=1, has_side_effects=True, vmem_limit_bytes=60 * 2 ** 20),
        cost_estimate=pl.CostEstimate(flops=2 * tokens * dim * (2 * dim + width), bytes_accessed=30 * 2 ** 20,
                                      transcendentals=0),
    )(o, dy, r, dq, dkv, gp)


def solution(mesh):
    cp_size = mesh.shape['cp']
    perm = [(i, (i + 1) % cp_size) for i in range(cp_size)]

    def shard_fn(hidden, tok_pos, grad_out, norm_gain, w_query, w_key, w_value, w_out):
        n_seq, rows, dim = hidden.shape
        tokens = n_seq * rows
        n_q = w_query.shape[1]
        n_kv = w_key.shape[1]
        groups = n_kv // HEAD
        gather = lambda a: lax.all_gather(a, AXES, axis=0, tiled=True)
        w_kv = jnp.stack([w_key.reshape(-1, groups, HEAD), w_value.reshape(-1, groups, HEAD)], axis=2)
        w_kv = w_kv.reshape(-1, 2 * n_kv)
        w_in = gather(jnp.concatenate([w_query, w_kv], axis=1))
        w_o = gather(w_out)
        gain = gather(norm_gain)
        inv_freq = THETA ** (-jnp.arange(HEAD // 2, dtype=F32) / (HEAD // 2))
        ang = tok_pos.reshape(tokens, 1).astype(F32) * inv_freq
        cos, sin = jnp.cos(ang), jnp.sin(ang)
        cos2 = jnp.concatenate([cos, cos], axis=1)
        sin2 = jnp.concatenate([-sin, sin], axis=1)
        x = hidden.reshape(tokens, dim).astype(F32)
        dy = grad_out.reshape(tokens, dim)
        inv = lax.rsqrt(jnp.mean(x * x, axis=1, keepdims=True) + EPS)
        r = (x * inv * gain).astype(BF16)

        def rope_heads(lin):
            lin = lin.reshape(tokens, -1, HEAD)
            half = HEAD // 2
            rot = jnp.concatenate([lin[..., half:], lin[..., :half]], axis=-1)
            return (lin * cos2[:, None] + rot * sin2[:, None]).astype(BF16)

        q = rope_heads(dot(r, w_in[:, :n_q])).reshape(tokens, n_q)
        kv = dot(r, w_in[:, n_q:]).reshape(tokens, groups, 2, HEAD)
        k = rope_heads(kv[:, :, 0])
        kv = jnp.stack([k, kv[:, :, 1].astype(BF16)], axis=2).reshape(tokens, 2 * n_kv)
        kv_oth = lax.ppermute(kv, 'cp', perm)
        pos_oth = lax.ppermute(tok_pos, 'cp', perm)
        do = dot(dy, w_o, NT).astype(BF16)
        o, dq, dkv = attention(q, do, kv, kv_oth, tok_pos, pos_oth, cos2, sin2)
        result = (x + dot(o, w_o)).astype(BF16)
        dkv = jnp.transpose(dkv, (0, 2, 1, 3, 4)).reshape(tokens, 2 * n_kv)
        d_in = jnp.concatenate([dq, dkv], axis=1)
        dr = dot(d_in, w_in, NT)
        xh = x * inv
        gp = jnp.sum(dr * xh, axis=0, keepdims=True)
        a = dr * gain
        gx = inv * (a - xh * jnp.mean(a * xh, axis=1, keepdims=True))
        grad_hidden = (dy.astype(F32) + gx).astype(BF16)
        g_in, g_wo, gg = wgrad(o, dy, r, dq, dkv, gp)
        shard = lax.axis_index('fsdp') * cp_size + lax.axis_index('cp')
        g_gain = lax.dynamic_slice(gg[0], (shard * norm_gain.shape[0],), norm_gain.shape)
        g_kv = g_in[:, n_q:].reshape(-1, groups, 2, HEAD)
        return (result.reshape(hidden.shape), grad_hidden.reshape(hidden.shape), g_in[:, :n_q],
                g_kv[:, :, 0].reshape(-1, n_kv), g_kv[:, :, 1].reshape(-1, n_kv), g_wo, g_gain)

    row = P('fsdp', 'cp', None)
    pos = P('fsdp', 'cp')
    w = P(AXES, None)
    g = P(AXES)
    return jax.shard_map(shard_fn, mesh=mesh, in_specs=(row, pos, row, g, w, w, w, w),
                         out_specs=(row, row, w, w, w, w, g), check_vma=False)
```

```python
import functools
import math

import jax
import jax.numpy as jnp
from jax import lax
from jax.experimental import pallas as pl
from jax.experimental.pallas import tpu as pltpu
from jax.sharding import PartitionSpec as P

HEAD = 128
THETA = 1000000.0
EPS = 1e-5
NEG = -1e30
SCALE = HEAD ** -0.5
LOG2E = math.log2(math.e)
AXES = ('fsdp', 'cp')
MESH = pl.DeviceIdType.MESH
F32 = jnp.float32
BF16 = jnp.bfloat16
NT = (((1,), (1,)), ((), ()))
TN = (((0,), (0,)), ((), ()))
NN = (((1,), (0,)), ((), ()))


def dot(a, b, dims=NN):
    return lax.dot_general(a, b, dims, preferred_element_type=F32)


def rope(v, cos2, sin2):
    return v * cos2 + pltpu.roll(v, HEAD // 2, 1) * sin2


def unrope(v, cos2, sin2):
    return v * cos2 - pltpu.roll(v, HEAD // 2, 1) * sin2


def attn_kernel(n_seq, rows, groups, gsize,
                q_ref, do_ref, kvo_ref, kvx_ref, pq_ref, pk_ref, px_ref, cos_ref, sin_ref,
                o_ref, dq_ref, dkv_ref,
                mask, p_s, ds_s, own, snd, rcv, send_sem, recv_sem):
    step = pl.program_id(0)
    n_steps = n_seq * groups
    seq = step // groups
    grp = step % groups
    cp = lax.axis_index('cp')
    peer = {'cp': 1 - cp}

    @pl.when(step == 0)
    def _():
        barrier = pltpu.get_barrier_semaphore()
        pl.semaphore_signal(barrier, inc=1, device_id=peer, device_id_type=MESH)
        pl.semaphore_wait(barrier, 1)

    @pl.when(grp == 0)
    def _():
        pq = pq_ref[...]
        mask[:, :rows] = jnp.where(pk_ref[0] <= pq, 0.0, NEG)
        mask[:, rows:] = jnp.where(px_ref[0] <= pq, 0.0, NEG)

    row0 = pl.multiple_of(seq * rows, rows)
    cos2 = cos_ref[pl.ds(row0, rows), :]
    sin2 = sin_ref[pl.ds(row0, rows), :]
    k = jnp.concatenate([kvo_ref[:, :HEAD], kvx_ref[:, :HEAD]], axis=0)
    v = jnp.concatenate([kvo_ref[:, HEAD:], kvx_ref[:, HEAD:]], axis=0)
    for h in range(gsize):
        cols = slice(h * HEAD, (h + 1) * HEAD)
        hrow = slice(h * rows, (h + 1) * rows)
        q = q_ref[:, cols]
        do = do_ref[:, cols]
        s = dot(q, k, NT) * (SCALE * LOG2E) + mask[...]
        m = jnp.max(s, axis=1, keepdims=True)
        e = jnp.exp2(s - m)
        l = jnp.sum(e, axis=1, keepdims=True)
        rl = 1.0 / l
        o = (dot(e.astype(BF16), v) * rl).astype(BF16)
        o_ref[:, cols] = o
        delta = jnp.sum(do.astype(F32) * o.astype(F32), axis=1, keepdims=True)
        p = e * rl
        p_s[hrow, :] = p.astype(BF16)
        ds = (p * (dot(do, v, NT) - delta)).astype(BF16)
        ds_s[hrow, :] = ds
        dq_ref[:, cols] = unrope(dot(ds, k) * SCALE, cos2, sin2).astype(BF16)
    do6 = jnp.concatenate([do_ref[:, h * HEAD:(h + 1) * HEAD] for h in range(gsize)], axis=0)
    q6 = jnp.concatenate([q_ref[:, h * HEAD:(h + 1) * HEAD] for h in range(gsize)], axis=0)
    dv = dot(p_s[...], do6, TN)
    dk = dot(ds_s[...], q6, TN) * SCALE
    own[step, :, :HEAD] = dk[:rows]
    own[step, :, HEAD:] = dv[:rows]
    snd[step, :, :HEAD] = dk[rows:]
    snd[step, :, HEAD:] = dv[rows:]

    def copy(i):
        return pltpu.make_async_remote_copy(snd.at[i], rcv.at[i], send_sem.at[i], recv_sem.at[i],
                                            device_id=peer, device_id_type=MESH)

    copy(step).start()

    @pl.when(step == n_steps - 1)
    def _():
        def fin(i, carry):
            copy(i).wait()
            r0 = pl.multiple_of((i // groups) * rows, rows)
            tot = own[i] + rcv[i]
            c2 = cos_ref[pl.ds(r0, rows), :]
            s2 = sin_ref[pl.ds(r0, rows), :]
            dkv_ref[i, :, :HEAD] = unrope(tot[:, :HEAD], c2, s2).astype(BF16)
            dkv_ref[i, :, HEAD:] = tot[:, HEAD:].astype(BF16)
            return carry
        lax.fori_loop(0, n_steps, fin, 0)


def attention(q, do, kv_own, kv_oth, pos, pos_oth, cos2, sin2):
    n_seq, rows = pos.shape
    groups = kv_own.shape[1] // (2 * HEAD)
    gsize = q.shape[1] // HEAD // groups
    steps = n_seq * groups
    gcols = gsize * HEAD
    tokens = n_seq * rows
    blk = lambda c: pl.BlockSpec((rows, c), lambda i: (i // groups, i % groups))
    row3 = pl.BlockSpec((1, 1, rows), lambda i: (i // groups, 0, 0))
    full = lambda *s: pl.BlockSpec(s, lambda i: (0,) * len(s))
    o, dq, dkv = pl.pallas_call(
        functools.partial(attn_kernel, n_seq, rows, groups, gsize),
        grid=(steps,),
        in_specs=[blk(gcols), blk(gcols), blk(2 * HEAD), blk(2 * HEAD),
                  pl.BlockSpec((rows, 1), lambda i: (i // groups, 0)), row3, row3,
                  full(tokens, HEAD), full(tokens, HEAD)],
        out_specs=[blk(gcols), blk(gcols), full(steps, rows, 2 * HEAD)],
        out_shape=[jax.ShapeDtypeStruct(q.shape, BF16), jax.ShapeDtypeStruct(q.shape, BF16),
                   jax.ShapeDtypeStruct((steps, rows, 2 * HEAD), BF16)],
        scratch_shapes=[
            pltpu.VMEM((rows, 2 * rows), F32),
            pltpu.VMEM((gsize * rows, 2 * rows), BF16),
            pltpu.VMEM((gsize * rows, 2 * rows), BF16),
            pltpu.VMEM((steps, rows, 2 * HEAD), F32),
            pltpu.VMEM((steps, rows, 2 * HEAD), F32),
            pltpu.VMEM((steps, rows, 2 * HEAD), F32),
            pltpu.SemaphoreType.DMA((steps,)),
            pltpu.SemaphoreType.DMA((steps,)),
        ],
        compiler_params=pltpu.CompilerParams(
            collective_id=0, has_side_effects=True, dimension_semantics=('arbitrary',),
            vmem_limit_bytes=60 * 2 ** 20),
        cost_estimate=pl.CostEstimate(flops=2 * 7 * tokens * 2 * rows * gcols * groups,
                                      bytes_accessed=24 * 2 ** 20, transcendentals=0),
    )(q, do, kv_own, kv_oth, pos.reshape(tokens, 1), pos[:, None, :], pos_oth, cos2, sin2)
    return o, dq, dkv.reshape(n_seq, groups, rows, 2, HEAD)

COLORS = ('xyz', 'yzx', 'zxy')


def place():
    f = lax.axis_index('fsdp')
    z = lax.axis_index('cp')
    bits = {'y': f // 4, 'x': (f // 2) % 2, 'c': f % 2, 'z': z}
    peers = {'y': {'fsdp': f + 4 - 8 * bits['y']}, 'x': {'fsdp': f + 2 - 4 * bits['x']},
             'c': {'fsdp': f + 1 - 2 * bits['c']}, 'z': {'cp': 1 - z}}
    return bits, peers


def meet(peers):
    barrier = pltpu.get_barrier_semaphore()
    for a in 'cxyz':
        pl.semaphore_signal(barrier, inc=1, device_id=peers[a], device_id_type=MESH)
    pl.semaphore_wait(barrier, 4)


def wgrad_kernel(shapes, o_hbm, dy_hbm, r_hbm, dq_hbm, dkv_hbm, gp_ref,
                 gin_ref, gwo_ref, gg_ref,
                 lhs, rhs, g, rcv_a, h, rcv1, rcv2, rcv3, gain_rcv,
                 load_sem, d2d_send, d2d_recv, ici_send, ici_recv, gain_send, gain_recv, credit):
    tokens, dim, width, sub = shapes
    bits, peers = place()
    core = bits['c']
    chunks = [(0, dy_hbm, j, gwo_ref, j) for j in range(dim // width)]
    chunks += [(1, dq_hbm, j, gin_ref, j) for j in range(dim // width)]
    chunks += [(1, dkv_hbm, 0, gin_ref, dim // width)]
    n = len(chunks)
    seg = dim // 4
    half = seg // 2

    def load_lhs(i):
        return pltpu.make_async_copy((o_hbm, r_hbm)[i], lhs.at[i], load_sem.at[i])

    def load_rhs(t):
        src, j = chunks[t][1], chunks[t][2]
        return pltpu.make_async_copy(src.at[:, pl.ds(j * width, width)], rhs.at[t % 2], load_sem.at[2 + t])

    load_lhs(0).start()
    load_rhs(0).start()
    load_lhs(1).start()
    load_rhs(1).start()
    meet(peers)

    def d2d(t):
        return pltpu.make_async_remote_copy(g.at[t % 2, :, 1 - core], rcv_a.at[t % 2], d2d_send.at[t], d2d_recv.at[t],
                                            device_id=peers['c'], device_id_type=MESH)

    def ici(t, c, p):
        b1, b2, b3 = (bits[a] for a in COLORS[c])
        if p == 0:
            src, dst = h.at[t, c, pl.ds((1 - b1) * 4, 4)], rcv1.at[t, c]
        elif p == 1:
            src, dst = h.at[t, c, pl.ds(b1 * 4 + (1 - b2) * 2, 2)], rcv2.at[t, c]
        else:
            src, dst = h.at[t, c, pl.ds(b1 * 4 + b2 * 2 + (1 - b3), 1)], rcv3.at[t, c]
        return pltpu.make_async_remote_copy(src, dst, ici_send.at[t, c, p], ici_recv.at[t, c, p],
                                            device_id=peers[COLORS[c][p]], device_id_type=MESH)

    def compute(t):
        li = chunks[t][0]
        if t == 0 or chunks[t - 1][0] != li:
            load_lhs(li).wait()
        load_rhs(t).wait()

        def body(yx, carry):
            cols = pl.ds(pl.multiple_of(yx * seg, HEAD), seg)
            res = dot(lhs[li, :, cols], rhs[t % 2], TN)
            g[t % 2, yx, 0] = res[:half]
            g[t % 2, yx, 1] = res[half:]
            return carry
        lax.fori_loop(0, 4, body, 0)
        if t + 2 < n:
            load_rhs(t + 2).start()
        if t >= 2:
            pl.semaphore_wait(credit, 1)
        d2d(t).start()

    def fold(t):
        d2d(t).wait()
        for y in range(2):
            for x in range(2):
                for z in range(2):
                    at = {'y': y, 'x': x, 'z': z}
                    for c in range(3):
                        a1, a2, a3 = (at[a] for a in COLORS[c])
                        rows = slice(z * 3 * sub + c * sub, z * 3 * sub + (c + 1) * sub)
                        h[t, c, a1 * 4 + a2 * 2 + a3] = g[t % 2, y * 2 + x, core, rows] + rcv_a[t % 2, y * 2 + x, rows]
        for c in range(3):
            ici(t, c, 0).start()
        if t + 2 < n:
            pl.semaphore_signal(credit, inc=1, device_id=peers['c'], device_id_type=MESH)

    def reduce(t, p):
        for c in range(3):
            b1, b2, b3 = (bits[a] for a in COLORS[c])
            ici(t, c, p).wait()
            if p == 0:
                for j in range(4):
                    h[t, c, b1 * 4 + j] = h[t, c, b1 * 4 + j] + rcv1[t, c, j]
                ici(t, c, 1).start()
            elif p == 1:
                for j in range(2):
                    k = b1 * 4 + b2 * 2 + j
                    h[t, c, k] = h[t, c, k] + rcv2[t, c, j]
                ici(t, c, 2).start()
            else:
                out, j = chunks[t][3], chunks[t][4]
                k = b1 * 4 + b2 * 2 + b3
                out[c * sub:(c + 1) * sub, j * width:(j + 1) * width] = h[t, c, k] + rcv3[t, c, 0]

    gg_ref[...] = gp_ref[...]

    def gain_copy(i):
        return pltpu.make_async_remote_copy(gg_ref, gain_rcv.at[i], gain_send.at[i], gain_recv.at[i],
                                            device_id=peers['cxyz'[i]], device_id_type=MESH)

    gain_copy(0).start()
    for i in range(n + 4):
        if i < n:
            compute(i)
        if 0 <= i - 1 < n:
            fold(i - 1)
        if i < 4:
            gain_copy(i).wait()
            gg_ref[...] = gg_ref[...] + gain_rcv[i]
            if i < 3:
                gain_copy(i + 1).start()
        for p in range(3):
            if 0 <= i - 2 - p < n:
                reduce(i - 2 - p, p)


def wgrad(o, dy, r, dq, dkv, gp):
    tokens, dim = o.shape
    width = dkv.shape[1]
    shard = dim // 16
    sub = shard // 3
    n = 2 * (dim // width) + 1
    hbm = pl.BlockSpec(memory_space=pl.ANY)
    vm = pl.BlockSpec(memory_space=pltpu.VMEM)
    dma = pltpu.SemaphoreType.DMA
    return pl.pallas_call(
        functools.partial(wgrad_kernel, (tokens, dim, width, sub)),
        in_specs=[hbm] * 5 + [vm],
        out_specs=[vm] * 3,
        out_shape=[jax.ShapeDtypeStruct((shard, dim + width), F32), jax.ShapeDtypeStruct((shard, dim), F32),
                   jax.ShapeDtypeStruct((1, dim), F32)],
        scratch_shapes=[
            pltpu.VMEM((2, tokens, dim), BF16),
            pltpu.VMEM((2, tokens, width), BF16),
            pltpu.VMEM((2, 4, 2, dim // 8, width), F32),
            pltpu.VMEM((2, 4, dim // 8, width), F32),
            pltpu.VMEM((n, 3, 8, sub, width), F32),
            pltpu.VMEM((n, 3, 4, sub, width), F32),
            pltpu.VMEM((n, 3, 2, sub, width), F32),
            pltpu.VMEM((n, 3, 1, sub, width), F32),
            pltpu.VMEM((4, 1, dim), F32),
            dma((2 + n,)), dma((n,)), dma((n,)), dma((n, 3, 3)), dma((n, 3, 3)), dma((4,)), dma((4,)),
            pltpu.SemaphoreType.REGULAR,
        ],
        compiler_params=pltpu.CompilerParams(collective_id=1, has_side_effects=True, vmem_limit_bytes=60 * 2 ** 20),
        cost_estimate=pl.CostEstimate(flops=2 * tokens * dim * (2 * dim + width), bytes_accessed=30 * 2 ** 20,
                                      transcendentals=0),
    )(o, dy, r, dq, dkv, gp)


def gather_kernel(shapes, x_hbm, dy_hbm, wq_hbm, wk_hbm, wv_hbm, wo_hbm, gain_ref, pcol_ref, prow_ref, freq_ref,
                  q_hbm, do_hbm, r_hbm, kvo_hbm, kvx_hbm, wi_hbm, wf_hbm, cos_ref, sin_ref, gain_out, px_out,
                  x, dy, r, q, do, kvo, kvx, wi, wo, gbuf, grow, px,
                  load_sem, out_sem, ici_send, ici_recv, fwd_send, fwd_recv, own_send, own_recv,
                  g_send, g_recv, kv_send, kv_recv):
    n_seq, rows, dim, n_kv = shapes
    bits, peers = place()
    by, bx, bc, bz = (bits[a] for a in 'yxcz')
    shard = dim // 16
    third, mid = shard // 3, shard // 2
    fast = [(a, slice(i * third, (i + 1) * third)) for i, a in enumerate(COLORS)]
    slim = [(a, slice(i * mid, (i + 1) * mid)) for i, a in enumerate(('zxy', 'zyx'))]
    hq = dim // 2
    pieces = [(wi, slice(dim, dim + 2 * n_kv), fast), (wo, slice(0, dim), slim),
              (wi, slice(0, hq), slim), (wi, slice(hq, dim), slim)]

    loads = []

    def load(src, dst):
        c = pltpu.make_async_copy(src, dst, load_sem.at[len(loads)])
        c.start()
        loads.append(c)
        return len(loads) - 1

    mine = lambda ref, cols: ref.at[by, bx, bc, bz, :, cols]
    for g in range(n_kv // HEAD):
        hc = slice(g * HEAD, (g + 1) * HEAD)
        load(wk_hbm.at[:, hc], mine(wi, slice(dim + 2 * g * HEAD, dim + (2 * g + 1) * HEAD)))
        load(wv_hbm.at[:, hc], mine(wi, slice(dim + (2 * g + 1) * HEAD, dim + (2 * g + 2) * HEAD)))
    n_first = len(loads)
    l_o = load(wo_hbm, mine(wo, slice(0, dim)))
    l_q = load(wq_hbm, mine(wi, slice(0, dim)))
    l_x = load(x_hbm, x)
    l_dy = load(dy_hbm, dy)
    gbuf[by, bx, bc, bz] = gain_ref[...]
    meet(peers)

    def region(p, c, f, flip):
        ref, cols, colors = pieces[p]
        order, rws = colors[c]
        idx = []
        for a in 'yxcz':
            if a in order[:f]:
                idx.append(slice(None))
            elif a == order[f] and flip:
                idx.append(1 - bits[a])
            else:
                idx.append(bits[a])
        return ref.at[idx[0], idx[1], idx[2], idx[3], rws, cols]

    def ici(p, c, f):
        s = region(p, c, f, False)
        return pltpu.make_async_remote_copy(s, s, ici_send.at[p, c, f], ici_recv.at[p, c, f],
                                            device_id=peers[pieces[p][2][c][0][f]], device_id_type=MESH)

    def fwd(p, c, f):
        s = region(p, c, f, True)
        return pltpu.make_async_remote_copy(s, s, fwd_send.at[p, c, f], fwd_recv.at[p, c, f],
                                            device_id=peers['c'], device_id_type=MESH)

    def own(p):
        s = mine(pieces[p][0], pieces[p][1])
        return pltpu.make_async_remote_copy(s, s, own_send.at[p], own_recv.at[p],
                                            device_id=peers['c'], device_id_type=MESH)

    def begin(p):
        for c in range(len(pieces[p][2])):
            ici(p, c, 0).start()
        own(p).start()

    def advance(p, f):
        for c in range(len(pieces[p][2])):
            ici(p, c, f).wait()
            if f < 2:
                ici(p, c, f + 1).start()
            fwd(p, c, f).start()

    def settle(p):
        own(p).wait()
        for c in range(len(pieces[p][2])):
            for f in range(3):
                fwd(p, c, f).wait()

    def gain_copy(i):
        s = (gbuf.at[by, bx, bc, bz], gbuf.at[by, bx, :, bz], gbuf.at[by, bx], gbuf.at[by])[i]
        return pltpu.make_async_remote_copy(s, s, g_send.at[i], g_recv.at[i],
                                            device_id=peers['czxy'[i]], device_id_type=MESH)

    def kv_copy(i):
        return pltpu.make_async_remote_copy(kvo.at[i], kvx.at[i], kv_send.at[i], kv_recv.at[i],
                                            device_id=peers['z'], device_id_type=MESH)

    def px_copy():
        return pltpu.make_async_remote_copy(prow_ref, px, kv_send.at[n_seq], kv_recv.at[n_seq],
                                            device_id=peers['z'], device_id_type=MESH)

    gain_copy(0).start()
    for i in range(n_first):
        loads[i].wait()
    begin(0)
    px_copy().start()
    loads[l_o].wait()
    begin(1)
    loads[l_q].wait()
    begin(2)
    begin(3)
    gain_copy(0).wait()
    gain_copy(1).start()

    def tables(i, carry):
        rs = pl.ds(pl.multiple_of(i * rows, rows), rows)
        ang = pcol_ref[rs, :].astype(F32) * freq_ref[...]
        lane = lax.broadcasted_iota(jnp.int32, (rows, HEAD), 1)
        cos_ref[rs, :] = jnp.cos(ang)
        sn = jnp.sin(ang)
        sin_ref[rs, :] = jnp.where(lane < HEAD // 2, -sn, sn)
        return carry

    lax.fori_loop(0, n_seq // 2, tables, 0)
    gain_copy(1).wait()
    gain_copy(2).start()
    advance(0, 0)
    lax.fori_loop(n_seq // 2, n_seq, tables, 0)
    gain_copy(2).wait()
    gain_copy(3).start()
    advance(0, 1)
    gain_copy(3).wait()
    lane = lax.broadcasted_iota(jnp.int32, (8, HEAD), 1)
    for b in range(dim // HEAD):
        acc = jnp.zeros((8, HEAD), F32)
        for sh in range(16):
            lo = shard * sh - HEAD * b
            if lo >= HEAD or lo + shard <= 0:
                continue
            row = jnp.broadcast_to(gbuf[sh // 8, (sh // 4) % 2, (sh // 2) % 2, sh % 2], (8, HEAD))
            row = pltpu.roll(row, lo % HEAD, 1) if lo % HEAD else row
            acc = jnp.where((lane >= lo) & (lane < lo + shard), row, acc)
        grow[:, b * HEAD:(b + 1) * HEAD] = acc
    gain_out[...] = grow[0:1, :]
    loads[l_x].wait()

    def norm(i, carry):
        rs = pl.ds(pl.multiple_of(i * rows // 2, rows // 2), rows // 2)
        xf = x[rs, :].astype(F32)
        inv = lax.rsqrt(jnp.mean(xf * xf, axis=1, keepdims=True) + EPS)
        r[rs, :] = (xf * inv * grow[0:1, :]).astype(BF16)
        return carry

    lax.fori_loop(0, 2 * n_seq, norm, 0)
    r_out = pltpu.make_async_copy(r, r_hbm, out_sem.at[0])
    r_out.start()
    advance(0, 2)
    advance(1, 0)
    settle(0)

    def kv_proj(i, carry):
        rs = pl.ds(pl.multiple_of(i * rows, rows), rows)
        w = wi[:, :, :, :, :, dim:dim + 2 * n_kv].reshape(dim, 2 * n_kv)
        kv = dot(r[rs, :], w)
        for g in range(n_kv // HEAD):
            kc = slice(2 * g * HEAD, (2 * g + 1) * HEAD)
            vc = slice((2 * g + 1) * HEAD, (2 * g + 2) * HEAD)
            kvo[i, :, kc] = rope(kv[:, kc], cos_ref[rs, :], sin_ref[rs, :]).astype(BF16)
            kvo[i, :, vc] = kv[:, vc].astype(BF16)
        kv_copy(i).start()
        return carry

    lax.fori_loop(0, n_seq, kv_proj, 0)
    kvo_out = pltpu.make_async_copy(kvo, kvo_hbm, out_sem.at[1])
    kvo_out.start()
    advance(1, 1)
    advance(2, 0)
    advance(1, 2)
    settle(1)
    loads[l_dy].wait()

    def do_proj(i, carry):
        rs = pl.ds(pl.multiple_of(i * rows, rows), rows)
        do[rs, :] = dot(dy[rs, :], wo[...].reshape(dim, dim), NT).astype(BF16)
        return carry

    def q_proj(half):
        def body(i, carry):
            rs = pl.ds(pl.multiple_of(i * rows, rows), rows)
            res = dot(r[rs, :], wi[:, :, :, :, :, half * hq:(half + 1) * hq].reshape(dim, hq))
            for h in range(hq // HEAD):
                hc = slice(h * HEAD, (h + 1) * HEAD)
                q[rs, half * hq + h * HEAD:half * hq + (h + 1) * HEAD] = rope(
                    res[:, hc], cos_ref[rs, :], sin_ref[rs, :]).astype(BF16)
            return carry
        return body

    lax.fori_loop(0, n_seq // 2, do_proj, 0)
    advance(2, 1)
    advance(3, 0)
    lax.fori_loop(n_seq // 2, n_seq, do_proj, 0)
    do_out = pltpu.make_async_copy(do, do_hbm, out_sem.at[2])
    do_out.start()
    wf_out = pltpu.make_async_copy(wo, wf_hbm, out_sem.at[3])
    wf_out.start()
    advance(2, 2)
    advance(3, 1)
    settle(2)
    lax.fori_loop(0, n_seq, q_proj(0), 0)
    advance(3, 2)
    settle(3)
    wi_out = pltpu.make_async_copy(wi, wi_hbm, out_sem.at[4])
    wi_out.start()
    lax.fori_loop(0, n_seq, q_proj(1), 0)
    q_out = pltpu.make_async_copy(q, q_hbm, out_sem.at[5])
    q_out.start()
    px_copy().wait()
    px_out[...] = px[...]
    for i in range(n_seq):
        kv_copy(i).wait()
    kvx_out = pltpu.make_async_copy(kvx, kvx_hbm, out_sem.at[6])
    kvx_out.start()
    for c in (r_out, kvo_out, do_out, wf_out, wi_out, q_out, kvx_out):
        c.wait()


def gather_project(x, dy, wq, wk, wv, wo, gain, pos):
    tokens, dim = x.shape
    n_seq, rows = pos.shape
    n_kv = wk.shape[1]
    shard = dim // 16
    half = HEAD // 2
    freq = THETA ** (-jnp.arange(half, dtype=F32) / half)
    freq = jnp.concatenate([freq, freq])[None]
    gain = jnp.pad(gain, (0, HEAD - shard))[None]
    hbm = pl.BlockSpec(memory_space=pl.ANY)
    vm = pl.BlockSpec(memory_space=pltpu.VMEM)
    dma = pltpu.SemaphoreType.DMA
    sds = jax.ShapeDtypeStruct
    wshape = (2, 2, 2, 2, shard)
    return pl.pallas_call(
        functools.partial(gather_kernel, (n_seq, rows, dim, n_kv)),
        in_specs=[hbm] * 6 + [vm] * 4,
        out_specs=[hbm] * 7 + [vm] * 4,
        out_shape=[sds((tokens, dim), BF16), sds((tokens, dim), BF16), sds((tokens, dim), BF16),
                   sds((n_seq, rows, 2 * n_kv), BF16), sds((n_seq, rows, 2 * n_kv), BF16),
                   sds(wshape + (dim + 2 * n_kv,), BF16), sds(wshape + (dim,), BF16),
                   sds((tokens, HEAD), F32), sds((tokens, HEAD), F32), sds((1, dim), F32),
                   sds((n_seq, 1, rows), jnp.int32)],
        scratch_shapes=[pltpu.VMEM((tokens, dim), BF16)] * 5 + [
            pltpu.VMEM((n_seq, rows, 2 * n_kv), BF16),
            pltpu.VMEM((n_seq, rows, 2 * n_kv), BF16),
            pltpu.VMEM(wshape + (dim + 2 * n_kv,), BF16),
            pltpu.VMEM(wshape + (dim,), BF16),
            pltpu.VMEM((2, 2, 2, 2, 1, HEAD), F32),
            pltpu.VMEM((8, dim), F32),
            pltpu.VMEM((n_seq, 1, rows), jnp.int32),
            dma((2 * n_kv // HEAD + 4,)), dma((7,)), dma((4, 3, 3)), dma((4, 3, 3)), dma((4, 3, 3)), dma((4, 3, 3)),
            dma((4,)), dma((4,)), dma((4,)), dma((4,)), dma((n_seq + 1,)), dma((n_seq + 1,)),
        ],
        compiler_params=pltpu.CompilerParams(collective_id=2, has_side_effects=True, vmem_limit_bytes=60 * 2 ** 20),
        cost_estimate=pl.CostEstimate(flops=2 * tokens * dim * (2 * dim + 2 * n_kv), bytes_accessed=40 * 2 ** 20,
                                      transcendentals=0),
    )(x, dy, wq, wk, wv, wo, gain, pos.reshape(tokens, 1), pos[:, None, :], freq)


def solution(mesh):
    cp_size = mesh.shape['cp']

    def shard_fn(hidden, tok_pos, grad_out, norm_gain, w_query, w_key, w_value, w_out):
        n_seq, rows, dim = hidden.shape
        tokens = n_seq * rows
        n_q = w_query.shape[1]
        n_kv = w_key.shape[1]
        groups = n_kv // HEAD
        x16 = hidden.reshape(tokens, dim)
        dy = grad_out.reshape(tokens, dim)
        q, do, r, kv, kv_oth, w_in, w_o, cos2, sin2, gain, pos_oth = gather_project(
            x16, dy, w_query, w_key, w_value, w_out, norm_gain, tok_pos)
        w_in = w_in.reshape(dim, n_q + 2 * n_kv)
        w_o = w_o.reshape(n_q, dim)
        o, dq, dkv = attention(q, do, kv.reshape(tokens, -1), kv_oth.reshape(tokens, -1), tok_pos, pos_oth, cos2, sin2)
        x = x16.astype(F32)
        inv = lax.rsqrt(jnp.mean(x * x, axis=1, keepdims=True) + EPS)
        result = (x + dot(o, w_o)).astype(BF16)
        dkv = jnp.transpose(dkv, (0, 2, 1, 3, 4)).reshape(tokens, 2 * n_kv)
        d_in = jnp.concatenate([dq, dkv], axis=1)
        dr = dot(d_in, w_in, NT)
        xh = x * inv
        gp = jnp.sum(dr * xh, axis=0, keepdims=True)
        a = dr * gain
        gx = inv * (a - xh * jnp.mean(a * xh, axis=1, keepdims=True))
        grad_hidden = (dy.astype(F32) + gx).astype(BF16)
        g_in, g_wo, gg = wgrad(o, dy, r, dq, dkv, gp)
        shard = lax.axis_index('fsdp') * cp_size + lax.axis_index('cp')
        g_gain = lax.dynamic_slice(gg[0], (shard * norm_gain.shape[0],), norm_gain.shape)
        g_kv = g_in[:, n_q:].reshape(-1, groups, 2, HEAD)
        return (result.reshape(hidden.shape), grad_hidden.reshape(hidden.shape), g_in[:, :n_q],
                g_kv[:, :, 0].reshape(-1, n_kv), g_kv[:, :, 1].reshape(-1, n_kv), g_wo, g_gain)

    row = P('fsdp', 'cp', None)
    pos = P('fsdp', 'cp')
    w = P(AXES, None)
    g = P(AXES)
    return jax.shard_map(shard_fn, mesh=mesh, in_specs=(row, pos, row, g, w, w, w, w),
                         out_specs=(row, row, w, w, w, w, g), check_vma=False)
```

```python
import functools
import math

import jax
import jax.numpy as jnp
from jax import lax
from jax.experimental import pallas as pl
from jax.experimental.pallas import tpu as pltpu
from jax.sharding import PartitionSpec as P

HEAD = 128
THETA = 1000000.0
EPS = 1e-5
NEG = -1e30
SCALE = HEAD ** -0.5
LOG2E = math.log2(math.e)
AXES = ('fsdp', 'cp')
MESH = pl.DeviceIdType.MESH
F32 = jnp.float32
BF16 = jnp.bfloat16
NT = (((1,), (1,)), ((), ()))
TN = (((0,), (0,)), ((), ()))
NN = (((1,), (0,)), ((), ()))


def dot(a, b, dims=NN):
    return lax.dot_general(a, b, dims, preferred_element_type=F32)


def rope(v, cos2, sin2):
    return v * cos2 + pltpu.roll(v, HEAD // 2, 1) * sin2


def unrope(v, cos2, sin2):
    return v * cos2 - pltpu.roll(v, HEAD // 2, 1) * sin2


def attn_kernel(n_seq, rows, groups, gsize,
                q_ref, do_ref, kvo_ref, kvx_ref, pq_ref, pk_ref, px_ref, cos_ref, sin_ref,
                o_ref, dq_ref, dkv_ref,
                mask, p_s, ds_s, own, snd, rcv, send_sem, recv_sem):
    step = pl.program_id(0)
    n_steps = n_seq * groups
    seq = step // groups
    grp = step % groups
    cp = lax.axis_index('cp')
    peer = {'cp': 1 - cp}

    @pl.when(step == 0)
    def _():
        barrier = pltpu.get_barrier_semaphore()
        pl.semaphore_signal(barrier, inc=1, device_id=peer, device_id_type=MESH)
        pl.semaphore_wait(barrier, 1)

    @pl.when(grp == 0)
    def _():
        pq = pq_ref[...]
        mask[:, :rows] = jnp.where(pk_ref[0] <= pq, 0.0, NEG)
        mask[:, rows:] = jnp.where(px_ref[0] <= pq, 0.0, NEG)

    row0 = pl.multiple_of(seq * rows, rows)
    cos2 = cos_ref[pl.ds(row0, rows), :]
    sin2 = sin_ref[pl.ds(row0, rows), :]
    k = jnp.concatenate([kvo_ref[:, :HEAD], kvx_ref[:, :HEAD]], axis=0)
    v = jnp.concatenate([kvo_ref[:, HEAD:], kvx_ref[:, HEAD:]], axis=0)
    for h in range(gsize):
        cols = slice(h * HEAD, (h + 1) * HEAD)
        hrow = slice(h * rows, (h + 1) * rows)
        q = q_ref[:, cols]
        do = do_ref[:, cols]
        s = dot(q, k, NT) * (SCALE * LOG2E) + mask[...]
        m = jnp.max(s, axis=1, keepdims=True)
        e = jnp.exp2(s - m)
        l = jnp.sum(e, axis=1, keepdims=True)
        rl = 1.0 / l
        o = (dot(e.astype(BF16), v) * rl).astype(BF16)
        o_ref[:, cols] = o
        delta = jnp.sum(do.astype(F32) * o.astype(F32), axis=1, keepdims=True)
        p = e * rl
        p_s[hrow, :] = p.astype(BF16)
        ds = (p * (dot(do, v, NT) - delta)).astype(BF16)
        ds_s[hrow, :] = ds
        dq_ref[:, cols] = unrope(dot(ds, k) * SCALE, cos2, sin2).astype(BF16)
    do6 = jnp.concatenate([do_ref[:, h * HEAD:(h + 1) * HEAD] for h in range(gsize)], axis=0)
    q6 = jnp.concatenate([q_ref[:, h * HEAD:(h + 1) * HEAD] for h in range(gsize)], axis=0)
    dv = dot(p_s[...], do6, TN)
    dk = dot(ds_s[...], q6, TN) * SCALE
    own[step, :, :HEAD] = dk[:rows]
    own[step, :, HEAD:] = dv[:rows]
    snd[step, :, :HEAD] = dk[rows:]
    snd[step, :, HEAD:] = dv[rows:]

    def copy(i):
        return pltpu.make_async_remote_copy(snd.at[i], rcv.at[i], send_sem.at[i], recv_sem.at[i],
                                            device_id=peer, device_id_type=MESH)

    copy(step).start()

    @pl.when(step == n_steps - 1)
    def _():
        def fin(i, carry):
            copy(i).wait()
            r0 = pl.multiple_of((i // groups) * rows, rows)
            tot = own[i] + rcv[i]
            c2 = cos_ref[pl.ds(r0, rows), :]
            s2 = sin_ref[pl.ds(r0, rows), :]
            kc = pl.multiple_of((i % groups) * 2 * HEAD, HEAD)
            dkv_ref[pl.ds(r0, rows), pl.ds(kc, HEAD)] = unrope(tot[:, :HEAD], c2, s2).astype(BF16)
            dkv_ref[pl.ds(r0, rows), pl.ds(kc + HEAD, HEAD)] = tot[:, HEAD:].astype(BF16)
            return carry
        lax.fori_loop(0, n_steps, fin, 0)


def attention(q, do, kv_own, kv_oth, pos, pos_oth, cos2, sin2):
    n_seq, rows = pos.shape
    groups = kv_own.shape[1] // (2 * HEAD)
    gsize = q.shape[1] // HEAD // groups
    steps = n_seq * groups
    gcols = gsize * HEAD
    tokens = n_seq * rows
    blk = lambda c: pl.BlockSpec((rows, c), lambda i: (i // groups, i % groups))
    row3 = pl.BlockSpec((1, 1, rows), lambda i: (i // groups, 0, 0))
    full = lambda *s: pl.BlockSpec(s, lambda i: (0,) * len(s))
    o, dq, dkv = pl.pallas_call(
        functools.partial(attn_kernel, n_seq, rows, groups, gsize),
        grid=(steps,),
        in_specs=[blk(gcols), blk(gcols), blk(2 * HEAD), blk(2 * HEAD),
                  pl.BlockSpec((rows, 1), lambda i: (i // groups, 0)), row3, row3,
                  full(tokens, HEAD), full(tokens, HEAD)],
        out_specs=[blk(gcols), blk(gcols), full(tokens, groups * 2 * HEAD)],
        out_shape=[jax.ShapeDtypeStruct(q.shape, BF16), jax.ShapeDtypeStruct(q.shape, BF16),
                   jax.ShapeDtypeStruct((tokens, groups * 2 * HEAD), BF16)],
        scratch_shapes=[
            pltpu.VMEM((rows, 2 * rows), F32),
            pltpu.VMEM((gsize * rows, 2 * rows), BF16),
            pltpu.VMEM((gsize * rows, 2 * rows), BF16),
            pltpu.VMEM((steps, rows, 2 * HEAD), F32),
            pltpu.VMEM((steps, rows, 2 * HEAD), F32),
            pltpu.VMEM((steps, rows, 2 * HEAD), F32),
            pltpu.SemaphoreType.DMA((steps,)),
            pltpu.SemaphoreType.DMA((steps,)),
        ],
        compiler_params=pltpu.CompilerParams(
            collective_id=0, has_side_effects=True, dimension_semantics=('arbitrary',),
            vmem_limit_bytes=60 * 2 ** 20),
        cost_estimate=pl.CostEstimate(flops=2 * 7 * tokens * 2 * rows * gcols * groups,
                                      bytes_accessed=24 * 2 ** 20, transcendentals=0),
    )(q, do, kv_own, kv_oth, pos.reshape(tokens, 1), pos[:, None, :], pos_oth, cos2, sin2)
    return o, dq, dkv

COLORS = ('xyz', 'yzx', 'zxy')
SLIM = ('zxy', 'zyx')
BLOCK = 256


def place():
    f = lax.axis_index('fsdp')
    z = lax.axis_index('cp')
    bits = {'y': f // 4, 'x': (f // 2) % 2, 'c': f % 2, 'z': z}
    peers = {'y': {'fsdp': f + 4 - 8 * bits['y']}, 'x': {'fsdp': f + 2 - 4 * bits['x']},
             'c': {'fsdp': f + 1 - 2 * bits['c']}, 'z': {'cp': 1 - z}}
    return bits, peers


def meet(peers):
    barrier = pltpu.get_barrier_semaphore()
    for a in 'cxyz':
        pl.semaphore_signal(barrier, inc=1, device_id=peers[a], device_id_type=MESH)
    pl.semaphore_wait(barrier, 4)


def wgrad_kernel(shapes, o_hbm, dy_hbm, r_hbm, dq_hbm, dkv_hbm, x_hbm, wo_hbm, wa_hbm, wb_hbm, wkv_hbm, gain_ref,
                 gin_ref, gwo_ref, gg_ref, res_hbm, gh_hbm,
                 lhs, rhs, g, rcv_a, h, rcv1, rcv2, rcv3, gain_rcv, wo, wkv, xb, dyb, dqb, dkvb, outb,
                 load_sem, w_sem, blk_sem, out_sem, d2d_send, d2d_recv, ici_send, ici_recv, gain_send, gain_recv, credit):
    tokens, dim, width, sub = shapes
    bits, peers = place()
    core = bits['c']
    chunks = [(0, dy_hbm, j, gwo_ref, j) for j in range(dim // width)]
    chunks += [(1, dq_hbm, j, gin_ref, j) for j in range(dim // width)]
    chunks += [(1, dkv_hbm, 0, gin_ref, dim // width)]
    n = len(chunks)
    seg = dim // 4
    half = seg // 2

    def load_lhs(i):
        return pltpu.make_async_copy((o_hbm, r_hbm)[i], lhs.at[i], load_sem.at[i])

    def load_rhs(t):
        src, j = chunks[t][1], chunks[t][2]
        return pltpu.make_async_copy(src.at[:, pl.ds(j * width, width)], rhs.at[t % 2], load_sem.at[2 + t])

    load_lhs(0).start()
    load_rhs(0).start()
    load_lhs(1).start()
    load_rhs(1).start()
    hd = dim // 2
    w_loads = [pltpu.make_async_copy(a, b, w_sem.at[i]) for i, (a, b) in enumerate((
        (wo_hbm, wo), (wkv_hbm, wkv), (wa_hbm, lhs.at[0, :, pl.ds(0, hd)]), (wb_hbm, lhs.at[0, :, pl.ds(hd, hd)])))]
    w_loads[0].start()
    w_loads[1].start()
    n_blk = tokens // BLOCK

    def blk_loads(b, which):
        rs = pl.ds(pl.multiple_of(b * BLOCK, BLOCK), BLOCK)
        srcs = ((x_hbm, xb), (dy_hbm, dyb), (dq_hbm, dqb), (dkv_hbm, dkvb))
        return [pltpu.make_async_copy(srcs[k][0].at[rs, :], srcs[k][1].at[b % 2], blk_sem.at[k, b % 2])
                for k in which]

    def out_copy(dst, b):
        rs = pl.ds(pl.multiple_of(b * BLOCK, BLOCK), BLOCK)
        return pltpu.make_async_copy(outb.at[b % 2], dst.at[rs, :], out_sem.at[b % 2])

    def blocks(lo, hi, which, dst, body):
        def run(b, carry):
            for c in blk_loads(b, which):
                c.wait()

            @pl.when(b + 1 < n_blk)
            def _():
                for c in blk_loads(b + 1, which):
                    c.start()

            @pl.when(b >= 2)
            def _():
                out_copy(dst, b - 2).wait()

            outb[b % 2] = body(b)
            out_copy(dst, b).start()
            return carry
        lax.fori_loop(lo, hi, run, 0)

    def res_body(b):
        rs = pl.ds(pl.multiple_of(b * BLOCK, BLOCK), BLOCK)
        return (xb[b % 2].astype(F32) + dot(lhs[0, rs, :], wo[...])).astype(BF16)

    def dr_body(b):
        xf = xb[b % 2].astype(F32)
        inv = lax.rsqrt(jnp.mean(xf * xf, axis=1, keepdims=True) + EPS)
        xh = xf * inv
        dr = dot(dqb[b % 2], lhs[0], NT) + dot(dkvb[b % 2], wkv[...], NT)
        gg_ref[...] = gg_ref[...] + jnp.sum(dr * xh, axis=0, keepdims=True)
        a = dr * gain_ref[...]
        gx = inv * (a - xh * jnp.mean(a * xh, axis=1, keepdims=True))
        return (dyb[b % 2].astype(F32) + gx).astype(BF16)

    for c in blk_loads(0, (0,)):
        c.start()
    meet(peers)

    def d2d(t):
        return pltpu.make_async_remote_copy(g.at[t % 2, :, 1 - core], rcv_a.at[t % 2], d2d_send.at[t], d2d_recv.at[t],
                                            device_id=peers['c'], device_id_type=MESH)

    def ici(t, c, p):
        b1, b2, b3 = (bits[a] for a in COLORS[c])
        if p == 0:
            src, dst = h.at[t, c, pl.ds((1 - b1) * 4, 4)], rcv1.at[t, c]
        elif p == 1:
            src, dst = h.at[t, c, pl.ds(b1 * 4 + (1 - b2) * 2, 2)], rcv2.at[t, c]
        else:
            src, dst = h.at[t, c, pl.ds(b1 * 4 + b2 * 2 + (1 - b3), 1)], rcv3.at[t, c]
        return pltpu.make_async_remote_copy(src, dst, ici_send.at[t, c, p], ici_recv.at[t, c, p],
                                            device_id=peers[COLORS[c][p]], device_id_type=MESH)

    def compute(t):
        li = chunks[t][0]
        if t == 0 or chunks[t - 1][0] != li:
            load_lhs(li).wait()
        load_rhs(t).wait()

        def body(yx, carry):
            cols = pl.ds(pl.multiple_of(yx * seg, HEAD), seg)
            res = dot(lhs[li, :, cols], rhs[t % 2], TN)
            g[t % 2, yx, 0] = res[:half]
            g[t % 2, yx, 1] = res[half:]
            return carry
        lax.fori_loop(0, 4, body, 0)
        if t + 2 < n:
            load_rhs(t + 2).start()
        if t >= 2:
            pl.semaphore_wait(credit, 1)
        d2d(t).start()

    def fold(t):
        d2d(t).wait()
        for y in range(2):
            for x in range(2):
                for z in range(2):
                    at = {'y': y, 'x': x, 'z': z}
                    for c in range(3):
                        a1, a2, a3 = (at[a] for a in COLORS[c])
                        rows = slice(z * 3 * sub + c * sub, z * 3 * sub + (c + 1) * sub)
                        h[t, c, a1 * 4 + a2 * 2 + a3] = g[t % 2, y * 2 + x, core, rows] + rcv_a[t % 2, y * 2 + x, rows]
        for c in range(3):
            ici(t, c, 0).start()
        if t + 2 < n:
            pl.semaphore_signal(credit, inc=1, device_id=peers['c'], device_id_type=MESH)

    def reduce(t, p):
        for c in range(3):
            b1, b2, b3 = (bits[a] for a in COLORS[c])
            ici(t, c, p).wait()
            if p == 0:
                for j in range(4):
                    h[t, c, b1 * 4 + j] = h[t, c, b1 * 4 + j] + rcv1[t, c, j]
                ici(t, c, 1).start()
            elif p == 1:
                for j in range(2):
                    k = b1 * 4 + b2 * 2 + j
                    h[t, c, k] = h[t, c, k] + rcv2[t, c, j]
                ici(t, c, 2).start()
            else:
                out, j = chunks[t][3], chunks[t][4]
                k = b1 * 4 + b2 * 2 + b3
                out[c * sub:(c + 1) * sub, j * width:(j + 1) * width] = h[t, c, k] + rcv3[t, c, 0]

    gg_ref[...] = jnp.zeros_like(gg_ref)

    def gain_copy(i):
        return pltpu.make_async_remote_copy(gg_ref, gain_rcv.at[i], gain_send.at[i], gain_recv.at[i],
                                            device_id=peers['cxyz'[i]], device_id_type=MESH)

    def flush(dst):
        out_copy(dst, n_blk - 2).wait()
        out_copy(dst, n_blk - 1).wait()

    every = (0, 1, 2, 3)
    half_blk = n_blk // 3
    for i in range(n + 4):
        if i < n:
            compute(i)
        if 0 <= i - 1 < n:
            fold(i - 1)
        for p in range(3):
            if 0 <= i - 2 - p < n:
                reduce(i - 2 - p, p)
        if i < 3:
            if i == 0:
                w_loads[0].wait()
            blocks(i * half_blk, (i + 1) * half_blk, (0,), res_hbm, res_body)
            if i == 2:
                flush(res_hbm)
                for c in [*w_loads[2:], *blk_loads(0, every)]:
                    c.start()
        elif i < 6:
            if i == 3:
                for c in w_loads[1:]:
                    c.wait()
            blocks((i - 3) * half_blk, (i - 2) * half_blk, every, gh_hbm, dr_body)
            if i == 5:
                flush(gh_hbm)
                gain_copy(0).start()
        elif i < 10:
            gain_copy(i - 6).wait()
            gg_ref[...] = gg_ref[...] + gain_rcv[i - 6]
            if i < 9:
                gain_copy(i - 5).start()


def wgrad(o, dy, r, dq, dkv, x, w_o, w_a, w_b, w_kv, gain):
    tokens, dim = o.shape
    width = dkv.shape[1]
    shard = dim // 16
    sub = shard // 3
    n = 2 * (dim // width) + 1
    hbm = pl.BlockSpec(memory_space=pl.ANY)
    vm = pl.BlockSpec(memory_space=pltpu.VMEM)
    dma = pltpu.SemaphoreType.DMA
    return pl.pallas_call(
        functools.partial(wgrad_kernel, (tokens, dim, width, sub)),
        in_specs=[hbm] * 10 + [vm],
        out_specs=[vm] * 3 + [hbm] * 2,
        out_shape=[jax.ShapeDtypeStruct((shard, dim + width), F32), jax.ShapeDtypeStruct((shard, dim), F32),
                   jax.ShapeDtypeStruct((1, dim), F32)] + [jax.ShapeDtypeStruct((tokens, dim), BF16)] * 2,
        scratch_shapes=[
            pltpu.VMEM((2, tokens, dim), BF16),
            pltpu.VMEM((2, tokens, width), BF16),
            pltpu.VMEM((2, 4, 2, dim // 8, width), F32),
            pltpu.VMEM((2, 4, dim // 8, width), F32),
            pltpu.VMEM((n, 3, 8, sub, width), F32),
            pltpu.VMEM((n, 3, 4, sub, width), F32),
            pltpu.VMEM((n, 3, 2, sub, width), F32),
            pltpu.VMEM((n, 3, 1, sub, width), F32),
            pltpu.VMEM((4, 1, dim), F32),
            pltpu.VMEM((dim, dim), BF16),
            pltpu.VMEM((dim, width), BF16),
            pltpu.VMEM((2, BLOCK, dim), BF16),
            pltpu.VMEM((2, BLOCK, dim), BF16),
            pltpu.VMEM((2, BLOCK, dim), BF16),
            pltpu.VMEM((2, BLOCK, width), BF16),
            pltpu.VMEM((2, BLOCK, dim), BF16),
            dma((2 + n,)), dma((4,)), dma((4, 2)), dma((2,)), dma((n,)), dma((n,)), dma((n, 3, 3)), dma((n, 3, 3)), dma((4,)), dma((4,)),
            pltpu.SemaphoreType.REGULAR,
        ],
        compiler_params=pltpu.CompilerParams(collective_id=1, has_side_effects=True, vmem_limit_bytes=60 * 2 ** 20),
        cost_estimate=pl.CostEstimate(flops=2 * tokens * dim * (2 * dim + width), bytes_accessed=30 * 2 ** 20,
                                      transcendentals=0),
    )(o, dy, r, dq, dkv, x, w_o, w_a, w_b, w_kv, gain)


def gather_kernel(shapes, x_hbm, dy_hbm, wq_hbm, wk_hbm, wv_hbm, wo_hbm, gain_ref, pcol_ref, prow_ref, freq_ref,
                  q_hbm, do_hbm, r_hbm, kvo_hbm, kvx_hbm, wkv_hbm, wa_hbm, wb_hbm, wf_hbm, cos_ref, sin_ref, gain_out, px_out,
                  x, dy, r, q, do, kvo, kvx, wkv, wa, wb, wo, gbuf, grow, px,
                  load_sem, out_sem, ici_send, ici_recv, fwd_send, fwd_recv, own_send, own_recv,
                  g_send, g_recv, kv_send, kv_recv):
    n_seq, rows, dim, n_kv = shapes
    bits, peers = place()
    by, bx, bc, bz = (bits[a] for a in 'yxcz')
    shard = dim // 16
    third, mid = shard // 3, shard // len(SLIM)
    hq = dim // 2
    fast = COLORS
    slim = SLIM
    pieces = [(wkv, fast), (wo, slim), (wa, slim), (wb, slim)]

    loads = []

    def load(src, dst):
        c = pltpu.make_async_copy(src, dst, load_sem.at[len(loads)])
        c.start()
        loads.append(c)
        return len(loads) - 1

    mine = lambda ref: ref.at[by, bx, bc, bz]
    for c in range(3):
        for g in range(n_kv // HEAD):
            hc = slice(g * HEAD, (g + 1) * HEAD)
            rws = slice(c * third, (c + 1) * third)
            for j, w_hbm in enumerate((wk_hbm, wv_hbm)):
                oc = slice((2 * g + j) * HEAD, (2 * g + j + 1) * HEAD)
                load(w_hbm.at[rws, hc], wkv.at[by, bx, bc, bz, c, :, oc])
    n_first = len(loads)
    for c in range(len(SLIM)):
        rws = slice(c * mid, (c + 1) * mid)
        load(wo_hbm.at[rws, :], wo.at[by, bx, bc, bz, c])
        load(wq_hbm.at[rws, slice(0, hq)], wa.at[by, bx, bc, bz, c])
        load(wq_hbm.at[rws, slice(hq, dim)], wb.at[by, bx, bc, bz, c])
    n_all = len(loads)
    l_x = load(x_hbm, x)
    l_dy = load(dy_hbm, dy)
    gbuf[by, bx, bc, bz] = gain_ref[...]
    meet(peers)

    def region(p, c, f, flip):
        ref, order = pieces[p][0], pieces[p][1][c]
        idx = []
        for a in 'yxcz':
            if a in order[:f]:
                idx.append(slice(None))
            elif a == order[f] and flip:
                idx.append(1 - bits[a])
            else:
                idx.append(bits[a])
        return ref.at[idx[0], idx[1], idx[2], idx[3], c]

    def ici(p, c, f):
        s = region(p, c, f, False)
        return pltpu.make_async_remote_copy(s, s, ici_send.at[p, c, f], ici_recv.at[p, c, f],
                                            device_id=peers[pieces[p][1][c][f]], device_id_type=MESH)

    def fwd(p, c, f):
        s = region(p, c, f, True)
        return pltpu.make_async_remote_copy(s, s, fwd_send.at[p, c, f], fwd_recv.at[p, c, f],
                                            device_id=peers['c'], device_id_type=MESH)

    def own(p):
        s = mine(pieces[p][0])
        return pltpu.make_async_remote_copy(s, s, own_send.at[p], own_recv.at[p],
                                            device_id=peers['c'], device_id_type=MESH)

    def begin(p):
        for c in range(len(pieces[p][1])):
            ici(p, c, 0).start()
        own(p).start()

    def advance(p, f):
        for c in range(len(pieces[p][1])):
            ici(p, c, f).wait()
            if f < 2:
                ici(p, c, f + 1).start()
            fwd(p, c, f).start()

    def settle(p):
        own(p).wait()
        for c in range(len(pieces[p][1])):
            for f in range(3):
                fwd(p, c, f).wait()

    def gain_copy(i):
        s = (gbuf.at[by, bx, bc, bz], gbuf.at[by, bx, :, bz], gbuf.at[by, bx], gbuf.at[by])[i]
        return pltpu.make_async_remote_copy(s, s, g_send.at[i], g_recv.at[i],
                                            device_id=peers['czxy'[i]], device_id_type=MESH)

    def kv_copy(i):
        return pltpu.make_async_remote_copy(kvo.at[i], kvx.at[i], kv_send.at[i], kv_recv.at[i],
                                            device_id=peers['z'], device_id_type=MESH)

    def px_copy():
        return pltpu.make_async_remote_copy(prow_ref, px, kv_send.at[n_seq], kv_recv.at[n_seq],
                                            device_id=peers['z'], device_id_type=MESH)

    gain_copy(0).start()
    for i in range(n_first):
        loads[i].wait()
    begin(0)
    px_copy().start()
    for i in range(n_first, n_all):
        loads[i].wait()
    begin(1)
    begin(2)
    begin(3)
    gain_copy(0).wait()
    gain_copy(1).start()

    def tables(i, carry):
        rs = pl.ds(pl.multiple_of(i * rows, rows), rows)
        ang = pcol_ref[rs, :].astype(F32) * freq_ref[...]
        lane = lax.broadcasted_iota(jnp.int32, (rows, HEAD), 1)
        cos_ref[rs, :] = jnp.cos(ang)
        sn = jnp.sin(ang)
        sin_ref[rs, :] = jnp.where(lane < HEAD // 2, -sn, sn)
        return carry

    lax.fori_loop(0, n_seq // 2, tables, 0)
    gain_copy(1).wait()
    gain_copy(2).start()
    advance(0, 0)
    advance(1, 0)
    lax.fori_loop(n_seq // 2, n_seq, tables, 0)
    gain_copy(2).wait()
    gain_copy(3).start()
    advance(0, 1)
    advance(2, 0)
    gain_copy(3).wait()
    advance(3, 0)
    lane = lax.broadcasted_iota(jnp.int32, (8, HEAD), 1)
    for b in range(dim // HEAD):
        acc = jnp.zeros((8, HEAD), F32)
        for sh in range(16):
            lo = shard * sh - HEAD * b
            if lo >= HEAD or lo + shard <= 0:
                continue
            row = jnp.broadcast_to(gbuf[sh // 8, (sh // 4) % 2, (sh // 2) % 2, sh % 2], (8, HEAD))
            row = pltpu.roll(row, lo % HEAD, 1) if lo % HEAD else row
            acc = jnp.where((lane >= lo) & (lane < lo + shard), row, acc)
        grow[:, b * HEAD:(b + 1) * HEAD] = acc
    gain_out[...] = grow[0:1, :]
    loads[l_x].wait()

    def norm(i, carry):
        rs = pl.ds(pl.multiple_of(i * rows // 2, rows // 2), rows // 2)
        xf = x[rs, :].astype(F32)
        inv = lax.rsqrt(jnp.mean(xf * xf, axis=1, keepdims=True) + EPS)
        r[rs, :] = (xf * inv * grow[0:1, :]).astype(BF16)
        return carry

    lax.fori_loop(0, 2 * n_seq, norm, 0)
    r_out = pltpu.make_async_copy(r, r_hbm, out_sem.at[0])
    r_out.start()
    advance(0, 2)
    settle(0)

    def kv_proj(i, carry):
        rs = pl.ds(pl.multiple_of(i * rows, rows), rows)
        kv = dot(r[rs, :], wkv[...].reshape(dim, 2 * n_kv))
        for g in range(n_kv // HEAD):
            kc = slice(2 * g * HEAD, (2 * g + 1) * HEAD)
            vc = slice((2 * g + 1) * HEAD, (2 * g + 2) * HEAD)
            kvo[i, :, kc] = rope(kv[:, kc], cos_ref[rs, :], sin_ref[rs, :]).astype(BF16)
            kvo[i, :, vc] = kv[:, vc].astype(BF16)
        kv_copy(i).start()
        return carry

    lax.fori_loop(0, n_seq, kv_proj, 0)
    kvo_out = pltpu.make_async_copy(kvo, kvo_hbm, out_sem.at[1])
    kvo_out.start()
    advance(1, 1)
    advance(2, 1)
    advance(3, 1)
    advance(1, 2)
    settle(1)
    loads[l_dy].wait()

    def do_proj(i, carry):
        rs = pl.ds(pl.multiple_of(i * rows, rows), rows)
        do[rs, :] = dot(dy[rs, :], wo[...].reshape(dim, dim), NT).astype(BF16)
        return carry

    def q_proj(half):
        def body(i, carry):
            rs = pl.ds(pl.multiple_of(i * rows, rows), rows)
            res = dot(r[rs, :], (wa, wb)[half][...].reshape(dim, hq))
            for h in range(hq // HEAD):
                hc = slice(h * HEAD, (h + 1) * HEAD)
                q[rs, half * hq + h * HEAD:half * hq + (h + 1) * HEAD] = rope(
                    res[:, hc], cos_ref[rs, :], sin_ref[rs, :]).astype(BF16)
            return carry
        return body

    lax.fori_loop(0, n_seq // 2, do_proj, 0)
    advance(2, 2)
    lax.fori_loop(n_seq // 2, n_seq, do_proj, 0)
    advance(3, 2)
    do_out = pltpu.make_async_copy(do, do_hbm, out_sem.at[2])
    do_out.start()
    wf_out = pltpu.make_async_copy(wo, wf_hbm, out_sem.at[3])
    wf_out.start()
    settle(2)
    lax.fori_loop(0, n_seq, q_proj(0), 0)
    settle(3)
    wi_out = [pltpu.make_async_copy(v, o, out_sem.at[7 + i])
              for i, (v, o) in enumerate(((wkv, wkv_hbm), (wa, wa_hbm), (wb, wb_hbm)))]
    for c in wi_out:
        c.start()
    lax.fori_loop(0, n_seq, q_proj(1), 0)
    q_out = pltpu.make_async_copy(q, q_hbm, out_sem.at[5])
    q_out.start()
    px_copy().wait()
    px_out[...] = px[...]
    for i in range(n_seq):
        kv_copy(i).wait()
    kvx_out = pltpu.make_async_copy(kvx, kvx_hbm, out_sem.at[6])
    kvx_out.start()
    for c in (r_out, kvo_out, do_out, wf_out, q_out, kvx_out, *wi_out):
        c.wait()


def gather_project(x, dy, wq, wk, wv, wo, gain, pos):
    tokens, dim = x.shape
    n_seq, rows = pos.shape
    n_kv = wk.shape[1]
    shard = dim // 16
    half = HEAD // 2
    freq = THETA ** (-jnp.arange(half, dtype=F32) / half)
    freq = jnp.concatenate([freq, freq])[None]
    gain = jnp.pad(gain, (0, HEAD - shard))[None]
    hbm = pl.BlockSpec(memory_space=pl.ANY)
    vm = pl.BlockSpec(memory_space=pltpu.VMEM)
    dma = pltpu.SemaphoreType.DMA
    sds = jax.ShapeDtypeStruct
    wshapes = [(2, 2, 2, 2, 3, shard // 3, 2 * n_kv)] + [
        (2, 2, 2, 2, len(SLIM), shard // len(SLIM), c) for c in (dim // 2, dim // 2, dim)]
    return pl.pallas_call(
        functools.partial(gather_kernel, (n_seq, rows, dim, n_kv)),
        in_specs=[hbm] * 6 + [vm] * 4,
        out_specs=[hbm] * 9 + [vm] * 4,
        out_shape=[sds((tokens, dim), BF16), sds((tokens, dim), BF16), sds((tokens, dim), BF16),
                   sds((n_seq, rows, 2 * n_kv), BF16), sds((n_seq, rows, 2 * n_kv), BF16),
                   *[sds(w, BF16) for w in wshapes],
                   sds((tokens, HEAD), F32), sds((tokens, HEAD), F32), sds((1, dim), F32),
                   sds((n_seq, 1, rows), jnp.int32)],
        scratch_shapes=[pltpu.VMEM((tokens, dim), BF16)] * 5 + [
            pltpu.VMEM((n_seq, rows, 2 * n_kv), BF16),
            pltpu.VMEM((n_seq, rows, 2 * n_kv), BF16),
            *[pltpu.VMEM(w, BF16) for w in wshapes],
            pltpu.VMEM((2, 2, 2, 2, 1, HEAD), F32),
            pltpu.VMEM((8, dim), F32),
            pltpu.VMEM((n_seq, 1, rows), jnp.int32),
            dma((6 * n_kv // HEAD + 2 + 3 * len(SLIM),)), dma((10,)), dma((4, 3, 3)), dma((4, 3, 3)), dma((4, 3, 3)), dma((4, 3, 3)),
            dma((4,)), dma((4,)), dma((4,)), dma((4,)), dma((n_seq + 1,)), dma((n_seq + 1,)),
        ],
        compiler_params=pltpu.CompilerParams(collective_id=2, has_side_effects=True, vmem_limit_bytes=60 * 2 ** 20),
        cost_estimate=pl.CostEstimate(flops=2 * tokens * dim * (2 * dim + 2 * n_kv), bytes_accessed=40 * 2 ** 20,
                                      transcendentals=0),
    )(x, dy, wq, wk, wv, wo, gain, pos.reshape(tokens, 1), pos[:, None, :], freq)


def solution(mesh):
    cp_size = mesh.shape['cp']

    def shard_fn(hidden, tok_pos, grad_out, norm_gain, w_query, w_key, w_value, w_out):
        n_seq, rows, dim = hidden.shape
        tokens = n_seq * rows
        n_q = w_query.shape[1]
        n_kv = w_key.shape[1]
        groups = n_kv // HEAD
        x16 = hidden.reshape(tokens, dim)
        dy = grad_out.reshape(tokens, dim)
        q, do, r, kv, kv_oth, w_kv, w_a, w_b, w_o, cos2, sin2, gain, pos_oth = gather_project(
            x16, dy, w_query, w_key, w_value, w_out, norm_gain, tok_pos)
        w_a, w_b, w_kv, w_o = (w.reshape(dim, -1) for w in (w_a, w_b, w_kv, w_o))
        o, dq, dkv = attention(q, do, kv.reshape(tokens, -1), kv_oth.reshape(tokens, -1), tok_pos, pos_oth, cos2, sin2)
        g_in, g_wo, gg, result, grad_hidden = wgrad(o, dy, r, dq, dkv, x16, w_o, w_a, w_b, w_kv, gain)
        shard = lax.axis_index('fsdp') * cp_size + lax.axis_index('cp')
        g_gain = lax.dynamic_slice(gg[0], (shard * norm_gain.shape[0],), norm_gain.shape)
        g_kv = g_in[:, n_q:].reshape(-1, groups, 2, HEAD)
        return (result.reshape(hidden.shape), grad_hidden.reshape(hidden.shape), g_in[:, :n_q],
                g_kv[:, :, 0].reshape(-1, n_kv), g_kv[:, :, 1].reshape(-1, n_kv), g_wo, g_gain)

    row = P('fsdp', 'cp', None)
    pos = P('fsdp', 'cp')
    w = P(AXES, None)
    g = P(AXES)
    return jax.shard_map(shard_fn, mesh=mesh, in_specs=(row, pos, row, g, w, w, w, w),
                         out_specs=(row, row, w, w, w, w, g), check_vma=False)
```

```python
import functools
import math

import jax
import jax.numpy as jnp
import numpy as np
from jax import lax
from jax.experimental import pallas as pl
from jax.experimental.pallas import tpu as pltpu
from jax.sharding import PartitionSpec as P

HEAD = 128
THETA = 1000000.0
EPS = 1e-5
NEG = -1e30
SCALE = HEAD ** -0.5
LOG2E = math.log2(math.e)
AXES = ('fsdp', 'cp')
MESH = pl.DeviceIdType.MESH
F32 = jnp.float32
BF16 = jnp.bfloat16
NT = (((1,), (1,)), ((), ()))
TN = (((0,), (0,)), ((), ()))
NN = (((1,), (0,)), ((), ()))


def dot(a, b, dims=NN):
    return lax.dot_general(a, b, dims, preferred_element_type=F32)


def loop(lo, hi, body):
    def run(i, carry):
        body(i)
        return carry
    lax.fori_loop(lo, hi, run, None)


def span(i, size):
    return pl.ds(pl.multiple_of(i * size, size), size)


def lanes(i):
    return slice(i * HEAD, (i + 1) * HEAD)


def rope(v, cos2, sin2):
    return v * cos2 + pltpu.roll(v, HEAD // 2, 1) * sin2


def unrope(v, cos2, sin2):
    return v * cos2 - pltpu.roll(v, HEAD // 2, 1) * sin2


def attn_kernel(n_seq, rows, groups, gsize,
                q_ref, do_ref, kvo_ref, kvx_ref, pq_ref, pk_ref, px_ref, cos_ref, sin_ref,
                o_ref, dq_ref, dkv_ref,
                mask, p_s, ds_s, own, snd, rcv, send_sem, recv_sem):
    step = pl.program_id(0)
    n_steps = n_seq * groups
    seq = step // groups
    grp = step % groups
    cp = lax.axis_index('cp')
    peer = {'cp': 1 - cp}

    @pl.when(step == 0)
    def _():
        barrier = pltpu.get_barrier_semaphore()
        pl.semaphore_signal(barrier, inc=1, device_id=peer, device_id_type=MESH)
        pl.semaphore_wait(barrier, 1)

    @pl.when(grp == 0)
    def _():
        pq = pq_ref[...]
        for j, ref in enumerate((pk_ref, px_ref)):
            for b in range(rows // HEAD):
                key = ref[0, :, lanes(b)].astype(F32)
                mask[:, lanes(j * (rows // HEAD) + b)] = jnp.where(key <= pq, 0.0, NEG)

    row0 = pl.multiple_of(seq * rows, rows)
    cos2 = cos_ref[pl.ds(row0, rows), :]
    sin2 = sin_ref[pl.ds(row0, rows), :]
    k = jnp.concatenate([kvo_ref[:, :HEAD], kvx_ref[:, :HEAD]], axis=0)
    v = jnp.concatenate([kvo_ref[:, HEAD:], kvx_ref[:, HEAD:]], axis=0)
    for h in range(gsize):
        cols = lanes(h)
        hrow = slice(h * rows, (h + 1) * rows)
        q = q_ref[:, cols]
        do = do_ref[:, cols]
        s = dot(q, k, NT) * (SCALE * LOG2E) + mask[...]
        m = jnp.max(s, axis=1, keepdims=True)
        e = jnp.exp2(s - m)
        l = jnp.sum(e, axis=1, keepdims=True)
        rl = 1.0 / l
        o = (dot(e.astype(BF16), v) * rl).astype(BF16)
        o_ref[:, cols] = o
        delta = jnp.sum(do.astype(F32) * o.astype(F32), axis=1, keepdims=True)
        p = e * rl
        p_s[hrow, :] = p.astype(BF16)
        ds = (p * (dot(do, v, NT) - delta)).astype(BF16)
        ds_s[hrow, :] = ds
        dq_ref[:, cols] = unrope(dot(ds, k) * SCALE, cos2, sin2).astype(BF16)
    do6 = jnp.concatenate([do_ref[:, lanes(h)] for h in range(gsize)], axis=0)
    q6 = jnp.concatenate([q_ref[:, lanes(h)] for h in range(gsize)], axis=0)
    dv = dot(p_s[...], do6, TN)
    dk = dot(ds_s[...], q6, TN) * SCALE
    own[step, :, :HEAD] = dk[:rows]
    own[step, :, HEAD:] = dv[:rows]
    snd[step, :, :HEAD] = dk[rows:]
    snd[step, :, HEAD:] = dv[rows:]

    def copy(i):
        return pltpu.make_async_remote_copy(snd.at[i], rcv.at[i], send_sem.at[i], recv_sem.at[i],
                                            device_id=peer, device_id_type=MESH)

    copy(step).start()

    @pl.when(step == n_steps - 1)
    def _():
        def fin(i, carry):
            copy(i).wait()
            r0 = pl.multiple_of((i // groups) * rows, rows)
            tot = own[i] + rcv[i]
            c2 = cos_ref[pl.ds(r0, rows), :]
            s2 = sin_ref[pl.ds(r0, rows), :]
            kc = pl.multiple_of((i % groups) * 2 * HEAD, HEAD)
            dkv_ref[pl.ds(r0, rows), pl.ds(kc, HEAD)] = unrope(tot[:, :HEAD], c2, s2).astype(BF16)
            dkv_ref[pl.ds(r0, rows), pl.ds(kc + HEAD, HEAD)] = tot[:, HEAD:].astype(BF16)
            return carry
        lax.fori_loop(0, n_steps, fin, 0)


def attention(q, do, kv_own, kv_oth, pos_col, pos, pos_oth, cos2, sin2):
    n_seq, _, rows = pos.shape
    groups = kv_own.shape[1] // (2 * HEAD)
    gsize = q.shape[1] // HEAD // groups
    steps = n_seq * groups
    gcols = gsize * HEAD
    tokens = n_seq * rows
    blk = lambda c: pl.BlockSpec((rows, c), lambda i: (i // groups, i % groups))
    row3 = pl.BlockSpec((1, 1, rows), lambda i: (i // groups, 0, 0))
    full = lambda *s: pl.BlockSpec(s, lambda i: (0,) * len(s))
    o, dq, dkv = pl.pallas_call(
        functools.partial(attn_kernel, n_seq, rows, groups, gsize),
        grid=(steps,),
        in_specs=[blk(gcols), blk(gcols), blk(2 * HEAD), blk(2 * HEAD),
                  pl.BlockSpec((rows, HEAD), lambda i: (i // groups, 0)), row3, row3,
                  full(tokens, HEAD), full(tokens, HEAD)],
        out_specs=[blk(gcols), blk(gcols), full(tokens, groups * 2 * HEAD)],
        out_shape=[jax.ShapeDtypeStruct(q.shape, BF16), jax.ShapeDtypeStruct(q.shape, BF16),
                   jax.ShapeDtypeStruct((tokens, groups * 2 * HEAD), BF16)],
        scratch_shapes=[
            pltpu.VMEM((rows, 2 * rows), F32),
            pltpu.VMEM((gsize * rows, 2 * rows), BF16),
            pltpu.VMEM((gsize * rows, 2 * rows), BF16),
            pltpu.VMEM((steps, rows, 2 * HEAD), F32),
            pltpu.VMEM((steps, rows, 2 * HEAD), F32),
            pltpu.VMEM((steps, rows, 2 * HEAD), F32),
            pltpu.SemaphoreType.DMA((steps,)),
            pltpu.SemaphoreType.DMA((steps,)),
        ],
        compiler_params=pltpu.CompilerParams(
            collective_id=0, has_side_effects=True, dimension_semantics=('arbitrary',),
            vmem_limit_bytes=60 * 2 ** 20),
        cost_estimate=pl.CostEstimate(flops=2 * 7 * tokens * 2 * rows * gcols * groups,
                                      bytes_accessed=24 * 2 ** 20, transcendentals=0),
    )(q, do, kv_own, kv_oth, pos_col, pos, pos_oth, cos2, sin2)
    return o, dq, dkv

COLORS = ('xyz', 'yzx', 'zxy')
SLIM = ('zxy', 'zyx')
BLOCK = 256


def place():
    f = lax.axis_index('fsdp')
    z = lax.axis_index('cp')
    bits = {'y': f // 4, 'x': (f // 2) % 2, 'c': f % 2, 'z': z}
    peers = {'y': {'fsdp': f + 4 - 8 * bits['y']}, 'x': {'fsdp': f + 2 - 4 * bits['x']},
             'c': {'fsdp': f + 1 - 2 * bits['c']}, 'z': {'cp': 1 - z}}
    return bits, peers


def meet(peers):
    barrier = pltpu.get_barrier_semaphore()
    for a in 'cxyz':
        pl.semaphore_signal(barrier, inc=1, device_id=peers[a], device_id_type=MESH)
    pl.semaphore_wait(barrier, 4)


def chunk_list(dim, width):
    half = width // 2
    out = [('o', 0, half), ('o', half, half)]
    out += [('o', c, width) for c in range(width, dim, width)]
    out += [('q', c, width) for c in range(0, dim, width)]
    return out + [('kv', 0, half), ('kv', half, half)]


def wgrad_kernel(shapes, o_hbm, dy_hbm, r_hbm, dq_hbm, dkv_hbm, x_hbm, wo_hbm, wa_hbm, wb_hbm, wkv_hbm, gain_ref,
                 gwq_ref, gwk_ref, gwv_ref, gwo_ref, gg_ref, res_hbm, gh_hbm,
                 lhs, rhs, g, rcv_a, gain_rcv, wo, wkv, xb, dyb, dqb, dkvb, outb,
                 load_sem, w_sem, blk_sem, out_sem, *rest):
    tokens, dim, width, sub = shapes
    bits, peers = place()
    core = bits['c']
    chunks = chunk_list(dim, width)
    n = len(chunks)
    h, rcv = rest[:n], [rest[n + t * 3:n + t * 3 + 3] for t in range(n)]
    d2d_send, d2d_recv, ici_send, ici_recv, gain_send, gain_recv, credit = rest[4 * n:]
    seg = dim // 4
    half = seg // 2

    def load_lhs(i):
        return pltpu.make_async_copy((o_hbm, r_hbm)[i], lhs.at[i], load_sem.at[i])

    def load_rhs(t):
        kind, col, w = chunks[t]
        src = {'o': dy_hbm, 'q': dq_hbm, 'kv': dkv_hbm}[kind]
        return pltpu.make_async_copy(src.at[:, pl.ds(col, w)], rhs.at[t % 2, :, pl.ds(0, w)], load_sem.at[2 + t])

    load_lhs(0).start()
    load_rhs(0).start()
    load_lhs(1).start()
    load_rhs(1).start()
    hd = dim // 2
    w_loads = [pltpu.make_async_copy(a, b, w_sem.at[i]) for i, (a, b) in enumerate((
        (wo_hbm, wo), (wkv_hbm, wkv), (wa_hbm, lhs.at[0, :, pl.ds(0, hd)]), (wb_hbm, lhs.at[0, :, pl.ds(hd, hd)])))]
    w_loads[0].start()
    w_loads[1].start()
    n_blk = tokens // BLOCK

    def blk_loads(b, which):
        rs = pl.ds(pl.multiple_of(b * BLOCK, BLOCK), BLOCK)
        srcs = ((x_hbm, xb), (dy_hbm, dyb), (dq_hbm, dqb), (dkv_hbm, dkvb))
        return [pltpu.make_async_copy(srcs[k][0].at[rs, :], srcs[k][1].at[b % 2], blk_sem.at[k, b % 2])
                for k in which]

    def out_copy(dst, b):
        rs = pl.ds(pl.multiple_of(b * BLOCK, BLOCK), BLOCK)
        return pltpu.make_async_copy(outb.at[b % 2], dst.at[rs, :], out_sem.at[b % 2])

    def blocks(lo, hi, which, dst, body):
        def run(b, carry):
            for c in blk_loads(b, which):
                c.wait()

            @pl.when(b + 1 < n_blk)
            def _():
                for c in blk_loads(b + 1, which):
                    c.start()

            @pl.when(b >= 2)
            def _():
                out_copy(dst, b - 2).wait()

            outb[b % 2] = body(b)
            out_copy(dst, b).start()
            return carry
        lax.fori_loop(lo, hi, run, 0)

    def res_body(b):
        rs = pl.ds(pl.multiple_of(b * BLOCK, BLOCK), BLOCK)
        return (xb[b % 2].astype(F32) + dot(lhs[0, rs, :], wo[...])).astype(BF16)

    def dr_body(b):
        xf = xb[b % 2].astype(F32)
        inv = lax.rsqrt(jnp.mean(xf * xf, axis=1, keepdims=True) + EPS)
        xh = xf * inv
        dr = dot(dqb[b % 2], lhs[0], NT) + dot(dkvb[b % 2], wkv[...], NT)
        gg_ref[...] = gg_ref[...] + jnp.sum(dr * xh, axis=0, keepdims=True)
        a = dr * gain_ref[...]
        gx = inv * (a - xh * jnp.mean(a * xh, axis=1, keepdims=True))
        return (dyb[b % 2].astype(F32) + gx).astype(BF16)

    for c in blk_loads(0, (0,)):
        c.start()
    meet(peers)

    def d2d(t):
        w = pl.ds(0, chunks[t][2])
        return pltpu.make_async_remote_copy(g.at[t % 2, :, 1 - core, :, w], rcv_a.at[t % 2, :, :, w], d2d_send.at[t], d2d_recv.at[t],
                                            device_id=peers['c'], device_id_type=MESH)

    def ici(t, c, p):
        b1, b2, b3 = (bits[a] for a in COLORS[c])
        if p == 0:
            src = h[t].at[c, pl.ds((1 - b1) * 4, 4)]
        elif p == 1:
            src = h[t].at[c, pl.ds(b1 * 4 + (1 - b2) * 2, 2)]
        else:
            src = h[t].at[c, pl.ds(b1 * 4 + b2 * 2 + (1 - b3), 1)]
        return pltpu.make_async_remote_copy(src, rcv[t][p].at[c], ici_send.at[t, c, p], ici_recv.at[t, c, p],
                                            device_id=peers[COLORS[c][p]], device_id_type=MESH)

    def compute(t):
        kind, _, w = chunks[t]
        li = int(kind != 'o')
        if t == 0 or (li and chunks[t - 1][0] == 'o'):
            load_lhs(li).wait()
        load_rhs(t).wait()

        def body(yx):
            res = dot(lhs[li, :, span(yx, seg)], rhs[t % 2, :, :w], TN)
            g[t % 2, yx, 0, :, :w] = res[:half]
            g[t % 2, yx, 1, :, :w] = res[half:]
        loop(0, 4, body)
        if t + 2 < n:
            load_rhs(t + 2).start()
        if t >= 2:
            pl.semaphore_wait(credit, 1)
        d2d(t).start()

    def fold(t):
        w = chunks[t][2]
        d2d(t).wait()
        for y in range(2):
            for x in range(2):
                for z in range(2):
                    at = {'y': y, 'x': x, 'z': z}
                    for c in range(3):
                        a1, a2, a3 = (at[a] for a in COLORS[c])
                        rows = slice(z * 3 * sub + c * sub, z * 3 * sub + (c + 1) * sub)
                        h[t][c, a1 * 4 + a2 * 2 + a3] = g[t % 2, y * 2 + x, core, rows, :w] + rcv_a[t % 2, y * 2 + x, rows, :w]
        for c in range(3):
            ici(t, c, 0).start()
        if t + 2 < n:
            pl.semaphore_signal(credit, inc=1, device_id=peers['c'], device_id_type=MESH)

    def reduce(t, p):
        for c in range(3):
            b1, b2, b3 = (bits[a] for a in COLORS[c])
            ici(t, c, p).wait()
            k = (0, b1 * 4, b1 * 4 + b2 * 2, b1 * 4 + b2 * 2 + b3)[p + 1]
            if p < 2:
                for j in range(4 >> p):
                    h[t][c, k + j] = h[t][c, k + j] + rcv[t][p][c, j]
                ici(t, c, p + 1).start()
                continue
            kind, col, w = chunks[t]
            rws = slice(c * sub, (c + 1) * sub)
            tot = h[t][c, k] + rcv[t][p][c, 0]
            if kind == 'kv':
                for j in range(w // HEAD):
                    b = col // HEAD + j
                    (gwk_ref, gwv_ref)[b % 2][rws, lanes(b // 2)] = tot[:, lanes(j)]
            else:
                (gwo_ref if kind == 'o' else gwq_ref)[rws, col:col + w] = tot

    gg_ref[...] = jnp.zeros_like(gg_ref)

    def gain_copy(i):
        return pltpu.make_async_remote_copy(gg_ref, gain_rcv.at[i], gain_send.at[i], gain_recv.at[i],
                                            device_id=peers['cxyz'[i]], device_id_type=MESH)

    def flush(dst):
        out_copy(dst, n_blk - 2).wait()
        out_copy(dst, n_blk - 1).wait()

    every = (0, 1, 2, 3)
    third, fill = n_blk // 3, n_blk // 2
    assert [c[0] for c in chunks].count('o') == 4
    for i in range(n + 4):
        if i < n:
            compute(i)
        if 0 <= i - 1 < n:
            fold(i - 1)
        for p in range(3):
            if 0 <= i - 2 - p < n:
                reduce(i - 2 - p, p)
        if 2 <= i < 4:
            if i == 2:
                w_loads[0].wait()
            blocks((i - 2) * fill, (i - 1) * fill, (0,), res_hbm, res_body)
            if i == 3:
                flush(res_hbm)
                for c in [*w_loads[2:], *blk_loads(0, every)]:
                    c.start()
        elif 4 <= i < 7:
            if i == 4:
                for c in w_loads[1:]:
                    c.wait()
            blocks((i - 4) * third, (i - 3) * third, every, gh_hbm, dr_body)
            if i == 6:
                flush(gh_hbm)
                gain_copy(0).start()
        elif 7 <= i < 11:
            gain_copy(i - 7).wait()
            gg_ref[...] = gg_ref[...] + gain_rcv[i - 7]
            if i < 10:
                gain_copy(i - 6).start()


def wgrad(o, dy, r, dq, dkv, x, w_o, w_a, w_b, w_kv, gain):
    tokens, dim = o.shape
    width = dkv.shape[1]
    shard = dim // 16
    sub = shard // 3
    chunks = chunk_list(dim, width)
    n = len(chunks)
    hbm = pl.BlockSpec(memory_space=pl.ANY)
    vm = pl.BlockSpec(memory_space=pltpu.VMEM)
    dma = pltpu.SemaphoreType.DMA
    return pl.pallas_call(
        functools.partial(wgrad_kernel, (tokens, dim, width, sub)),
        in_specs=[hbm] * 10 + [vm],
        out_specs=[vm] * 5 + [hbm] * 2,
        out_shape=[jax.ShapeDtypeStruct(a, F32) for a in (
            (shard, dim), (shard, width // 2), (shard, width // 2), (shard, dim), (1, dim))] + [jax.ShapeDtypeStruct((tokens, dim), BF16)] * 2,
        scratch_shapes=[
            pltpu.VMEM((2, tokens, dim), BF16),
            pltpu.VMEM((2, tokens, width), BF16),
            pltpu.VMEM((2, 4, 2, dim // 8, width), F32),
            pltpu.VMEM((2, 4, dim // 8, width), F32),
            pltpu.VMEM((4, 1, dim), F32),
            pltpu.VMEM((dim, dim), BF16),
            pltpu.VMEM((dim, width), BF16),
            *[pltpu.VMEM((2, BLOCK, c), BF16) for c in (dim, dim, dim, width, dim)],
            dma((2 + n,)), dma((4,)), dma((4, 2)), dma((2,)),
            *[pltpu.VMEM((3, 8, sub, c[2]), F32) for c in chunks],
            *[pltpu.VMEM((3, k, sub, c[2]), F32) for c in chunks for k in (4, 2, 1)],
            *[dma((n,))] * 2, *[dma((n, 3, 3))] * 2, *[dma((4,))] * 2,
            pltpu.SemaphoreType.REGULAR,
        ],
        compiler_params=pltpu.CompilerParams(collective_id=1, has_side_effects=True, vmem_limit_bytes=60 * 2 ** 20),
        cost_estimate=pl.CostEstimate(flops=2 * tokens * dim * (2 * dim + width), bytes_accessed=30 * 2 ** 20,
                                      transcendentals=0),
    )(o, dy, r, dq, dkv, x, w_o, w_a, w_b, w_kv, gain)


def gather_kernel(shapes, x_hbm, dy_hbm, wq_hbm, wk_hbm, wv_hbm, wo_hbm, gain_ref, pos_ref, freq_ref,
                  q_hbm, do_hbm, r_hbm, kvo_hbm, kvx_hbm, wkv_hbm, wa_hbm, wb_hbm, wf_hbm, cos_ref, sin_ref, gain_out, pcol_out, pos_out, px_out,
                  x, dy, r, q, do, kvo, kvx, wkv, wa, wb, wo, gbuf, grow, px,
                  load_sem, out_sem, ici_send, ici_recv, fwd_send, fwd_recv, own_send, own_recv,
                  g_send, g_recv, kv_send, kv_recv):
    n_seq, rows, dim, n_kv = shapes
    bits, peers = place()
    by, bx, bc, bz = (bits[a] for a in 'yxcz')
    shard = dim // 16
    third, mid = shard // 3, shard // len(SLIM)
    hq = dim // 2
    fast = COLORS
    slim = SLIM
    pieces = [(wkv, fast), (wo, fast), (wa, slim), (wb, slim)]

    loads = []

    def load(src, dst):
        c = pltpu.make_async_copy(src, dst, load_sem.at[len(loads)])
        c.start()
        loads.append(c)
        return len(loads) - 1

    mine = lambda ref: ref.at[by, bx, bc, bz]
    for c in range(3):
        for g in range(n_kv // HEAD):
            hc = slice(g * HEAD, (g + 1) * HEAD)
            rws = slice(c * third, (c + 1) * third)
            for j, w_hbm in enumerate((wk_hbm, wv_hbm)):
                oc = slice((2 * g + j) * HEAD, (2 * g + j + 1) * HEAD)
                load(w_hbm.at[rws, hc], wkv.at[by, bx, bc, bz, c, :, oc])
    n_first = len(loads)
    for c in range(3):
        load(wo_hbm.at[c * third:(c + 1) * third, :], wo.at[by, bx, bc, bz, c])
    for c in range(len(SLIM)):
        rws = slice(c * mid, (c + 1) * mid)
        load(wq_hbm.at[rws, :hq], wa.at[by, bx, bc, bz, c])
        load(wq_hbm.at[rws, hq:], wb.at[by, bx, bc, bz, c])
    n_all = len(loads)
    l_x = load(x_hbm, x)
    l_dy = load(dy_hbm, dy)
    gbuf[by, bx, bc, bz] = jnp.zeros((1, HEAD), F32)
    gbuf[by, bx, bc, bz, :, :shard] = gain_ref[...]
    meet(peers)

    def region(p, c, f, flip):
        ref, order = pieces[p][0], pieces[p][1][c]
        idx = []
        for a in 'yxcz':
            if a in order[:f]:
                idx.append(slice(None))
            elif a == order[f] and flip:
                idx.append(1 - bits[a])
            else:
                idx.append(bits[a])
        return ref.at[idx[0], idx[1], idx[2], idx[3], c]

    def ici(p, c, f):
        s = region(p, c, f, False)
        return pltpu.make_async_remote_copy(s, s, ici_send.at[p, c, f], ici_recv.at[p, c, f],
                                            device_id=peers[pieces[p][1][c][f]], device_id_type=MESH)

    def fwd(p, c, f):
        s = region(p, c, f, True)
        return pltpu.make_async_remote_copy(s, s, fwd_send.at[p, c, f], fwd_recv.at[p, c, f],
                                            device_id=peers['c'], device_id_type=MESH)

    def own(p):
        s = mine(pieces[p][0])
        return pltpu.make_async_remote_copy(s, s, own_send.at[p], own_recv.at[p],
                                            device_id=peers['c'], device_id_type=MESH)

    def begin(p):
        for c in range(len(pieces[p][1])):
            ici(p, c, 0).start()
        own(p).start()

    def advance(p, f):
        for c in range(len(pieces[p][1])):
            ici(p, c, f).wait()
            if f < 2:
                ici(p, c, f + 1).start()
            fwd(p, c, f).start()

    def settle(p):
        own(p).wait()
        for c in range(len(pieces[p][1])):
            for f in range(3):
                fwd(p, c, f).wait()

    def gain_copy(i):
        s = (gbuf.at[by, bx, bc, bz], gbuf.at[by, bx, :, bz], gbuf.at[by, bx], gbuf.at[by])[i]
        return pltpu.make_async_remote_copy(s, s, g_send.at[i], g_recv.at[i],
                                            device_id=peers['czxy'[i]], device_id_type=MESH)

    def kv_copy(i):
        return pltpu.make_async_remote_copy(kvo.at[i], kvx.at[i], kv_send.at[i], kv_recv.at[i],
                                            device_id=peers['z'], device_id_type=MESH)

    def px_copy():
        return pltpu.make_async_remote_copy(pos_ref, px, kv_send.at[n_seq], kv_recv.at[n_seq],
                                            device_id=peers['z'], device_id_type=MESH)

    gain_copy(0).start()
    for i in range(n_first):
        loads[i].wait()
    begin(0)
    px_copy().start()
    for i in range(n_first, n_all):
        loads[i].wait()
    for p in (1, 2, 3):
        begin(p)
    gain_copy(0).wait()
    gain_copy(1).start()

    def tables(i):
        rs = span(i, rows)
        row = pos_ref[pl.ds(i, 1), :]
        pos_out[i] = row
        col = jnp.transpose(jnp.broadcast_to(row.astype(F32), (HEAD, rows)))
        pcol_out[rs, :] = col
        ang = col * freq_ref[...]
        lane = lax.broadcasted_iota(jnp.int32, (rows, HEAD), 1)
        cos_ref[rs, :] = jnp.cos(ang)
        sn = jnp.sin(ang)
        sin_ref[rs, :] = jnp.where(lane < HEAD // 2, -sn, sn)

    mid_seq = n_seq // 2
    loop(0, mid_seq, tables)
    gain_copy(1).wait()
    gain_copy(2).start()
    advance(0, 0)
    advance(1, 0)
    loop(mid_seq, n_seq, tables)
    gain_copy(2).wait()
    gain_copy(3).start()
    advance(0, 1)
    advance(1, 1)
    gain_copy(3).wait()
    advance(2, 0)
    lane = lax.broadcasted_iota(jnp.int32, (8, HEAD), 1)
    for b in range(dim // HEAD):
        acc = jnp.zeros((8, HEAD), F32)
        for sh in range(16):
            lo = shard * sh - HEAD * b
            if lo >= HEAD or lo + shard <= 0:
                continue
            row = jnp.broadcast_to(gbuf[sh // 8, (sh // 4) % 2, (sh // 2) % 2, sh % 2], (8, HEAD))
            row = pltpu.roll(row, lo % HEAD, 1) if lo % HEAD else row
            acc = jnp.where((lane >= lo) & (lane < lo + shard), row, acc)
        grow[:, b * HEAD:(b + 1) * HEAD] = acc
    gain_out[...] = grow[0:1, :]
    loads[l_x].wait()

    def norm(i):
        rs = span(i, rows // 2)
        xf = x[rs, :].astype(F32)
        inv = lax.rsqrt(jnp.mean(xf * xf, axis=1, keepdims=True) + EPS)
        r[rs, :] = (xf * inv * grow[0:1, :]).astype(BF16)

    loop(0, 2 * n_seq, norm)
    r_out = pltpu.make_async_copy(r, r_hbm, out_sem.at[0])
    r_out.start()
    advance(0, 2)
    advance(3, 0)
    settle(0)
    wkv_out = pltpu.make_async_copy(wkv, wkv_hbm, out_sem.at[4])
    wkv_out.start()

    def kv_proj(i):
        rs = span(i, rows)
        kv = dot(r[rs, :], wkv[...].reshape(dim, 2 * n_kv))
        for g in range(0, 2 * n_kv // HEAD, 2):
            kvo[i, :, lanes(g)] = rope(kv[:, lanes(g)], cos_ref[rs, :], sin_ref[rs, :]).astype(BF16)
            kvo[i, :, lanes(g + 1)] = kv[:, lanes(g + 1)].astype(BF16)
        kv_copy(i).start()

    loop(0, mid_seq, kv_proj)
    advance(1, 2)
    loop(mid_seq, n_seq, kv_proj)
    kvo_out = pltpu.make_async_copy(kvo, kvo_hbm, out_sem.at[1])
    kvo_out.start()
    advance(2, 1)
    settle(1)
    wf_out = pltpu.make_async_copy(wo, wf_hbm, out_sem.at[3])
    wf_out.start()
    loads[l_dy].wait()

    def do_proj(i):
        rs = span(i, rows)
        do[rs, :] = dot(dy[rs, :], wo[...].reshape(dim, dim), NT).astype(BF16)

    def q_proj(half):
        def body(i):
            rs = span(i, rows)
            res = dot(r[rs, :], (wa, wb)[half][...].reshape(dim, hq))
            for h in range(hq // HEAD):
                q[rs, lanes(half * (hq // HEAD) + h)] = rope(res[:, lanes(h)], cos_ref[rs, :], sin_ref[rs, :]).astype(BF16)
        return body

    def q_out(half):
        hc = slice(half * hq, (half + 1) * hq)
        return pltpu.make_async_copy(q.at[:, hc], q_hbm.at[:, hc], out_sem.at[7 + half])

    loop(0, mid_seq, do_proj)
    advance(3, 1)
    advance(2, 2)
    loop(mid_seq, n_seq, do_proj)
    do_out = pltpu.make_async_copy(do, do_hbm, out_sem.at[2])
    do_out.start()
    settle(2)
    wa_out = pltpu.make_async_copy(wa, wa_hbm, out_sem.at[5])
    wa_out.start()
    loop(0, n_seq, q_proj(0))
    q_out(0).start()
    advance(3, 2)
    settle(3)
    wb_out = pltpu.make_async_copy(wb, wb_hbm, out_sem.at[9])
    wb_out.start()
    loop(0, n_seq, q_proj(1))
    q_out(1).start()
    px_copy().wait()
    for i in range(n_seq):
        px_out[i] = px[i:i + 1, :]
        kv_copy(i).wait()
    kvx_out = pltpu.make_async_copy(kvx, kvx_hbm, out_sem.at[6])
    kvx_out.start()
    for c in (r_out, kvo_out, do_out, wf_out, wkv_out, wa_out, wb_out, q_out(0), q_out(1), kvx_out):
        c.wait()


def gather_project(x, dy, wq, wk, wv, wo, gain, pos):
    tokens, dim = x.shape
    n_seq, rows = pos.shape
    n_kv = wk.shape[1]
    shard = dim // 16
    half = HEAD // 2
    freq = np.float32(THETA) ** (-np.arange(half, dtype=np.float32) / half)
    freq = jnp.asarray(np.tile(freq, 2)[None])
    hbm = pl.BlockSpec(memory_space=pl.ANY)
    vm = pl.BlockSpec(memory_space=pltpu.VMEM)
    dma = pltpu.SemaphoreType.DMA
    sds = jax.ShapeDtypeStruct
    wshapes = [(2, 2, 2, 2, len(k), shard // len(k), c) for k, c in (
        (COLORS, 2 * n_kv), (SLIM, dim // 2), (SLIM, dim // 2), (COLORS, dim))]
    return pl.pallas_call(
        functools.partial(gather_kernel, (n_seq, rows, dim, n_kv)),
        in_specs=[hbm] * 6 + [vm] * 3,
        out_specs=[hbm] * 9 + [vm] * 6,
        out_shape=[sds((tokens, dim), BF16)] * 3 + [sds((n_seq, rows, 2 * n_kv), BF16)] * 2 + [
            sds(w, BF16) for w in wshapes] + [sds((tokens, HEAD), F32)] * 2 + [
            sds((1, dim), F32), sds((tokens, HEAD), F32)] + [sds((n_seq, 1, rows), jnp.int32)] * 2,
        scratch_shapes=[pltpu.VMEM((tokens, dim), BF16)] * 5 + [
            pltpu.VMEM((n_seq, rows, 2 * n_kv), BF16),
            pltpu.VMEM((n_seq, rows, 2 * n_kv), BF16),
            *[pltpu.VMEM(w, BF16) for w in wshapes],
            pltpu.VMEM((2, 2, 2, 2, 1, HEAD), F32),
            pltpu.VMEM((8, dim), F32),
            pltpu.VMEM((n_seq, rows), jnp.int32),
            dma((6 * n_kv // HEAD + 5 + 2 * len(SLIM),)), dma((10,)), *[dma((4, 3, 3))] * 4,
            *[dma((4,))] * 4, *[dma((n_seq + 1,))] * 2,
        ],
        compiler_params=pltpu.CompilerParams(collective_id=2, has_side_effects=True, vmem_limit_bytes=60 * 2 ** 20),
        cost_estimate=pl.CostEstimate(flops=2 * tokens * dim * (2 * dim + 2 * n_kv), bytes_accessed=40 * 2 ** 20,
                                      transcendentals=0),
    )(x, dy, wq, wk, wv, wo, gain[None], pos, freq)


def solution(mesh):
    cp_size = mesh.shape['cp']

    def shard_fn(hidden, tok_pos, grad_out, norm_gain, w_query, w_key, w_value, w_out):
        n_seq, rows, dim = hidden.shape
        tokens = n_seq * rows
        n_q = w_query.shape[1]
        n_kv = w_key.shape[1]
        groups = n_kv // HEAD
        x16 = hidden.reshape(tokens, dim)
        dy = grad_out.reshape(tokens, dim)
        q, do, r, kv, kv_oth, w_kv, w_a, w_b, w_o, cos2, sin2, gain, pcol, pos, pos_oth = gather_project(
            x16, dy, w_query, w_key, w_value, w_out, norm_gain, tok_pos)
        w_a, w_b, w_kv, w_o = (w.reshape(dim, -1) for w in (w_a, w_b, w_kv, w_o))
        o, dq, dkv = attention(q, do, kv.reshape(tokens, -1), kv_oth.reshape(tokens, -1), pcol, pos, pos_oth, cos2, sin2)
        g_wq, g_wk, g_wv, g_wo, gg, result, grad_hidden = wgrad(o, dy, r, dq, dkv, x16, w_o, w_a, w_b, w_kv, gain)
        shard = lax.axis_index('fsdp') * cp_size + lax.axis_index('cp')
        g_gain = lax.dynamic_slice(gg[0], (shard * norm_gain.shape[0],), norm_gain.shape)
        return result.reshape(hidden.shape), grad_hidden.reshape(hidden.shape), g_wq, g_wk, g_wv, g_wo, g_gain

    row = P('fsdp', 'cp', None)
    pos_spec = P('fsdp', 'cp')
    w = P(AXES, None)
    g = P(AXES)
    return jax.shard_map(shard_fn, mesh=mesh, in_specs=(row, pos_spec, row, g, w, w, w, w),
                         out_specs=(row, row, w, w, w, w, g), check_vma=False)
```

```python
import functools
import math

import jax
import jax.numpy as jnp
import numpy as np
from jax import lax
from jax.experimental import pallas as pl
from jax.experimental.pallas import tpu as pltpu
from jax.sharding import PartitionSpec as P

HEAD = 128
THETA = 1000000.0
EPS = 1e-5
NEG = -1e30
SCALE = HEAD ** -0.5
LOG2E = math.log2(math.e)
AXES = ('fsdp', 'cp')
MESH = pl.DeviceIdType.MESH
F32 = jnp.float32
BF16 = jnp.bfloat16
NT = (((1,), (1,)), ((), ()))
TN = (((0,), (0,)), ((), ()))
NN = (((1,), (0,)), ((), ()))


def dot(a, b, dims=NN):
    return lax.dot_general(a, b, dims, preferred_element_type=F32)


def loop(lo, hi, body):
    def run(i, carry):
        body(i)
        return carry
    lax.fori_loop(lo, hi, run, None)


def span(i, size):
    return pl.ds(pl.multiple_of(i * size, size), size)


def lanes(i):
    return slice(i * HEAD, (i + 1) * HEAD)


def rope(v, cos2, sin2):
    return v * cos2 + pltpu.roll(v, HEAD // 2, 1) * sin2


def unrope(v, cos2, sin2):
    return v * cos2 - pltpu.roll(v, HEAD // 2, 1) * sin2


COLORS = ('xyz', 'yzx', 'zxy')
SLIM = ('zxy', 'zyx')
BLOCK = 256


def place():
    f = lax.axis_index('fsdp')
    z = lax.axis_index('cp')
    bits = {'y': f // 4, 'x': (f // 2) % 2, 'c': f % 2, 'z': z}
    peers = {'y': {'fsdp': f + 4 - 8 * bits['y']}, 'x': {'fsdp': f + 2 - 4 * bits['x']},
             'c': {'fsdp': f + 1 - 2 * bits['c']}, 'z': {'cp': 1 - z}}
    return bits, peers


def meet(peers):
    barrier = pltpu.get_barrier_semaphore()
    for a in 'cxyz':
        pl.semaphore_signal(barrier, inc=1, device_id=peers[a], device_id_type=MESH)
    pl.semaphore_wait(barrier, 4)


def chunk_list(dim, width):
    half = width // 2
    out = [('o', 0, half), ('o', half, half)]
    out += [('o', c, width) for c in range(width, dim, width)]
    out += [('q', c, width) for c in range(0, dim, width)]
    return out + [('kv', 0, half), ('kv', half, half)]


def wgrad_kernel(shapes, o_hbm, dy_hbm, r_hbm, dq_hbm, dkv_hbm, x_hbm, wo_hbm, wa_hbm, wb_hbm, wkv_hbm, gain_ref,
                 gwq_ref, gwk_ref, gwv_ref, gwo_ref, gg_ref, res_hbm, gh_hbm,
                 lhs, rhs, g, rcv_a, gain_rcv, wo, wkv, xb, dyb, dqb, dkvb, outb,
                 load_sem, w_sem, blk_sem, out_sem, *rest):
    tokens, dim, width, sub = shapes
    bits, peers = place()
    core = bits['c']
    chunks = chunk_list(dim, width)
    n = len(chunks)
    h, rcv = rest[:n], [rest[n + t * 3:n + t * 3 + 3] for t in range(n)]
    d2d_send, d2d_recv, ici_send, ici_recv, gain_send, gain_recv, credit = rest[4 * n:]
    seg = dim // 4
    half = seg // 2

    def load_lhs(i):
        return pltpu.make_async_copy((o_hbm, r_hbm)[i], lhs.at[i], load_sem.at[i])

    def load_rhs(t):
        kind, col, w = chunks[t]
        src = {'o': dy_hbm, 'q': dq_hbm, 'kv': dkv_hbm}[kind]
        return pltpu.make_async_copy(src.at[:, pl.ds(col, w)], rhs.at[t % 2, :, pl.ds(0, w)], load_sem.at[2 + t])

    load_lhs(0).start()
    load_rhs(0).start()
    load_lhs(1).start()
    load_rhs(1).start()
    hd = dim // 2
    w_loads = [pltpu.make_async_copy(a, b, w_sem.at[i]) for i, (a, b) in enumerate((
        (wo_hbm, wo), (wkv_hbm, wkv), (wa_hbm, lhs.at[0, :, pl.ds(0, hd)]), (wb_hbm, lhs.at[0, :, pl.ds(hd, hd)])))]
    w_loads[0].start()
    w_loads[1].start()
    n_blk = tokens // BLOCK

    def blk_loads(b, which):
        rs = pl.ds(pl.multiple_of(b * BLOCK, BLOCK), BLOCK)
        srcs = ((x_hbm, xb), (dy_hbm, dyb), (dq_hbm, dqb), (dkv_hbm, dkvb))
        return [pltpu.make_async_copy(srcs[k][0].at[rs, :], srcs[k][1].at[b % 2], blk_sem.at[k, b % 2])
                for k in which]

    def out_copy(dst, b):
        rs = pl.ds(pl.multiple_of(b * BLOCK, BLOCK), BLOCK)
        return pltpu.make_async_copy(outb.at[b % 2], dst.at[rs, :], out_sem.at[b % 2])

    def blocks(lo, hi, which, dst, body):
        def run(b, carry):
            for c in blk_loads(b, which):
                c.wait()

            @pl.when(b + 1 < n_blk)
            def _():
                for c in blk_loads(b + 1, which):
                    c.start()

            @pl.when(b >= 2)
            def _():
                out_copy(dst, b - 2).wait()

            outb[b % 2] = body(b)
            out_copy(dst, b).start()
            return carry
        lax.fori_loop(lo, hi, run, 0)

    def res_body(b):
        rs = pl.ds(pl.multiple_of(b * BLOCK, BLOCK), BLOCK)
        return (xb[b % 2].astype(F32) + dot(lhs[0, rs, :], wo[...])).astype(BF16)

    def dr_body(b):
        xf = xb[b % 2].astype(F32)
        inv = lax.rsqrt(jnp.mean(xf * xf, axis=1, keepdims=True) + EPS)
        xh = xf * inv
        dr = dot(dqb[b % 2], lhs[0], NT) + dot(dkvb[b % 2], wkv[...], NT)
        gg_ref[...] = gg_ref[...] + jnp.sum(dr * xh, axis=0, keepdims=True)
        a = dr * gain_ref[...]
        gx = inv * (a - xh * jnp.mean(a * xh, axis=1, keepdims=True))
        return (dyb[b % 2].astype(F32) + gx).astype(BF16)

    for c in blk_loads(0, (0,)):
        c.start()
    meet(peers)

    def d2d(t):
        w = pl.ds(0, chunks[t][2])
        return pltpu.make_async_remote_copy(g.at[t % 2, :, 1 - core, :, w], rcv_a.at[t % 2, :, :, w], d2d_send.at[t], d2d_recv.at[t],
                                            device_id=peers['c'], device_id_type=MESH)

    def ici(t, c, p):
        b1, b2, b3 = (bits[a] for a in COLORS[c])
        if p == 0:
            src = h[t].at[c, pl.ds((1 - b1) * 4, 4)]
        elif p == 1:
            src = h[t].at[c, pl.ds(b1 * 4 + (1 - b2) * 2, 2)]
        else:
            src = h[t].at[c, pl.ds(b1 * 4 + b2 * 2 + (1 - b3), 1)]
        return pltpu.make_async_remote_copy(src, rcv[t][p].at[c], ici_send.at[t, c, p], ici_recv.at[t, c, p],
                                            device_id=peers[COLORS[c][p]], device_id_type=MESH)

    def compute(t):
        kind, _, w = chunks[t]
        li = int(kind != 'o')
        if t == 0 or (li and chunks[t - 1][0] == 'o'):
            load_lhs(li).wait()
        load_rhs(t).wait()

        def body(yx):
            res = dot(lhs[li, :, span(yx, seg)], rhs[t % 2, :, :w], TN)
            g[t % 2, yx, 0, :, :w] = res[:half]
            g[t % 2, yx, 1, :, :w] = res[half:]
        loop(0, 4, body)
        if t + 2 < n:
            load_rhs(t + 2).start()
        if t >= 2:
            pl.semaphore_wait(credit, 1)
        d2d(t).start()

    def fold(t):
        w = chunks[t][2]
        d2d(t).wait()
        for y in range(2):
            for x in range(2):
                for z in range(2):
                    at = {'y': y, 'x': x, 'z': z}
                    for c in range(3):
                        a1, a2, a3 = (at[a] for a in COLORS[c])
                        rows = slice(z * 3 * sub + c * sub, z * 3 * sub + (c + 1) * sub)
                        h[t][c, a1 * 4 + a2 * 2 + a3] = g[t % 2, y * 2 + x, core, rows, :w] + rcv_a[t % 2, y * 2 + x, rows, :w]
        for c in range(3):
            ici(t, c, 0).start()
        if t + 2 < n:
            pl.semaphore_signal(credit, inc=1, device_id=peers['c'], device_id_type=MESH)

    def reduce(t, p):
        for c in range(3):
            b1, b2, b3 = (bits[a] for a in COLORS[c])
            ici(t, c, p).wait()
            k = (0, b1 * 4, b1 * 4 + b2 * 2, b1 * 4 + b2 * 2 + b3)[p + 1]
            if p < 2:
                for j in range(4 >> p):
                    h[t][c, k + j] = h[t][c, k + j] + rcv[t][p][c, j]
                ici(t, c, p + 1).start()
                continue
            kind, col, w = chunks[t]
            rws = slice(c * sub, (c + 1) * sub)
            tot = h[t][c, k] + rcv[t][p][c, 0]
            if kind == 'kv':
                for j in range(w // HEAD):
                    b = col // HEAD + j
                    (gwk_ref, gwv_ref)[b % 2][rws, lanes(b // 2)] = tot[:, lanes(j)]
            else:
                (gwo_ref if kind == 'o' else gwq_ref)[rws, col:col + w] = tot

    gg_ref[...] = jnp.zeros_like(gg_ref)

    def gain_copy(i):
        return pltpu.make_async_remote_copy(gg_ref, gain_rcv.at[i], gain_send.at[i], gain_recv.at[i],
                                            device_id=peers['cxyz'[i]], device_id_type=MESH)

    def flush(dst):
        out_copy(dst, n_blk - 2).wait()
        out_copy(dst, n_blk - 1).wait()

    every = (0, 1, 2, 3)
    third, fill = n_blk // 3, n_blk // 2
    assert [c[0] for c in chunks].count('o') == 4
    for i in range(n + 4):
        if i < n:
            compute(i)
        if 0 <= i - 1 < n:
            fold(i - 1)
        for p in range(3):
            if 0 <= i - 2 - p < n:
                reduce(i - 2 - p, p)
        if 2 <= i < 4:
            if i == 2:
                w_loads[0].wait()
            blocks((i - 2) * fill, (i - 1) * fill, (0,), res_hbm, res_body)
            if i == 3:
                flush(res_hbm)
                for c in [*w_loads[2:], *blk_loads(0, every)]:
                    c.start()
        elif 4 <= i < 7:
            if i == 4:
                for c in w_loads[1:]:
                    c.wait()
            blocks((i - 4) * third, (i - 3) * third, every, gh_hbm, dr_body)
            if i == 6:
                flush(gh_hbm)
                gain_copy(0).start()
        elif 7 <= i < 11:
            gain_copy(i - 7).wait()
            gg_ref[...] = gg_ref[...] + gain_rcv[i - 7]
            if i < 10:
                gain_copy(i - 6).start()


def wgrad(o, dy, r, dq, dkv, x, w_o, w_a, w_b, w_kv, gain):
    tokens, dim = o.shape
    width = dkv.shape[1]
    shard = dim // 16
    sub = shard // 3
    chunks = chunk_list(dim, width)
    n = len(chunks)
    hbm = pl.BlockSpec(memory_space=pl.ANY)
    vm = pl.BlockSpec(memory_space=pltpu.VMEM)
    dma = pltpu.SemaphoreType.DMA
    return pl.pallas_call(
        functools.partial(wgrad_kernel, (tokens, dim, width, sub)),
        in_specs=[hbm] * 10 + [vm],
        out_specs=[vm] * 5 + [hbm] * 2,
        out_shape=[jax.ShapeDtypeStruct(a, F32) for a in (
            (shard, dim), (shard, width // 2), (shard, width // 2), (shard, dim), (1, dim))] + [jax.ShapeDtypeStruct((tokens, dim), BF16)] * 2,
        scratch_shapes=[
            pltpu.VMEM((2, tokens, dim), BF16),
            pltpu.VMEM((2, tokens, width), BF16),
            pltpu.VMEM((2, 4, 2, dim // 8, width), F32),
            pltpu.VMEM((2, 4, dim // 8, width), F32),
            pltpu.VMEM((4, 1, dim), F32),
            pltpu.VMEM((dim, dim), BF16),
            pltpu.VMEM((dim, width), BF16),
            *[pltpu.VMEM((2, BLOCK, c), BF16) for c in (dim, dim, dim, width, dim)],
            dma((2 + n,)), dma((4,)), dma((4, 2)), dma((2,)),
            *[pltpu.VMEM((3, 8, sub, c[2]), F32) for c in chunks],
            *[pltpu.VMEM((3, k, sub, c[2]), F32) for c in chunks for k in (4, 2, 1)],
            *[dma((n,))] * 2, *[dma((n, 3, 3))] * 2, *[dma((4,))] * 2,
            pltpu.SemaphoreType.REGULAR,
        ],
        compiler_params=pltpu.CompilerParams(collective_id=1, has_side_effects=True, vmem_limit_bytes=60 * 2 ** 20),
        cost_estimate=pl.CostEstimate(flops=2 * tokens * dim * (2 * dim + width), bytes_accessed=30 * 2 ** 20,
                                      transcendentals=0),
    )(o, dy, r, dq, dkv, x, w_o, w_a, w_b, w_kv, gain)


def gather_kernel(shapes, x_hbm, dy_hbm, wq_hbm, wk_hbm, wv_hbm, wo_hbm, gain_ref, pos_ref, freq_ref,
                  r_hbm, o_hbm, dq_hbm, wkv_hbm, wa_hbm, wb_hbm, wf_hbm, gain_out, dkv_out,
                  x, dy, r, q, do, kvo, kvx, wkv, wa, wb, wo, gbuf, grow, px, cos_ref, sin_ref, pcol,
                  mask, p_s, ds_s, mine_kv, snd, rcv,
                  load_sem, out_sem, blk_sem, ici_send, ici_recv, fwd_send, fwd_recv, own_send, own_recv,
                  g_send, g_recv, kv_send, kv_recv, dkv_send, dkv_recv):
    n_seq, rows, dim, n_kv = shapes
    bits, peers = place()
    by, bx, bc, bz = (bits[a] for a in 'yxcz')
    shard = dim // 16
    third, mid = shard // 3, shard // len(SLIM)
    hq = dim // 2
    groups = n_kv // HEAD
    gsize = dim // HEAD // groups
    fast = COLORS
    slim = SLIM
    pieces = [(wkv, fast), (wo, fast), (wa, slim), (wb, slim)]

    loads = []

    def load(src, dst):
        c = pltpu.make_async_copy(src, dst, load_sem.at[len(loads)])
        c.start()
        loads.append(c)
        return len(loads) - 1

    mine = lambda ref: ref.at[by, bx, bc, bz]
    for c in range(3):
        for g in range(n_kv // HEAD):
            hc = slice(g * HEAD, (g + 1) * HEAD)
            rws = slice(c * third, (c + 1) * third)
            for j, w_hbm in enumerate((wk_hbm, wv_hbm)):
                oc = slice((2 * g + j) * HEAD, (2 * g + j + 1) * HEAD)
                load(w_hbm.at[rws, hc], wkv.at[by, bx, bc, bz, c, :, oc])
    n_first = len(loads)
    for c in range(3):
        load(wo_hbm.at[c * third:(c + 1) * third, :], wo.at[by, bx, bc, bz, c])
    for c in range(len(SLIM)):
        rws = slice(c * mid, (c + 1) * mid)
        load(wq_hbm.at[rws, :hq], wa.at[by, bx, bc, bz, c])
        load(wq_hbm.at[rws, hq:], wb.at[by, bx, bc, bz, c])
    n_all = len(loads)
    l_x = load(x_hbm, x)
    l_dy = load(dy_hbm, dy)
    gbuf[by, bx, bc, bz] = jnp.zeros((1, HEAD), F32)
    gbuf[by, bx, bc, bz, :, :shard] = gain_ref[...]
    meet(peers)

    def region(p, c, f, flip):
        ref, order = pieces[p][0], pieces[p][1][c]
        idx = []
        for a in 'yxcz':
            if a in order[:f]:
                idx.append(slice(None))
            elif a == order[f] and flip:
                idx.append(1 - bits[a])
            else:
                idx.append(bits[a])
        return ref.at[idx[0], idx[1], idx[2], idx[3], c]

    def ici(p, c, f):
        s = region(p, c, f, False)
        return pltpu.make_async_remote_copy(s, s, ici_send.at[p, c, f], ici_recv.at[p, c, f],
                                            device_id=peers[pieces[p][1][c][f]], device_id_type=MESH)

    def fwd(p, c, f):
        s = region(p, c, f, True)
        return pltpu.make_async_remote_copy(s, s, fwd_send.at[p, c, f], fwd_recv.at[p, c, f],
                                            device_id=peers['c'], device_id_type=MESH)

    def own(p):
        s = mine(pieces[p][0])
        return pltpu.make_async_remote_copy(s, s, own_send.at[p], own_recv.at[p],
                                            device_id=peers['c'], device_id_type=MESH)

    def begin(p):
        for c in range(len(pieces[p][1])):
            ici(p, c, 0).start()
        own(p).start()

    def advance(p, f):
        for c in range(len(pieces[p][1])):
            ici(p, c, f).wait()
            if f < 2:
                ici(p, c, f + 1).start()
            fwd(p, c, f).start()

    def settle(p):
        own(p).wait()
        for c in range(len(pieces[p][1])):
            for f in range(3):
                fwd(p, c, f).wait()

    def gain_copy(i):
        s = (gbuf.at[by, bx, bc, bz], gbuf.at[by, bx, :, bz], gbuf.at[by, bx], gbuf.at[by])[i]
        return pltpu.make_async_remote_copy(s, s, g_send.at[i], g_recv.at[i],
                                            device_id=peers['czxy'[i]], device_id_type=MESH)

    def kv_copy(i):
        return pltpu.make_async_remote_copy(kvo.at[i], kvx.at[i], kv_send.at[i], kv_recv.at[i],
                                            device_id=peers['z'], device_id_type=MESH)

    def px_copy():
        return pltpu.make_async_remote_copy(pos_ref, px, kv_send.at[n_seq], kv_recv.at[n_seq],
                                            device_id=peers['z'], device_id_type=MESH)

    gain_copy(0).start()
    for i in range(n_first):
        loads[i].wait()
    begin(0)
    px_copy().start()
    for i in range(n_first, n_all):
        loads[i].wait()
    for p in (1, 2, 3):
        begin(p)
    gain_copy(0).wait()
    gain_copy(1).start()

    def tables(i):
        rs = span(i, rows)
        row = pos_ref[pl.ds(i, 1), :]
        col = jnp.transpose(jnp.broadcast_to(row.astype(F32), (HEAD, rows)))
        pcol[rs, :] = col
        ang = col * freq_ref[...]
        lane = lax.broadcasted_iota(jnp.int32, (rows, HEAD), 1)
        cos_ref[rs, :] = jnp.cos(ang)
        sn = jnp.sin(ang)
        sin_ref[rs, :] = jnp.where(lane < HEAD // 2, -sn, sn)

    mid_seq = n_seq // 2
    loop(0, mid_seq, tables)
    gain_copy(1).wait()
    gain_copy(2).start()
    advance(0, 0)
    advance(1, 0)
    loop(mid_seq, n_seq, tables)
    gain_copy(2).wait()
    gain_copy(3).start()
    advance(0, 1)
    advance(1, 1)
    gain_copy(3).wait()
    advance(2, 0)
    lane = lax.broadcasted_iota(jnp.int32, (8, HEAD), 1)
    for b in range(dim // HEAD):
        acc = jnp.zeros((8, HEAD), F32)
        for sh in range(16):
            lo = shard * sh - HEAD * b
            if lo >= HEAD or lo + shard <= 0:
                continue
            row = jnp.broadcast_to(gbuf[sh // 8, (sh // 4) % 2, (sh // 2) % 2, sh % 2], (8, HEAD))
            row = pltpu.roll(row, lo % HEAD, 1) if lo % HEAD else row
            acc = jnp.where((lane >= lo) & (lane < lo + shard), row, acc)
        grow[:, b * HEAD:(b + 1) * HEAD] = acc
    gain_out[...] = grow[0:1, :]
    loads[l_x].wait()

    def norm(i):
        rs = span(i, rows // 2)
        xf = x[rs, :].astype(F32)
        inv = lax.rsqrt(jnp.mean(xf * xf, axis=1, keepdims=True) + EPS)
        r[rs, :] = (xf * inv * grow[0:1, :]).astype(BF16)

    loop(0, 2 * n_seq, norm)
    r_out = pltpu.make_async_copy(r, r_hbm, out_sem.at[0])
    r_out.start()
    advance(0, 2)
    advance(3, 0)
    settle(0)
    wkv_out = pltpu.make_async_copy(wkv, wkv_hbm, out_sem.at[4])
    wkv_out.start()

    def kv_proj(i):
        rs = span(i, rows)
        kv = dot(r[rs, :], wkv[...].reshape(dim, 2 * n_kv))
        for g in range(0, 2 * n_kv // HEAD, 2):
            kvo[i, :, lanes(g)] = rope(kv[:, lanes(g)], cos_ref[rs, :], sin_ref[rs, :]).astype(BF16)
            kvo[i, :, lanes(g + 1)] = kv[:, lanes(g + 1)].astype(BF16)
        kv_copy(i).start()

    loop(0, mid_seq, kv_proj)
    advance(1, 2)
    loop(mid_seq, n_seq, kv_proj)
    advance(2, 1)
    settle(1)
    wf_out = pltpu.make_async_copy(wo, wf_hbm, out_sem.at[3])
    wf_out.start()
    loads[l_dy].wait()

    def do_proj(i):
        rs = span(i, rows)
        do[rs, :] = dot(dy[rs, :], wo[...].reshape(dim, dim), NT).astype(BF16)

    def q_proj(half):
        def body(i):
            rs = span(i, rows)
            res = dot(r[rs, :], (wa, wb)[half][...].reshape(dim, hq))
            for h in range(hq // HEAD):
                q[rs, lanes(half * (hq // HEAD) + h)] = rope(res[:, lanes(h)], cos_ref[rs, :], sin_ref[rs, :]).astype(BF16)
        return body

    def dkv_copy(t):
        return pltpu.make_async_remote_copy(snd.at[t], rcv.at[t], dkv_send.at[t], dkv_recv.at[t],
                                            device_id=peers['z'], device_id_type=MESH)

    def blk_out(g, i):
        rs, hc = span(i, rows), pl.ds(g * gsize * HEAD, gsize * HEAD)
        return [pltpu.make_async_copy(src.at[rs, hc], dst.at[rs, hc], blk_sem.at[j, g * n_seq + i])
                for j, (src, dst) in enumerate(((dy, o_hbm), (x, dq_hbm)))]

    def attend(g):
        def body(i):
            if g == 0:
                kv_copy(i).wait()
            rs = span(i, rows)
            pq = pcol[rs, :]
            for j, ref in enumerate((pos_ref, px)):
                key = ref[pl.ds(i, 1), :].astype(F32)
                for b in range(rows // HEAD):
                    mask[:, lanes(j * (rows // HEAD) + b)] = jnp.where(key[:, lanes(b)] <= pq, 0.0, NEG)
            cos2, sin2 = cos_ref[rs, :], sin_ref[rs, :]
            k = jnp.concatenate([kvo[i, :, lanes(2 * g)], kvx[i, :, lanes(2 * g)]], axis=0)
            v = jnp.concatenate([kvo[i, :, lanes(2 * g + 1)], kvx[i, :, lanes(2 * g + 1)]], axis=0)
            heads = [lanes(g * gsize + h) for h in range(gsize)]
            for h, hc in enumerate(heads):
                hrow = slice(h * rows, (h + 1) * rows)
                qh, doh = q[rs, hc], do[rs, hc]
                s = dot(qh, k, NT) * (SCALE * LOG2E) + mask[...]
                m = jnp.max(s, axis=1, keepdims=True)
                e = jnp.exp2(s - m)
                rl = 1.0 / jnp.sum(e, axis=1, keepdims=True)
                o = (dot(e.astype(BF16), v) * rl).astype(BF16)
                dy[rs, hc] = o
                delta = jnp.sum(doh.astype(F32) * o.astype(F32), axis=1, keepdims=True)
                p = e * rl
                p_s[hrow, :] = p.astype(BF16)
                ds = (p * (dot(doh, v, NT) - delta)).astype(BF16)
                ds_s[hrow, :] = ds
                x[rs, hc] = unrope(dot(ds, k) * SCALE, cos2, sin2).astype(BF16)
            do6 = jnp.concatenate([do[rs, hc] for hc in heads], axis=0)
            q6 = jnp.concatenate([q[rs, hc] for hc in heads], axis=0)
            dk = dot(ds_s[...], q6, TN) * SCALE
            dv = dot(p_s[...], do6, TN)
            t = g * n_seq + i
            for j, val in enumerate((dk, dv)):
                mine_kv[t, :, lanes(j)] = val[:rows]
                snd[t, :, lanes(j)] = val[rows:]
            dkv_copy(t).start()
            for c in blk_out(g, i):
                c.start()
        return body

    def finish(g):
        def body(i):
            t = g * n_seq + i
            rs = span(i, rows)
            dkv_copy(t).wait()
            tot = mine_kv[t] + rcv[t]
            dkv_out[rs, lanes(2 * g)] = unrope(tot[:, :HEAD], cos_ref[rs, :], sin_ref[rs, :]).astype(BF16)
            dkv_out[rs, lanes(2 * g + 1)] = tot[:, HEAD:].astype(BF16)
            for c in blk_out(g, i):
                c.wait()
        return body

    loop(0, mid_seq, do_proj)
    advance(3, 1)
    advance(2, 2)
    loop(mid_seq, n_seq, do_proj)
    settle(2)
    wa_out = pltpu.make_async_copy(wa, wa_hbm, out_sem.at[5])
    wa_out.start()
    loop(0, n_seq, q_proj(0))
    px_copy().wait()
    loop(0, mid_seq, attend(0))
    advance(3, 2)
    loop(mid_seq, n_seq, attend(0))
    settle(3)
    wb_out = pltpu.make_async_copy(wb, wb_hbm, out_sem.at[1])
    wb_out.start()
    loop(0, n_seq, q_proj(1))
    for g in range(1, groups):
        loop(0, n_seq, attend(g))
    for g in range(groups):
        loop(0, n_seq, finish(g))
    for c in (r_out, wf_out, wkv_out, wa_out, wb_out):
        c.wait()


def gather_project(x, dy, wq, wk, wv, wo, gain, pos):
    tokens, dim = x.shape
    n_seq, rows = pos.shape
    n_kv = wk.shape[1]
    shard = dim // 16
    steps = n_seq * n_kv // HEAD
    half = HEAD // 2
    freq = np.float32(THETA) ** (-np.arange(half, dtype=np.float32) / half)
    freq = jnp.asarray(np.tile(freq, 2)[None])
    hbm = pl.BlockSpec(memory_space=pl.ANY)
    vm = pl.BlockSpec(memory_space=pltpu.VMEM)
    dma = pltpu.SemaphoreType.DMA
    sds = jax.ShapeDtypeStruct
    wshapes = [(2, 2, 2, 2, len(k), shard // len(k), c) for k, c in (
        (COLORS, 2 * n_kv), (SLIM, dim // 2), (SLIM, dim // 2), (COLORS, dim))]
    return pl.pallas_call(
        functools.partial(gather_kernel, (n_seq, rows, dim, n_kv)),
        in_specs=[hbm] * 6 + [vm] * 3,
        out_specs=[hbm] * 7 + [vm] * 2,
        out_shape=[sds((tokens, dim), BF16)] * 3 + [sds(w, BF16) for w in wshapes] + [
            sds((1, dim), F32), sds((tokens, 2 * n_kv), BF16)],
        scratch_shapes=[pltpu.VMEM((tokens, dim), BF16)] * 5 + [
            pltpu.VMEM((n_seq, rows, 2 * n_kv), BF16),
            pltpu.VMEM((n_seq, rows, 2 * n_kv), BF16),
            *[pltpu.VMEM(w, BF16) for w in wshapes],
            pltpu.VMEM((2, 2, 2, 2, 1, HEAD), F32),
            pltpu.VMEM((8, dim), F32),
            pltpu.VMEM((n_seq, rows), jnp.int32),
            *[pltpu.VMEM((tokens, HEAD), F32)] * 3,
            pltpu.VMEM((rows, 2 * rows), F32),
            *[pltpu.VMEM((dim // n_kv * rows, 2 * rows), BF16)] * 2,
            *[pltpu.VMEM((steps, rows, 2 * HEAD), F32)] * 3,
            dma((6 * n_kv // HEAD + 5 + 2 * len(SLIM),)), dma((6,)), dma((2, steps)), *[dma((4, 3, 3))] * 4,
            *[dma((4,))] * 4, *[dma((n_seq + 1,))] * 2, *[dma((steps,))] * 2,
        ],
        compiler_params=pltpu.CompilerParams(collective_id=2, has_side_effects=True, vmem_limit_bytes=63 * 2 ** 20),
        cost_estimate=pl.CostEstimate(flops=2 * tokens * dim * (2 * dim + 2 * n_kv), bytes_accessed=40 * 2 ** 20,
                                      transcendentals=0),
    )(x, dy, wq, wk, wv, wo, gain[None], pos, freq)


def solution(mesh):
    cp_size = mesh.shape['cp']

    def shard_fn(hidden, tok_pos, grad_out, norm_gain, w_query, w_key, w_value, w_out):
        n_seq, rows, dim = hidden.shape
        tokens = n_seq * rows
        n_q = w_query.shape[1]
        n_kv = w_key.shape[1]
        groups = n_kv // HEAD
        x16 = hidden.reshape(tokens, dim)
        dy = grad_out.reshape(tokens, dim)
        r, o, dq, w_kv, w_a, w_b, w_o, gain, dkv = gather_project(
            x16, dy, w_query, w_key, w_value, w_out, norm_gain, tok_pos)
        w_a, w_b, w_kv, w_o = (w.reshape(dim, -1) for w in (w_a, w_b, w_kv, w_o))
        g_wq, g_wk, g_wv, g_wo, gg, result, grad_hidden = wgrad(o, dy, r, dq, dkv, x16, w_o, w_a, w_b, w_kv, gain)
        shard = lax.axis_index('fsdp') * cp_size + lax.axis_index('cp')
        g_gain = lax.dynamic_slice(gg[0], (shard * norm_gain.shape[0],), norm_gain.shape)
        return result.reshape(hidden.shape), grad_hidden.reshape(hidden.shape), g_wq, g_wk, g_wv, g_wo, g_gain

    row = P('fsdp', 'cp', None)
    pos_spec = P('fsdp', 'cp')
    w = P(AXES, None)
    g = P(AXES)
    return jax.shard_map(shard_fn, mesh=mesh, in_specs=(row, pos_spec, row, g, w, w, w, w),
                         out_specs=(row, row, w, w, w, w, g), check_vma=False)
```

```python
import functools
import math

import jax
import jax.numpy as jnp
import numpy as np
from jax import lax
from jax.experimental import pallas as pl
from jax.experimental.pallas import tpu as pltpu
from jax.sharding import PartitionSpec as P

HEAD = 128
THETA = 1000000.0
EPS = 1e-5
NEG = -1e30
SCALE = HEAD ** -0.5
LOG2E = math.log2(math.e)
AXES = ('fsdp', 'cp')
MESH = pl.DeviceIdType.MESH
F32 = jnp.float32
BF16 = jnp.bfloat16
NT = (((1,), (1,)), ((), ()))
TN = (((0,), (0,)), ((), ()))
NN = (((1,), (0,)), ((), ()))


def dot(a, b, dims=NN):
    return lax.dot_general(a, b, dims, preferred_element_type=F32)


def loop(lo, hi, body):
    def run(i, carry):
        body(i)
        return carry
    lax.fori_loop(lo, hi, run, None)


def total(a):
    return jnp.sum(a, axis=1, keepdims=True)


def average(a):
    return jnp.mean(a, axis=1, keepdims=True)


def span(i, size):
    return pl.ds(pl.multiple_of(i * size, size), size)


def span_of(i, size):
    return slice(i * size, (i + 1) * size)


def lanes(i):
    return span_of(i, HEAD)


def rope(v, cos2, sin2):
    return v * cos2 + pltpu.roll(v, HEAD // 2, 1) * sin2


def unrope(v, cos2, sin2):
    return v * cos2 - pltpu.roll(v, HEAD // 2, 1) * sin2


COLORS = ('xyz', 'yzx', 'zxy')
SLIM = ('zxy', 'zyx')
BLOCK = 256
EARLY = 256


def place():
    f = lax.axis_index('fsdp')
    z = lax.axis_index('cp')
    bits = {'y': f // 4, 'x': (f // 2) % 2, 'c': f % 2, 'z': z}
    peers = {'y': {'fsdp': f + 4 - 8 * bits['y']}, 'x': {'fsdp': f + 2 - 4 * bits['x']},
             'c': {'fsdp': f + 1 - 2 * bits['c']}, 'z': {'cp': 1 - z}}
    return bits, peers


def meet(peers):
    barrier = pltpu.get_barrier_semaphore()
    for a in 'cxyz':
        pl.semaphore_signal(barrier, inc=1, device_id=peers[a], device_id_type=MESH)
    pl.semaphore_wait(barrier, 4)


def chunk_list(dim, width):
    half = width // 2
    out = [('o', 0, half), ('o', half, half)]
    out += [('o', c, width) for c in range(width, dim, width)]
    out += [('q', dim // 2, half), ('q', dim - width, width)]
    return out + [('kv', 0, half), ('kv', half, half)]


def wgrad_kernel(shapes, o_hbm, dy_hbm, r_hbm, dq_hbm, dkv_hbm, x_hbm, wo_hbm, wa_hbm, wb_hbm, wkv_hbm, gain_ref, part_ref,
                 gwq_ref, gwk_ref, gwv_ref, gwo_ref, gg_ref, res_hbm, gh_hbm,
                 lhs, rhs, g, rcv_a, part_rcv, part_sem, gain_rcv, wo, wkv, xb, dyb, dqb, dkvb, outb,
                 load_sem, w_sem, blk_sem, out_sem, *rest):
    tokens, dim, width, sub = shapes
    bits, peers = place()
    core = bits['c']
    chunks = chunk_list(dim, width)
    n = len(chunks)
    h, rcv = rest[:n], [rest[n + t * 3:n + t * 3 + 3] for t in range(n)]
    d2d_send, d2d_recv, ici_send, ici_recv, gain_send, gain_recv, credit = rest[4 * n:]
    seg = dim // 4
    half = seg // 2

    def load_lhs(i):
        return pltpu.make_async_copy((o_hbm, r_hbm)[i], lhs.at[i], load_sem.at[i])

    def load_rhs(t):
        kind, col, w = chunks[t]
        src = {'o': dy_hbm, 'q': dq_hbm, 'kv': dkv_hbm}[kind]
        return pltpu.make_async_copy(src.at[:, pl.ds(col, w)], rhs.at[t % 2, :, pl.ds(0, w)], load_sem.at[2 + t])

    load_lhs(0).start()
    load_rhs(0).start()
    load_lhs(1).start()
    load_rhs(1).start()
    hd = dim // 2
    w_loads = [pltpu.make_async_copy(a, b, w_sem.at[i]) for i, (a, b) in enumerate((
        (wo_hbm, wo), (wkv_hbm, wkv), (wa_hbm, lhs.at[0, :, pl.ds(0, hd)]), (wb_hbm, lhs.at[0, :, pl.ds(hd, hd)])))]
    w_loads[0].start()
    w_loads[1].start()
    n_blk = tokens // BLOCK

    def blk_loads(b, which):
        rs = pl.ds(pl.multiple_of(b * BLOCK, BLOCK), BLOCK)
        srcs = ((x_hbm, xb), (dy_hbm, dyb), (dq_hbm, dqb), (dkv_hbm, dkvb))
        return [pltpu.make_async_copy(srcs[k][0].at[rs, :], srcs[k][1].at[b % 2], blk_sem.at[k, b % 2])
                for k in which]

    def out_copy(dst, b):
        rs = pl.ds(pl.multiple_of(b * BLOCK, BLOCK), BLOCK)
        return pltpu.make_async_copy(outb.at[b % 2], dst.at[rs, :], out_sem.at[b % 2])

    def blocks(lo, hi, which, dst, body):
        def run(b, carry):
            for c in blk_loads(b, which):
                c.wait()

            @pl.when(b + 1 < n_blk)
            def _():
                for c in blk_loads(b + 1, which):
                    c.start()

            @pl.when(b >= 2)
            def _():
                out_copy(dst, b - 2).wait()

            outb[b % 2] = body(b)
            out_copy(dst, b).start()
            return carry
        lax.fori_loop(lo, hi, run, 0)

    def res_body(b):
        rs = pl.ds(pl.multiple_of(b * BLOCK, BLOCK), BLOCK)
        return (xb[b % 2].astype(F32) + dot(lhs[0, rs, :], wo[...])).astype(BF16)

    def dr_body(b):
        xf = xb[b % 2].astype(F32)
        inv = lax.rsqrt(average(xf * xf) + EPS)
        xh = xf * inv
        dr = dot(dqb[b % 2], lhs[0], NT) + dot(dkvb[b % 2], wkv[...], NT)
        gg_ref[...] = gg_ref[...] + jnp.sum(dr * xh, axis=0, keepdims=True)
        a = dr * gain_ref[...]
        gx = inv * (a - xh * average(a * xh))
        return (dyb[b % 2].astype(F32) + gx).astype(BF16)

    for c in blk_loads(0, (0,)):
        c.start()
    meet(peers)

    def d2d(t):
        w = pl.ds(0, chunks[t][2])
        return pltpu.make_async_remote_copy(g.at[t % 2, :, 1 - core, :, w], rcv_a.at[t % 2, :, :, w], d2d_send.at[t], d2d_recv.at[t],
                                            device_id=peers['c'], device_id_type=MESH)

    def ici(t, c, p):
        b1, b2, b3 = (bits[a] for a in COLORS[c])
        if p == 0:
            src = h[t].at[c, pl.ds((1 - b1) * 4, 4)]
        elif p == 1:
            src = h[t].at[c, pl.ds(b1 * 4 + (1 - b2) * 2, 2)]
        else:
            src = h[t].at[c, pl.ds(b1 * 4 + b2 * 2 + (1 - b3), 1)]
        return pltpu.make_async_remote_copy(src, rcv[t][p].at[c], ici_send.at[t, c, p], ici_recv.at[t, c, p],
                                            device_id=peers[COLORS[c][p]], device_id_type=MESH)

    def compute(t):
        kind, _, w = chunks[t]
        li = int(kind != 'o')
        if t == 0 or (li and chunks[t - 1][0] == 'o'):
            load_lhs(li).wait()
        load_rhs(t).wait()

        def body(yx):
            res = dot(lhs[li, :, span(yx, seg)], rhs[t % 2, :, :w], TN)
            g[t % 2, yx, 0, :, :w] = res[:half]
            g[t % 2, yx, 1, :, :w] = res[half:]
        loop(0, 4, body)
        if t + 2 < n:
            load_rhs(t + 2).start()
        if t >= 2:
            pl.semaphore_wait(credit, 1)
        d2d(t).start()

    def fold(t):
        w = chunks[t][2]
        d2d(t).wait()
        for y, x, z, c in np.ndindex(2, 2, 2, 3):
            at = {'y': y, 'x': x, 'z': z}
            a1, a2, a3 = (at[a] for a in COLORS[c])
            rows = span_of(z * 3 + c, sub)
            h[t][c, a1 * 4 + a2 * 2 + a3] = g[t % 2, y * 2 + x, core, rows, :w] + rcv_a[t % 2, y * 2 + x, rows, :w]
        for c in range(3):
            ici(t, c, 0).start()
        if t + 2 < n:
            pl.semaphore_signal(credit, inc=1, device_id=peers['c'], device_id_type=MESH)

    def reduce(t, p):
        for c in range(3):
            b1, b2, b3 = (bits[a] for a in COLORS[c])
            ici(t, c, p).wait()
            k = (0, b1 * 4, b1 * 4 + b2 * 2, b1 * 4 + b2 * 2 + b3)[p + 1]
            if p < 2:
                for j in range(4 >> p):
                    h[t][c, k + j] = h[t][c, k + j] + rcv[t][p][c, j]
                ici(t, c, p + 1).start()
                continue
            kind, col, w = chunks[t]
            rws = span_of(c, sub)
            tot = h[t][c, k] + rcv[t][p][c, 0]
            if kind == 'kv':
                for j in range(w // HEAD):
                    b = col // HEAD + j
                    (gwk_ref, gwv_ref)[b % 2][rws, lanes(b // 2)] = tot[:, lanes(j)]
            else:
                (gwo_ref if kind == 'o' else gwq_ref)[rws, col:col + w] = tot

    gg_ref[...] = jnp.zeros_like(gg_ref)
    part_copy = pltpu.make_async_remote_copy(part_ref.at[1 - bits['z']], part_rcv, part_sem.at[0], part_sem.at[1],
                                             device_id=peers['z'], device_id_type=MESH)
    part_copy.start()

    def gain_copy(i):
        return pltpu.make_async_remote_copy(gg_ref, gain_rcv.at[i], gain_send.at[i], gain_recv.at[i],
                                            device_id=peers['cxyz'[i]], device_id_type=MESH)

    def flush(dst):
        out_copy(dst, n_blk - 2).wait()
        out_copy(dst, n_blk - 1).wait()

    every = (0, 1, 2, 3)
    third, fill = n_blk // 3, n_blk // 2
    assert [c[0] for c in chunks].count('o') == 4
    for i in range(n + 4):
        if i < n:
            compute(i)
        if 0 <= i - 1 < n:
            fold(i - 1)
        for p in range(3):
            if 0 <= i - 2 - p < n:
                reduce(i - 2 - p, p)
        if 2 <= i < 4:
            if i == 2:
                w_loads[0].wait()
            blocks((i - 2) * fill, (i - 1) * fill, (0,), res_hbm, res_body)
            if i == 3:
                part_copy.wait()
                gwq_ref[:, :hd] = part_ref[bits['z']] + part_rcv[...]
                flush(res_hbm)
                for c in [*w_loads[2:], *blk_loads(0, every)]:
                    c.start()
        elif 4 <= i < 7:
            if i == 4:
                for c in w_loads[1:]:
                    c.wait()
            blocks((i - 4) * third, (i - 3) * third, every, gh_hbm, dr_body)
            if i == 6:
                flush(gh_hbm)
                gain_copy(0).start()
        elif 7 <= i < 11:
            gain_copy(i - 7).wait()
            gg_ref[...] = gg_ref[...] + gain_rcv[i - 7]
            if i < 10:
                gain_copy(i - 6).start()


def wgrad(o, dy, r, dq, dkv, x, w_o, w_a, w_b, w_kv, gain, part):
    tokens, dim = o.shape
    width = dkv.shape[1]
    shard = dim // 16
    sub = shard // 3
    chunks = chunk_list(dim, width)
    n = len(chunks)
    hbm = pl.BlockSpec(memory_space=pl.ANY)
    vm = pl.BlockSpec(memory_space=pltpu.VMEM)
    dma = pltpu.SemaphoreType.DMA
    return pl.pallas_call(
        functools.partial(wgrad_kernel, (tokens, dim, width, sub)),
        in_specs=[hbm] * 10 + [vm] * 2,
        out_specs=[vm] * 5 + [hbm] * 2,
        out_shape=[jax.ShapeDtypeStruct(a, F32) for a in (
            (shard, dim), (shard, width // 2), (shard, width // 2), (shard, dim), (1, dim))] + [jax.ShapeDtypeStruct((tokens, dim), BF16)] * 2,
        scratch_shapes=[
            pltpu.VMEM((2, tokens, dim), BF16),
            pltpu.VMEM((2, tokens, width), BF16),
            pltpu.VMEM((2, 4, 2, dim // 8, width), F32),
            pltpu.VMEM((2, 4, dim // 8, width), F32),
            pltpu.VMEM(part.shape[1:], F32), dma((2,)),
            pltpu.VMEM((4, 1, dim), F32),
            pltpu.VMEM((dim, dim), BF16),
            pltpu.VMEM((dim, width), BF16),
            *[pltpu.VMEM((2, BLOCK, c), BF16) for c in (dim, dim, dim, width, dim)],
            dma((2 + n,)), dma((4,)), dma((4, 2)), dma((2,)),
            *[pltpu.VMEM((3, 8, sub, c[2]), F32) for c in chunks],
            *[pltpu.VMEM((3, k, sub, c[2]), F32) for c in chunks for k in (4, 2, 1)],
            *[dma((n,))] * 2, *[dma((n, 3, 3))] * 2, *[dma((4,))] * 2,
            pltpu.SemaphoreType.REGULAR,
        ],
        compiler_params=pltpu.CompilerParams(collective_id=1, has_side_effects=True, vmem_limit_bytes=60 * 2 ** 20),
        cost_estimate=pl.CostEstimate(flops=2 * tokens * dim * (2 * dim + width), bytes_accessed=30 * 2 ** 20,
                                      transcendentals=0),
    )(o, dy, r, dq, dkv, x, w_o, w_a, w_b, w_kv, gain, part)


def gather_kernel(shapes, x_hbm, dy_hbm, wq_hbm, wk_hbm, wv_hbm, wo_hbm, gain_ref, pos_ref, freq_ref,
                  r_hbm, o_hbm, dq_hbm, wkv_hbm, wa_hbm, wb_hbm, wf_hbm, gain_out, dkv_out, part_out,
                  x, dy, r, q, do, kvo, kvx, wkv, wa, wb, wo, gbuf, grow, px, cos_ref, sin_ref, pcol,
                  mask, p_s, ds_s, mine_kv, snd, rcv, eg, ercv, eh, er1, er2,
                  load_sem, out_sem, blk_sem, ici_send, ici_recv, fwd_send, fwd_recv, own_send, own_recv,
                  g_send, g_recv, kv_send, kv_recv, dkv_send, dkv_recv,
                  ed_send, ed_recv, ei_send, ei_recv, credit):
    n_seq, rows, dim, n_kv = shapes
    bits, peers = place()
    by, bx, bc, bz = (bits[a] for a in 'yxcz')
    shard = dim // 16
    third, mid = shard // 3, shard // len(SLIM)
    hq = dim // 2
    groups = n_kv // HEAD
    gsize = dim // HEAD // groups
    fast = COLORS
    slim = SLIM
    pieces = [(wkv, fast), (wo, fast), (wa, slim), (wb, slim)]

    loads = []

    def load(src, dst):
        c = pltpu.make_async_copy(src, dst, load_sem.at[len(loads)])
        c.start()
        loads.append(c)
        return len(loads) - 1

    mine = lambda ref: ref.at[by, bx, bc, bz]
    for c in range(3):
        for g in range(n_kv // HEAD):
            hc = slice(g * HEAD, (g + 1) * HEAD)
            rws = span_of(c, third)
            for j, w_hbm in enumerate((wk_hbm, wv_hbm)):
                oc = slice((2 * g + j) * HEAD, (2 * g + j + 1) * HEAD)
                load(w_hbm.at[rws, hc], wkv.at[by, bx, bc, bz, c, :, oc])
    n_first = len(loads)
    for c in range(3):
        load(wo_hbm.at[span_of(c, third), :], wo.at[by, bx, bc, bz, c])
    for c in range(len(SLIM)):
        rws = span_of(c, mid)
        load(wq_hbm.at[rws, :hq], wa.at[by, bx, bc, bz, c])
        load(wq_hbm.at[rws, hq:], wb.at[by, bx, bc, bz, c])
    n_all = len(loads)
    l_x = load(x_hbm, x)
    l_dy = load(dy_hbm, dy)
    gbuf[by, bx, bc, bz] = jnp.zeros((1, HEAD), F32)
    gbuf[by, bx, bc, bz, :, :shard] = gain_ref[...]
    meet(peers)

    def region(p, c, f, flip):
        ref, order = pieces[p][0], pieces[p][1][c]
        idx = []
        for a in 'yxcz':
            if a in order[:f]:
                idx.append(slice(None))
            elif a == order[f] and flip:
                idx.append(1 - bits[a])
            else:
                idx.append(bits[a])
        return ref.at[idx[0], idx[1], idx[2], idx[3], c]

    def ici(p, c, f):
        s = region(p, c, f, False)
        return pltpu.make_async_remote_copy(s, s, ici_send.at[p, c, f], ici_recv.at[p, c, f],
                                            device_id=peers[pieces[p][1][c][f]], device_id_type=MESH)

    def fwd(p, c, f):
        s = region(p, c, f, True)
        return pltpu.make_async_remote_copy(s, s, fwd_send.at[p, c, f], fwd_recv.at[p, c, f],
                                            device_id=peers['c'], device_id_type=MESH)

    def own(p):
        s = mine(pieces[p][0])
        return pltpu.make_async_remote_copy(s, s, own_send.at[p], own_recv.at[p],
                                            device_id=peers['c'], device_id_type=MESH)

    def begin(p):
        for c in range(len(pieces[p][1])):
            ici(p, c, 0).start()
        own(p).start()

    def advance(p, f):
        for c in range(len(pieces[p][1])):
            ici(p, c, f).wait()
            if f < 2:
                ici(p, c, f + 1).start()
            fwd(p, c, f).start()

    def settle(p):
        own(p).wait()
        for c in range(len(pieces[p][1])):
            for f in range(3):
                fwd(p, c, f).wait()

    def gain_copy(i):
        s = (gbuf.at[by, bx, bc, bz], gbuf.at[by, bx, :, bz], gbuf.at[by, bx], gbuf.at[by])[i]
        return pltpu.make_async_remote_copy(s, s, g_send.at[i], g_recv.at[i],
                                            device_id=peers['czxy'[i]], device_id_type=MESH)

    def kv_copy(i):
        return pltpu.make_async_remote_copy(kvo.at[i], kvx.at[i], kv_send.at[i], kv_recv.at[i],
                                            device_id=peers['z'], device_id_type=MESH)

    def px_copy():
        return pltpu.make_async_remote_copy(pos_ref, px, kv_send.at[n_seq], kv_recv.at[n_seq],
                                            device_id=peers['z'], device_id_type=MESH)

    def hop(i):
        gain_copy(i).wait()
        gain_copy(i + 1).start()

    gain_copy(0).start()
    for i in range(n_first):
        loads[i].wait()
    begin(0)
    px_copy().start()
    for i in range(n_first, n_all):
        loads[i].wait()
    for p in (1, 2, 3):
        begin(p)
    hop(0)

    def tables(i):
        rs = span(i, rows)
        row = pos_ref[pl.ds(i, 1), :]
        col = jnp.transpose(jnp.broadcast_to(row.astype(F32), (HEAD, rows)))
        pcol[rs, :] = col
        ang = col * freq_ref[...]
        lane = lax.broadcasted_iota(jnp.int32, (rows, HEAD), 1)
        cos_ref[rs, :] = jnp.cos(ang)
        sn = jnp.sin(ang)
        sin_ref[rs, :] = jnp.where(lane < HEAD // 2, -sn, sn)

    mid_seq = n_seq // 2
    loop(0, mid_seq, tables)
    hop(1)
    advance(0, 0)
    advance(1, 0)
    loop(mid_seq, n_seq, tables)
    hop(2)
    advance(0, 1)
    advance(1, 1)
    gain_copy(3).wait()
    advance(2, 0)
    lane = lax.broadcasted_iota(jnp.int32, (8, HEAD), 1)
    for b in range(dim // HEAD):
        acc = jnp.zeros((8, HEAD), F32)
        for sh, at in enumerate(np.ndindex(2, 2, 2, 2)):
            lo = shard * sh - HEAD * b
            if lo >= HEAD or lo + shard <= 0:
                continue
            row = jnp.broadcast_to(gbuf[at], (8, HEAD))
            row = pltpu.roll(row, lo % HEAD, 1) if lo % HEAD else row
            acc = jnp.where((lane >= lo) & (lane < lo + shard), row, acc)
        grow[:, b * HEAD:(b + 1) * HEAD] = acc
    gain_out[...] = grow[0:1, :]
    loads[l_x].wait()

    def norm(i):
        rs = span(i, rows // 2)
        xf = x[rs, :].astype(F32)
        inv = lax.rsqrt(average(xf * xf) + EPS)
        r[rs, :] = (xf * inv * grow[0:1, :]).astype(BF16)

    loop(0, 2 * n_seq, norm)
    puts = []

    def put(src, dst):
        c = pltpu.make_async_copy(src, dst, out_sem.at[len(puts)])
        c.start()
        puts.append(c)

    put(r, r_hbm)
    advance(0, 2)
    advance(3, 0)
    settle(0)
    put(wkv, wkv_hbm)

    def kv_proj(i):
        rs = span(i, rows)
        kv = dot(r[rs, :], wkv[...].reshape(dim, 2 * n_kv))
        for g in range(0, 2 * n_kv // HEAD, 2):
            kvo[i, :, lanes(g)] = rope(kv[:, lanes(g)], cos_ref[rs, :], sin_ref[rs, :]).astype(BF16)
            kvo[i, :, lanes(g + 1)] = kv[:, lanes(g + 1)].astype(BF16)
        kv_copy(i).start()

    loop(0, mid_seq, kv_proj)
    advance(1, 2)
    loop(mid_seq, n_seq, kv_proj)
    advance(2, 1)
    settle(1)
    put(wo, wf_hbm)
    loads[l_dy].wait()

    def do_proj(i):
        rs = span(i, rows)
        do[rs, :] = dot(dy[rs, :], wo[...].reshape(dim, dim), NT).astype(BF16)

    def q_proj(half):
        def body(i):
            rs = span(i, rows)
            res = dot(r[rs, :], (wa, wb)[half][...].reshape(dim, hq))
            for h in range(hq // HEAD):
                q[rs, lanes(half * (hq // HEAD) + h)] = rope(res[:, lanes(h)], cos_ref[rs, :], sin_ref[rs, :]).astype(BF16)
        return body

    def dkv_copy(t):
        return pltpu.make_async_remote_copy(snd.at[t], rcv.at[t], dkv_send.at[t], dkv_recv.at[t],
                                            device_id=peers['z'], device_id_type=MESH)

    def blk_out(g, i):
        rs, hc = span(i, rows), pl.ds(g * gsize * HEAD, gsize * HEAD)
        return [pltpu.make_async_copy(src.at[rs, hc], dst.at[rs, hc], blk_sem.at[j, g * n_seq + i])
                for j, (src, dst) in enumerate(((dy, o_hbm), (x, dq_hbm)))]

    def attend(g):
        def body(i):
            if g == 0:
                kv_copy(i).wait()
            rs = span(i, rows)
            pq = pcol[rs, :]
            for j, ref in enumerate((pos_ref, px)):
                key = ref[pl.ds(i, 1), :].astype(F32)
                for b in range(rows // HEAD):
                    mask[:, lanes(j * (rows // HEAD) + b)] = jnp.where(key[:, lanes(b)] <= pq, 0.0, NEG)
            cos2, sin2 = cos_ref[rs, :], sin_ref[rs, :]
            k, v = (jnp.concatenate([kvo[i, :, lanes(j)], kvx[i, :, lanes(j)]], axis=0) for j in (2 * g, 2 * g + 1))
            heads = [lanes(g * gsize + h) for h in range(gsize)]
            for h, hc in enumerate(heads):
                hrow = span_of(h, rows)
                qh, doh = q[rs, hc], do[rs, hc]
                s = dot(qh, k, NT) * (SCALE * LOG2E) + mask[...]
                m = jnp.max(s, axis=1, keepdims=True)
                e = jnp.exp2(s - m)
                rl = 1.0 / total(e)
                o = (dot(e.astype(BF16), v) * rl).astype(BF16)
                dy[rs, hc] = o
                delta = total(doh.astype(F32) * o.astype(F32))
                p = e * rl
                p_s[hrow, :] = p.astype(BF16)
                ds = (p * (dot(doh, v, NT) - delta)).astype(BF16)
                ds_s[hrow, :] = ds
                x[rs, hc] = unrope(dot(ds, k) * SCALE, cos2, sin2).astype(BF16)
            do6 = jnp.concatenate([do[rs, hc] for hc in heads], axis=0)
            q6 = jnp.concatenate([q[rs, hc] for hc in heads], axis=0)
            dk = dot(ds_s[...], q6, TN) * SCALE
            dv = dot(p_s[...], do6, TN)
            t = g * n_seq + i
            for j, val in enumerate((dk, dv)):
                mine_kv[t, :, lanes(j)] = val[:rows]
                snd[t, :, lanes(j)] = val[rows:]
            dkv_copy(t).start()
            for c in blk_out(g, i):
                c.start()
        return body

    seg = dim // 4
    early = ('xy', 'yx')

    def e_swap(t):
        return pltpu.make_async_remote_copy(eg.at[:, 1 - bc], ercv, ed_send.at[t], ed_recv.at[t],
                                            device_id=peers['c'], device_id_type=MESH)

    def e_ici(t, c, p):
        b1, b2 = (bits[a] for a in early[c])
        src = (eh.at[t, c, 1 - b1], eh.at[t, c, b1, 1 - b2])[p]
        return pltpu.make_async_remote_copy(src, (er1, er2)[p].at[t, c], ei_send.at[t, c, p], ei_recv.at[t, c, p],
                                            device_id=peers[early[c][p]], device_id_type=MESH)

    def e_compute(t):
        def body(yx):
            res = dot(r[:, span(yx, seg)], x[:, span_of(t, EARLY)], TN)
            eg[yx, 0] = res[:seg // 2]
            eg[yx, 1] = res[seg // 2:]
        loop(0, 4, body)
        if t:
            pl.semaphore_wait(credit, 1)
        e_swap(t).start()

    def e_fold(t):
        e_swap(t).wait()
        for yy, xx, zz, c in np.ndindex(2, 2, 2, 2):
            rws = pl.ds(zz * shard + c * mid, mid)
            i1, i2 = (yy, xx) if early[c] == 'yx' else (xx, yy)
            eh[t, c, i1, i2, zz] = eg[yy * 2 + xx, bc, rws] + ercv[yy * 2 + xx, rws]
        for c in range(2):
            e_ici(t, c, 0).start()
        if t + 1 < hq // EARLY:
            pl.semaphore_signal(credit, inc=1, device_id=peers['c'], device_id_type=MESH)

    def e_reduce(t, p):
        for c in range(2):
            b1, b2 = (bits[a] for a in early[c])
            e_ici(t, c, p).wait()
            if p == 0:
                for j in range(2):
                    eh[t, c, b1, j] = eh[t, c, b1, j] + er1[t, c, j]
                e_ici(t, c, 1).start()
            else:
                part_out[:, span_of(c, mid), span_of(t, EARLY)] = eh[t, c, b1, b2] + er2[t, c]

    def gap(k):
        for p in (1, 0):
            if 0 <= k - 2 - p < hq // EARLY:
                e_reduce(k - 2 - p, p)
        if 0 <= k - 1 < hq // EARLY:
            e_fold(k - 1)
        if k < hq // EARLY:
            e_compute(k)

    def second(i):
        for k in range(hq // EARLY + 3):
            @pl.when(i == k)
            def _(k=k):
                gap(k)
        attend(1)(i)

    def finish(g):
        def body(i):
            t = g * n_seq + i
            rs = span(i, rows)
            dkv_copy(t).wait()
            tot = mine_kv[t] + rcv[t]
            dkv_out[rs, lanes(2 * g)] = unrope(tot[:, :HEAD], cos_ref[rs, :], sin_ref[rs, :]).astype(BF16)
            dkv_out[rs, lanes(2 * g + 1)] = tot[:, HEAD:].astype(BF16)
            for c in blk_out(g, i):
                c.wait()
        return body

    loop(0, mid_seq, do_proj)
    advance(3, 1)
    advance(2, 2)
    loop(mid_seq, n_seq, do_proj)
    settle(2)
    put(wa, wa_hbm)
    loop(0, n_seq, q_proj(0))
    px_copy().wait()

    def first(i):
        attend(0)(i)

        @pl.when(i == mid_seq - 1)
        def _():
            advance(3, 2)

    loop(0, n_seq, first)
    settle(3)
    put(wb, wb_hbm)
    loop(0, n_seq, q_proj(1))
    assert groups == 2 and hq // EARLY + 3 <= n_seq and hq == gsize * HEAD
    loop(0, n_seq, second)
    for g in range(groups):
        loop(0, n_seq, finish(g))
    for c in puts:
        c.wait()


def gather_project(x, dy, wq, wk, wv, wo, gain, pos):
    tokens, dim = x.shape
    n_seq, rows = pos.shape
    n_kv = wk.shape[1]
    shard = dim // 16
    steps = n_seq * n_kv // HEAD
    n_early = dim // 2 // EARLY
    half = HEAD // 2
    freq = np.float32(THETA) ** (-np.arange(half, dtype=np.float32) / half)
    freq = jnp.asarray(np.tile(freq, 2)[None])
    hbm = pl.BlockSpec(memory_space=pl.ANY)
    vm = pl.BlockSpec(memory_space=pltpu.VMEM)
    dma = pltpu.SemaphoreType.DMA
    sds = jax.ShapeDtypeStruct
    wshapes = [(2, 2, 2, 2, len(k), shard // len(k), c) for k, c in (
        (COLORS, 2 * n_kv), (SLIM, dim // 2), (SLIM, dim // 2), (COLORS, dim))]
    return pl.pallas_call(
        functools.partial(gather_kernel, (n_seq, rows, dim, n_kv)),
        in_specs=[hbm] * 6 + [vm] * 3,
        out_specs=[hbm] * 7 + [vm] * 3,
        out_shape=[sds((tokens, dim), BF16)] * 3 + [sds(w, BF16) for w in wshapes] + [
            sds((1, dim), F32), sds((tokens, 2 * n_kv), BF16), sds((2, shard, dim // 2), F32)],
        scratch_shapes=[pltpu.VMEM((tokens, dim), BF16)] * 5 + [
            pltpu.VMEM((n_seq, rows, 2 * n_kv), BF16),
            pltpu.VMEM((n_seq, rows, 2 * n_kv), BF16),
            *[pltpu.VMEM(w, BF16) for w in wshapes],
            pltpu.VMEM((2, 2, 2, 2, 1, HEAD), F32),
            pltpu.VMEM((8, dim), F32),
            pltpu.VMEM((n_seq, rows), jnp.int32),
            *[pltpu.VMEM((tokens, HEAD), F32)] * 3,
            pltpu.VMEM((rows, 2 * rows), F32),
            *[pltpu.VMEM((dim // n_kv * rows, 2 * rows), BF16)] * 2,
            *[pltpu.VMEM((steps, rows, 2 * HEAD), F32)] * 3,
            pltpu.VMEM((4, 2, dim // 8, EARLY), F32),
            pltpu.VMEM((4, dim // 8, EARLY), F32),
            *[pltpu.VMEM((n_early, 2) + k + (shard // 2, EARLY), F32) for k in ((2, 2, 2), (2, 2), (2,))],
            dma((6 * n_kv // HEAD + 5 + 2 * len(SLIM),)), dma((6,)), dma((2, steps)), *[dma((4, 3, 3))] * 4,
            *[dma((4,))] * 4, *[dma((n_seq + 1,))] * 2, *[dma((steps,))] * 2,
            *[dma((n_early,))] * 2, *[dma((n_early, 2, 2))] * 2, pltpu.SemaphoreType.REGULAR,
        ],
        compiler_params=pltpu.CompilerParams(collective_id=2, has_side_effects=True, vmem_limit_bytes=67043328),
        cost_estimate=pl.CostEstimate(flops=2 * tokens * dim * (2 * dim + 2 * n_kv), bytes_accessed=40 * 2 ** 20,
                                      transcendentals=0),
    )(x, dy, wq, wk, wv, wo, gain[None], pos, freq)


def solution(mesh):
    cp_size = mesh.shape['cp']

    def shard_fn(hidden, tok_pos, grad_out, norm_gain, w_query, w_key, w_value, w_out):
        n_seq, rows, dim = hidden.shape
        tokens = n_seq * rows
        n_q = w_query.shape[1]
        n_kv = w_key.shape[1]
        groups = n_kv // HEAD
        x16 = hidden.reshape(tokens, dim)
        dy = grad_out.reshape(tokens, dim)
        r, o, dq, w_kv, w_a, w_b, w_o, gain, dkv, part = gather_project(
            x16, dy, w_query, w_key, w_value, w_out, norm_gain, tok_pos)
        w_a, w_b, w_kv, w_o = (w.reshape(dim, -1) for w in (w_a, w_b, w_kv, w_o))
        g_wq, g_wk, g_wv, g_wo, gg, result, grad_hidden = wgrad(o, dy, r, dq, dkv, x16, w_o, w_a, w_b, w_kv, gain, part)
        shard = lax.axis_index('fsdp') * cp_size + lax.axis_index('cp')
        g_gain = lax.dynamic_slice(gg[0], (shard * norm_gain.shape[0],), norm_gain.shape)
        return result.reshape(hidden.shape), grad_hidden.reshape(hidden.shape), g_wq, g_wk, g_wv, g_wo, g_gain

    row = P('fsdp', 'cp', None)
    pos_spec = P('fsdp', 'cp')
    w = P(AXES, None)
    g = P(AXES)
    return jax.shard_map(shard_fn, mesh=mesh, in_specs=(row, pos_spec, row, g, w, w, w, w),
                         out_specs=(row, row, w, w, w, w, g), check_vma=False)
```

```python
import functools
import math

import jax
import jax.numpy as jnp
import numpy as np
from jax import lax
from jax.experimental import pallas as pl
from jax.experimental.pallas import tpu as pltpu
from jax.sharding import PartitionSpec as P

HEAD = 128
THETA = 1000000.0
EPS = 1e-5
NEG = -1e30
SCALE = HEAD ** -0.5
LOG2E = math.log2(math.e)
AXES = ('fsdp', 'cp')
MESH = pl.DeviceIdType.MESH
F32 = jnp.float32
BF16 = jnp.bfloat16
NT = (((1,), (1,)), ((), ()))
TN = (((0,), (0,)), ((), ()))
NN = (((1,), (0,)), ((), ()))


def dot(a, b, dims=NN):
    return lax.dot_general(a, b, dims, preferred_element_type=F32)


def loop(lo, hi, body):
    def run(i, carry):
        body(i)
        return carry
    lax.fori_loop(lo, hi, run, None)


def total(a):
    return jnp.sum(a, axis=1, keepdims=True)


def average(a):
    return jnp.mean(a, axis=1, keepdims=True)


def span(i, size):
    return pl.ds(pl.multiple_of(i * size, size), size)


def span_of(i, size):
    return slice(i * size, (i + 1) * size)


def lanes(i):
    return span_of(i, HEAD)


def rope(v, cos2, sin2):
    return v * cos2 + pltpu.roll(v, HEAD // 2, 1) * sin2


def unrope(v, cos2, sin2):
    return v * cos2 - pltpu.roll(v, HEAD // 2, 1) * sin2


COLORS = ('xyz', 'yzx', 'zxy')
SLIM = ('zxy', 'zyx')
BLOCK = 256
EARLY = 256


def place():
    f = lax.axis_index('fsdp')
    z = lax.axis_index('cp')
    bits = {'y': f // 4, 'x': (f // 2) % 2, 'c': f % 2, 'z': z}
    peers = {'y': {'fsdp': f + 4 - 8 * bits['y']}, 'x': {'fsdp': f + 2 - 4 * bits['x']},
             'c': {'fsdp': f + 1 - 2 * bits['c']}, 'z': {'cp': 1 - z}}
    return bits, peers


def meet(peers):
    barrier = pltpu.get_barrier_semaphore()
    for a in 'cxyz':
        pl.semaphore_signal(barrier, inc=1, device_id=peers[a], device_id_type=MESH)
    pl.semaphore_wait(barrier, 4)


def chunk_list(dim, width):
    half = width // 2
    out = [('o', 0, half), ('o', half, half)]
    out += [('o', c, width) for c in range(width, dim, width)]
    out += [('q', dim // 2, half), ('q', dim - width, width)]
    return out + [('kv', 0, half), ('kv', half, half)]


def wgrad_kernel(shapes, o_hbm, dy_hbm, r_hbm, dq_hbm, dkv_hbm, x_hbm, wo_hbm, wa_hbm, wb_hbm, wkv_hbm, gain_ref, part_ref,
                 gwq_ref, gwk_ref, gwv_ref, gwo_ref, gg_ref, res_hbm, gh_hbm,
                 lhs, rhs, g, rcv_a, part_rcv, part_sem, gain_rcv, wo, wkv, xb, dyb, dqb, dkvb, outb,
                 load_sem, w_sem, blk_sem, out_sem, *rest):
    tokens, dim, width, sub = shapes
    bits, peers = place()
    core = bits['c']
    chunks = chunk_list(dim, width)
    n = len(chunks)
    h, rcv = rest[:n], [rest[n + t * 3:n + t * 3 + 3] for t in range(n)]
    d2d_send, d2d_recv, ici_send, ici_recv, gain_send, gain_recv, credit = rest[4 * n:]
    seg = dim // 4
    half = seg // 2

    def load_lhs(i):
        return pltpu.make_async_copy((o_hbm, r_hbm)[i], lhs.at[i], load_sem.at[i])

    def load_rhs(t):
        kind, col, w = chunks[t]
        src = {'o': dy_hbm, 'q': dq_hbm, 'kv': dkv_hbm}[kind]
        return pltpu.make_async_copy(src.at[:, pl.ds(col, w)], rhs.at[t % 2, :, pl.ds(0, w)], load_sem.at[2 + t])

    load_lhs(0).start()
    load_rhs(0).start()
    load_lhs(1).start()
    load_rhs(1).start()
    hd = dim // 2
    w_loads = [pltpu.make_async_copy(a, b, w_sem.at[i]) for i, (a, b) in enumerate((
        (wo_hbm, wo), (wkv_hbm, wkv), (wa_hbm, lhs.at[0, :, pl.ds(0, hd)]), (wb_hbm, lhs.at[0, :, pl.ds(hd, hd)])))]
    w_loads[0].start()
    w_loads[1].start()
    n_blk = tokens // BLOCK

    def blk_loads(b, which):
        rs = pl.ds(pl.multiple_of(b * BLOCK, BLOCK), BLOCK)
        srcs = ((x_hbm, xb), (dy_hbm, dyb), (dq_hbm, dqb), (dkv_hbm, dkvb))
        return [pltpu.make_async_copy(srcs[k][0].at[rs, :], srcs[k][1].at[b % 2], blk_sem.at[k, b % 2])
                for k in which]

    def out_copy(dst, b):
        rs = pl.ds(pl.multiple_of(b * BLOCK, BLOCK), BLOCK)
        return pltpu.make_async_copy(outb.at[b % 2], dst.at[rs, :], out_sem.at[b % 2])

    def blocks(lo, hi, which, dst, body):
        def run(b, carry):
            for c in blk_loads(b, which):
                c.wait()

            @pl.when(b + 1 < n_blk)
            def _():
                for c in blk_loads(b + 1, which):
                    c.start()

            @pl.when(b >= 2)
            def _():
                out_copy(dst, b - 2).wait()

            outb[b % 2] = body(b)
            out_copy(dst, b).start()
            return carry
        lax.fori_loop(lo, hi, run, 0)

    def res_body(b):
        rs = pl.ds(pl.multiple_of(b * BLOCK, BLOCK), BLOCK)
        return (xb[b % 2].astype(F32) + dot(lhs[0, rs, :], wo[...])).astype(BF16)

    def dr_body(b):
        xf = xb[b % 2].astype(F32)
        inv = lax.rsqrt(average(xf * xf) + EPS)
        xh = xf * inv
        dr = dot(dqb[b % 2], lhs[0], NT) + dot(dkvb[b % 2], wkv[...], NT)
        gg_ref[...] = gg_ref[...] + jnp.sum(dr * xh, axis=0, keepdims=True)
        a = dr * gain_ref[...]
        gx = inv * (a - xh * average(a * xh))
        return (dyb[b % 2].astype(F32) + gx).astype(BF16)

    for c in blk_loads(0, (0,)):
        c.start()
    meet(peers)

    def d2d(t):
        w = pl.ds(0, chunks[t][2])
        return pltpu.make_async_remote_copy(g.at[t % 2, :, 1 - core, :, w], rcv_a.at[t % 2, :, :, w], d2d_send.at[t], d2d_recv.at[t],
                                            device_id=peers['c'], device_id_type=MESH)

    def ici(t, c, p):
        b1, b2, b3 = (bits[a] for a in COLORS[c])
        if p == 0:
            src = h[t].at[c, pl.ds((1 - b1) * 4, 4)]
        elif p == 1:
            src = h[t].at[c, pl.ds(b1 * 4 + (1 - b2) * 2, 2)]
        else:
            src = h[t].at[c, pl.ds(b1 * 4 + b2 * 2 + (1 - b3), 1)]
        return pltpu.make_async_remote_copy(src, rcv[t][p].at[c], ici_send.at[t, c, p], ici_recv.at[t, c, p],
                                            device_id=peers[COLORS[c][p]], device_id_type=MESH)

    def compute(t):
        kind, _, w = chunks[t]
        li = int(kind != 'o')
        if t == 0 or (li and chunks[t - 1][0] == 'o'):
            load_lhs(li).wait()
        load_rhs(t).wait()

        def body(yx):
            res = dot(lhs[li, :, span(yx, seg)], rhs[t % 2, :, :w], TN)
            g[t % 2, yx, 0, :, :w] = res[:half]
            g[t % 2, yx, 1, :, :w] = res[half:]
        loop(0, 4, body)
        if t + 2 < n:
            load_rhs(t + 2).start()
        if t >= 2:
            pl.semaphore_wait(credit, 1)
        d2d(t).start()

    def fold(t):
        w = chunks[t][2]
        d2d(t).wait()
        for y, x, z, c in np.ndindex(2, 2, 2, 3):
            at = {'y': y, 'x': x, 'z': z}
            a1, a2, a3 = (at[a] for a in COLORS[c])
            rows = span_of(z * 3 + c, sub)
            h[t][c, a1 * 4 + a2 * 2 + a3] = g[t % 2, y * 2 + x, core, rows, :w] + rcv_a[t % 2, y * 2 + x, rows, :w]
        for c in range(3):
            ici(t, c, 0).start()
        if t + 2 < n:
            pl.semaphore_signal(credit, inc=1, device_id=peers['c'], device_id_type=MESH)

    def reduce(t, p):
        for c in range(3):
            b1, b2, b3 = (bits[a] for a in COLORS[c])
            ici(t, c, p).wait()
            k = (0, b1 * 4, b1 * 4 + b2 * 2, b1 * 4 + b2 * 2 + b3)[p + 1]
            if p < 2:
                for j in range(4 >> p):
                    h[t][c, k + j] = h[t][c, k + j] + rcv[t][p][c, j]
                ici(t, c, p + 1).start()
                continue
            kind, col, w = chunks[t]
            rws = span_of(c, sub)
            tot = h[t][c, k] + rcv[t][p][c, 0]
            if kind == 'kv':
                for j in range(w // HEAD):
                    b = col // HEAD + j
                    (gwk_ref, gwv_ref)[b % 2][rws, lanes(b // 2)] = tot[:, lanes(j)]
            else:
                (gwo_ref if kind == 'o' else gwq_ref)[rws, col:col + w] = tot

    gg_ref[...] = jnp.zeros_like(gg_ref)
    part_copy = pltpu.make_async_remote_copy(part_ref.at[1 - bits['z']], part_rcv, part_sem.at[0], part_sem.at[1],
                                             device_id=peers['z'], device_id_type=MESH)
    part_copy.start()

    def gain_copy(i):
        return pltpu.make_async_remote_copy(gg_ref, gain_rcv.at[i], gain_send.at[i], gain_recv.at[i],
                                            device_id=peers['cxyz'[i]], device_id_type=MESH)

    def flush(dst):
        out_copy(dst, n_blk - 2).wait()
        out_copy(dst, n_blk - 1).wait()

    every = (0, 1, 2, 3)
    third, fill = n_blk // 3, n_blk // 2
    for i in range(n + 4):
        if i < n:
            compute(i)
        if 0 <= i - 1 < n:
            fold(i - 1)
        for p in range(3):
            if 0 <= i - 2 - p < n:
                reduce(i - 2 - p, p)
        if 2 <= i < 4:
            if i == 2:
                w_loads[0].wait()
            blocks((i - 2) * fill, (i - 1) * fill, (0,), res_hbm, res_body)
            if i == 3:
                part_copy.wait()
                gwq_ref[:, :hd] = part_ref[bits['z']] + part_rcv[...]
                flush(res_hbm)
                for c in [*w_loads[2:], *blk_loads(0, every)]:
                    c.start()
        elif 4 <= i < 7:
            if i == 4:
                for c in w_loads[1:]:
                    c.wait()
            blocks((i - 4) * third, (i - 3) * third, every, gh_hbm, dr_body)
            if i == 6:
                flush(gh_hbm)
                gain_copy(0).start()
        elif 7 <= i < 11:
            gain_copy(i - 7).wait()
            gg_ref[...] = gg_ref[...] + gain_rcv[i - 7]
            if i < 10:
                gain_copy(i - 6).start()


def wgrad(o, dy, r, dq, dkv, x, w_o, w_a, w_b, w_kv, gain, part):
    tokens, dim = o.shape
    width = dkv.shape[1]
    shard = dim // 16
    sub = shard // 3
    chunks = chunk_list(dim, width)
    n = len(chunks)
    hbm = pl.BlockSpec(memory_space=pl.ANY)
    vm = pl.BlockSpec(memory_space=pltpu.VMEM)
    dma = pltpu.SemaphoreType.DMA
    return pl.pallas_call(
        functools.partial(wgrad_kernel, (tokens, dim, width, sub)),
        in_specs=[hbm] * 10 + [vm] * 2,
        out_specs=[vm] * 5 + [hbm] * 2,
        out_shape=[jax.ShapeDtypeStruct(a, F32) for a in (
            (shard, dim), (shard, width // 2), (shard, width // 2), (shard, dim), (1, dim))] + [jax.ShapeDtypeStruct((tokens, dim), BF16)] * 2,
        scratch_shapes=[
            pltpu.VMEM((2, tokens, dim), BF16),
            pltpu.VMEM((2, tokens, width), BF16),
            pltpu.VMEM((2, 4, 2, dim // 8, width), F32),
            pltpu.VMEM((2, 4, dim // 8, width), F32),
            pltpu.VMEM(part.shape[1:], F32), dma((2,)),
            pltpu.VMEM((4, 1, dim), F32),
            pltpu.VMEM((dim, dim), BF16),
            pltpu.VMEM((dim, width), BF16),
            *[pltpu.VMEM((2, BLOCK, c), BF16) for c in (dim, dim, dim, width, dim)],
            dma((2 + n,)), dma((4,)), dma((4, 2)), dma((2,)),
            *[pltpu.VMEM((3, 8, sub, c[2]), F32) for c in chunks],
            *[pltpu.VMEM((3, k, sub, c[2]), F32) for c in chunks for k in (4, 2, 1)],
            *[dma((n,))] * 2, *[dma((n, 3, 3))] * 2, *[dma((4,))] * 2,
            pltpu.SemaphoreType.REGULAR,
        ],
        compiler_params=pltpu.CompilerParams(collective_id=1, has_side_effects=True, vmem_limit_bytes=60 * 2 ** 20),
        cost_estimate=pl.CostEstimate(flops=2 * tokens * dim * (2 * dim + width), bytes_accessed=30 * 2 ** 20,
                                      transcendentals=0),
    )(o, dy, r, dq, dkv, x, w_o, w_a, w_b, w_kv, gain, part)


def gather_kernel(shapes, x_hbm, dy_hbm, wq_hbm, wk_hbm, wv_hbm, wo_hbm, gain_ref, pos_ref, freq_ref,
                  r_hbm, o_hbm, dq_hbm, wkv_hbm, wa_hbm, wb_hbm, wf_hbm, gain_out, dkv_out, part_out,
                  x, dy, r, q, do, kvo, kvx, wkv, wa, wb, wo, gbuf, grow, px, cos_ref, sin_ref, pcol,
                  mask, p_s, ds_s, mine_kv, snd, rcv, eg, ercv, eh, er1, er2,
                  load_sem, out_sem, blk_sem, ici_send, ici_recv, fwd_send, fwd_recv, own_send, own_recv,
                  g_send, g_recv, kv_send, kv_recv, dkv_send, dkv_recv,
                  ed_send, ed_recv, ei_send, ei_recv, credit):
    n_seq, rows, dim, n_kv = shapes
    bits, peers = place()
    by, bx, bc, bz = (bits[a] for a in 'yxcz')
    shard = dim // 16
    third, mid = shard // 3, shard // len(SLIM)
    hq = dim // 2
    groups = n_kv // HEAD
    gsize = dim // HEAD // groups
    fast = COLORS
    slim = SLIM
    pieces = [(wkv, fast), (wo, fast), (wa, slim), (wb, slim)]

    loads = []

    def load(src, dst):
        c = pltpu.make_async_copy(src, dst, load_sem.at[len(loads)])
        c.start()
        loads.append(c)
        return len(loads) - 1

    mine = lambda ref: ref.at[by, bx, bc, bz]
    for c in range(3):
        for g in range(n_kv // HEAD):
            hc = slice(g * HEAD, (g + 1) * HEAD)
            rws = span_of(c, third)
            for j, w_hbm in enumerate((wk_hbm, wv_hbm)):
                oc = slice((2 * g + j) * HEAD, (2 * g + j + 1) * HEAD)
                load(w_hbm.at[rws, hc], wkv.at[by, bx, bc, bz, c, :, oc])
    n_first = len(loads)
    for c in range(3):
        load(wo_hbm.at[span_of(c, third), :], wo.at[by, bx, bc, bz, c])
    for c in range(len(SLIM)):
        rws = span_of(c, mid)
        load(wq_hbm.at[rws, :hq], wa.at[by, bx, bc, bz, c])
        load(wq_hbm.at[rws, hq:], wb.at[by, bx, bc, bz, c])
    n_all = len(loads)
    l_x = load(x_hbm, x)
    l_dy = load(dy_hbm, dy)
    gbuf[by, bx, bc, bz] = jnp.zeros((1, HEAD), F32)
    gbuf[by, bx, bc, bz, :, :shard] = gain_ref[...]
    meet(peers)

    def region(p, c, f, flip):
        ref, order = pieces[p][0], pieces[p][1][c]
        idx = []
        for a in 'yxcz':
            if a in order[:f]:
                idx.append(slice(None))
            elif a == order[f] and flip:
                idx.append(1 - bits[a])
            else:
                idx.append(bits[a])
        return ref.at[idx[0], idx[1], idx[2], idx[3], c]

    def ici(p, c, f):
        s = region(p, c, f, False)
        return pltpu.make_async_remote_copy(s, s, ici_send.at[p, c, f], ici_recv.at[p, c, f],
                                            device_id=peers[pieces[p][1][c][f]], device_id_type=MESH)

    def fwd(p, c, f):
        s = region(p, c, f, True)
        return pltpu.make_async_remote_copy(s, s, fwd_send.at[p, c, f], fwd_recv.at[p, c, f],
                                            device_id=peers['c'], device_id_type=MESH)

    def own(p):
        s = mine(pieces[p][0])
        return pltpu.make_async_remote_copy(s, s, own_send.at[p], own_recv.at[p],
                                            device_id=peers['c'], device_id_type=MESH)

    def begin(p):
        for c in range(len(pieces[p][1])):
            ici(p, c, 0).start()
        own(p).start()

    def advance(p, f):
        for c in range(len(pieces[p][1])):
            ici(p, c, f).wait()
            if f < 2:
                ici(p, c, f + 1).start()
            fwd(p, c, f).start()

    def settle(p):
        own(p).wait()
        for c in range(len(pieces[p][1])):
            for f in range(3):
                fwd(p, c, f).wait()

    def gain_copy(i):
        s = (gbuf.at[by, bx, bc, bz], gbuf.at[by, bx, :, bz], gbuf.at[by, bx], gbuf.at[by])[i]
        return pltpu.make_async_remote_copy(s, s, g_send.at[i], g_recv.at[i],
                                            device_id=peers['czxy'[i]], device_id_type=MESH)

    def kv_copy(i):
        return pltpu.make_async_remote_copy(kvo.at[i], kvx.at[i], kv_send.at[i], kv_recv.at[i],
                                            device_id=peers['z'], device_id_type=MESH)

    def px_copy():
        return pltpu.make_async_remote_copy(pos_ref, px, kv_send.at[n_seq], kv_recv.at[n_seq],
                                            device_id=peers['z'], device_id_type=MESH)

    def hop(i):
        gain_copy(i).wait()
        gain_copy(i + 1).start()

    gain_copy(0).start()
    for i in range(n_first):
        loads[i].wait()
    begin(0)
    px_copy().start()
    for i in range(n_first, n_all):
        loads[i].wait()
    for p in (1, 2, 3):
        begin(p)
    hop(0)

    def tables(i):
        rs = span(i, rows)
        row = pos_ref[pl.ds(i, 1), :]
        col = jnp.transpose(jnp.broadcast_to(row.astype(F32), (HEAD, rows)))
        pcol[rs, :] = col
        ang = col * freq_ref[...]
        lane = lax.broadcasted_iota(jnp.int32, (rows, HEAD), 1)
        cos_ref[rs, :] = jnp.cos(ang)
        sn = jnp.sin(ang)
        sin_ref[rs, :] = jnp.where(lane < HEAD // 2, -sn, sn)

    mid_seq = n_seq // 2
    loop(0, mid_seq, tables)
    hop(1)
    advance(0, 0)
    advance(1, 0)
    loop(mid_seq, n_seq, tables)
    hop(2)
    advance(0, 1)
    advance(1, 1)
    gain_copy(3).wait()
    advance(2, 0)
    lane = lax.broadcasted_iota(jnp.int32, (8, HEAD), 1)
    for b in range(dim // HEAD):
        acc = jnp.zeros((8, HEAD), F32)
        for sh, at in enumerate(np.ndindex(2, 2, 2, 2)):
            lo = shard * sh - HEAD * b
            if lo >= HEAD or lo + shard <= 0:
                continue
            row = jnp.broadcast_to(gbuf[at], (8, HEAD))
            row = pltpu.roll(row, lo % HEAD, 1) if lo % HEAD else row
            acc = jnp.where((lane >= lo) & (lane < lo + shard), row, acc)
        grow[:, b * HEAD:(b + 1) * HEAD] = acc
    gain_out[...] = grow[0:1, :]
    loads[l_x].wait()

    def norm(i):
        rs = span(i, rows // 2)
        xf = x[rs, :].astype(F32)
        inv = lax.rsqrt(average(xf * xf) + EPS)
        r[rs, :] = (xf * inv * grow[0:1, :]).astype(BF16)

    loop(0, 2 * n_seq, norm)
    puts = []

    def put(src, dst):
        c = pltpu.make_async_copy(src, dst, out_sem.at[len(puts)])
        c.start()
        puts.append(c)

    put(r, r_hbm)
    advance(0, 2)
    advance(3, 0)
    settle(0)
    put(wkv, wkv_hbm)

    def kv_proj(i):
        rs = span(i, rows)
        kv = dot(r[rs, :], wkv[...].reshape(dim, 2 * n_kv))
        for g in range(0, 2 * n_kv // HEAD, 2):
            kvo[i, :, lanes(g)] = rope(kv[:, lanes(g)], cos_ref[rs, :], sin_ref[rs, :]).astype(BF16)
            kvo[i, :, lanes(g + 1)] = kv[:, lanes(g + 1)].astype(BF16)
        kv_copy(i).start()

    loop(0, mid_seq, kv_proj)
    advance(1, 2)
    loop(mid_seq, n_seq, kv_proj)
    advance(2, 1)
    settle(1)
    put(wo, wf_hbm)
    loads[l_dy].wait()

    def do_proj(i):
        rs = span(i, rows)
        do[rs, :] = dot(dy[rs, :], wo[...].reshape(dim, dim), NT).astype(BF16)

    def q_proj(half):
        def body(i):
            rs = span(i, rows)
            res = dot(r[rs, :], (wa, wb)[half][...].reshape(dim, hq))
            for h in range(hq // HEAD):
                q[rs, lanes(half * (hq // HEAD) + h)] = rope(res[:, lanes(h)], cos_ref[rs, :], sin_ref[rs, :]).astype(BF16)
        return body

    def dkv_copy(t):
        return pltpu.make_async_remote_copy(snd.at[t], rcv.at[t], dkv_send.at[t], dkv_recv.at[t],
                                            device_id=peers['z'], device_id_type=MESH)

    def blk_out(g, i):
        rs, hc = span(i, rows), pl.ds(g * gsize * HEAD, gsize * HEAD)
        return [pltpu.make_async_copy(src.at[rs, hc], dst.at[rs, hc], blk_sem.at[j, g * n_seq + i])
                for j, (src, dst) in enumerate(((dy, o_hbm), (x, dq_hbm)))]

    def attend(g):
        def body(i):
            if g == 0:
                kv_copy(i).wait()
            rs = span(i, rows)
            pq = pcol[rs, :]
            for j, ref in enumerate((pos_ref, px)):
                key = ref[pl.ds(i, 1), :].astype(F32)
                for b in range(rows // HEAD):
                    mask[:, lanes(j * (rows // HEAD) + b)] = jnp.where(key[:, lanes(b)] <= pq, 0.0, NEG)
            cos2, sin2 = cos_ref[rs, :], sin_ref[rs, :]
            k, v = (jnp.concatenate([kvo[i, :, lanes(j)], kvx[i, :, lanes(j)]], axis=0) for j in (2 * g, 2 * g + 1))
            heads = [lanes(g * gsize + h) for h in range(gsize)]

            def products(hc):
                return dot(q[rs, hc], k, NT), dot(do[rs, hc], v, NT)

            coming = products(heads[0])
            for h, hc in enumerate(heads):
                hrow = span_of(h, rows)
                doh = do[rs, hc]
                raw, dp = coming
                s = raw * (SCALE * LOG2E) + mask[...]
                if hc != heads[-1]:
                    coming = products(heads[h + 1])
                m = jnp.max(s, axis=1, keepdims=True)
                e = jnp.exp2(s - m)
                rl = 1.0 / total(e)
                o = (dot(e.astype(BF16), v) * rl).astype(BF16)
                dy[rs, hc] = o
                delta = total(doh.astype(F32) * o.astype(F32))
                p = e * rl
                p_s[hrow, :] = p.astype(BF16)
                ds = (p * (dp - delta)).astype(BF16)
                ds_s[hrow, :] = ds
                x[rs, hc] = unrope(dot(ds, k) * SCALE, cos2, sin2).astype(BF16)
            do6 = jnp.concatenate([do[rs, hc] for hc in heads], axis=0)
            q6 = jnp.concatenate([q[rs, hc] for hc in heads], axis=0)
            dk = dot(ds_s[...], q6, TN) * SCALE
            dv = dot(p_s[...], do6, TN)
            t = g * n_seq + i
            for j, val in enumerate((dk, dv)):
                mine_kv[t, :, lanes(j)] = val[:rows]
                snd[t, :, lanes(j)] = val[rows:]
            dkv_copy(t).start()
            for c in blk_out(g, i):
                c.start()
        return body

    seg = dim // 4
    early = ('xy', 'yx')

    def e_swap(t):
        return pltpu.make_async_remote_copy(eg.at[:, 1 - bc], ercv, ed_send.at[t], ed_recv.at[t],
                                            device_id=peers['c'], device_id_type=MESH)

    def e_ici(t, c, p):
        b1, b2 = (bits[a] for a in early[c])
        src = (eh.at[t, c, 1 - b1], eh.at[t, c, b1, 1 - b2])[p]
        return pltpu.make_async_remote_copy(src, (er1, er2)[p].at[t, c], ei_send.at[t, c, p], ei_recv.at[t, c, p],
                                            device_id=peers[early[c][p]], device_id_type=MESH)

    def e_compute(t):
        def body(yx):
            res = dot(r[:, span(yx, seg)], x[:, span_of(t, EARLY)], TN)
            eg[yx, 0] = res[:seg // 2]
            eg[yx, 1] = res[seg // 2:]
        loop(0, 4, body)
        if t:
            pl.semaphore_wait(credit, 1)
        e_swap(t).start()

    def e_fold(t):
        e_swap(t).wait()
        for yy, xx, zz, c in np.ndindex(2, 2, 2, 2):
            rws = pl.ds(zz * shard + c * mid, mid)
            i1, i2 = (yy, xx) if early[c] == 'yx' else (xx, yy)
            eh[t, c, i1, i2, zz] = eg[yy * 2 + xx, bc, rws] + ercv[yy * 2 + xx, rws]
        for c in range(2):
            e_ici(t, c, 0).start()
        if t + 1 < hq // EARLY:
            pl.semaphore_signal(credit, inc=1, device_id=peers['c'], device_id_type=MESH)

    def e_reduce(t, p):
        for c in range(2):
            b1, b2 = (bits[a] for a in early[c])
            e_ici(t, c, p).wait()
            if p == 0:
                for j in range(2):
                    eh[t, c, b1, j] = eh[t, c, b1, j] + er1[t, c, j]
                e_ici(t, c, 1).start()
            else:
                part_out[:, span_of(c, mid), span_of(t, EARLY)] = eh[t, c, b1, b2] + er2[t, c]

    def gap(k):
        for p in (1, 0):
            if 0 <= k - 2 - p < hq // EARLY:
                e_reduce(k - 2 - p, p)
        if 0 <= k - 1 < hq // EARLY:
            e_fold(k - 1)
        if k < hq // EARLY:
            e_compute(k)

    def second(i):
        for k in range(hq // EARLY + 3):
            @pl.when(i == k)
            def _(k=k):
                gap(k)
        attend(1)(i)

    def finish(g):
        def body(i):
            t = g * n_seq + i
            rs = span(i, rows)
            dkv_copy(t).wait()
            tot = mine_kv[t] + rcv[t]
            dkv_out[rs, lanes(2 * g)] = unrope(tot[:, :HEAD], cos_ref[rs, :], sin_ref[rs, :]).astype(BF16)
            dkv_out[rs, lanes(2 * g + 1)] = tot[:, HEAD:].astype(BF16)
            for c in blk_out(g, i):
                c.wait()
        return body

    loop(0, mid_seq, do_proj)
    advance(3, 1)
    advance(2, 2)
    loop(mid_seq, n_seq, do_proj)
    settle(2)
    put(wa, wa_hbm)
    loop(0, n_seq, q_proj(0))
    px_copy().wait()

    def first(i):
        attend(0)(i)

        @pl.when(i == mid_seq - 1)
        def _():
            advance(3, 2)

    loop(0, n_seq, first)
    settle(3)
    put(wb, wb_hbm)
    loop(0, n_seq, q_proj(1))
    assert groups == 2 and hq // EARLY + 3 <= n_seq and hq == gsize * HEAD
    loop(0, n_seq, second)
    for g in range(groups):
        loop(0, n_seq, finish(g))
    for c in puts:
        c.wait()


def gather_project(x, dy, wq, wk, wv, wo, gain, pos):
    tokens, dim = x.shape
    n_seq, rows = pos.shape
    n_kv = wk.shape[1]
    shard = dim // 16
    steps = n_seq * n_kv // HEAD
    n_early = dim // 2 // EARLY
    half = HEAD // 2
    freq = np.float32(THETA) ** (-np.arange(half, dtype=np.float32) / half)
    freq = jnp.asarray(np.tile(freq, 2)[None])
    hbm = pl.BlockSpec(memory_space=pl.ANY)
    vm = pl.BlockSpec(memory_space=pltpu.VMEM)
    dma = pltpu.SemaphoreType.DMA
    sds = jax.ShapeDtypeStruct
    wshapes = [(2, 2, 2, 2, len(k), shard // len(k), c) for k, c in (
        (COLORS, 2 * n_kv), (SLIM, dim // 2), (SLIM, dim // 2), (COLORS, dim))]
    return pl.pallas_call(
        functools.partial(gather_kernel, (n_seq, rows, dim, n_kv)),
        in_specs=[hbm] * 6 + [vm] * 3,
        out_specs=[hbm] * 7 + [vm] * 3,
        out_shape=[sds((tokens, dim), BF16)] * 3 + [sds(w, BF16) for w in wshapes] + [
            sds((1, dim), F32), sds((tokens, 2 * n_kv), BF16), sds((2, shard, dim // 2), F32)],
        scratch_shapes=[pltpu.VMEM((tokens, dim), BF16)] * 5 + [
            pltpu.VMEM((n_seq, rows, 2 * n_kv), BF16),
            pltpu.VMEM((n_seq, rows, 2 * n_kv), BF16),
            *[pltpu.VMEM(w, BF16) for w in wshapes],
            pltpu.VMEM((2, 2, 2, 2, 1, HEAD), F32),
            pltpu.VMEM((8, dim), F32),
            pltpu.VMEM((n_seq, rows), jnp.int32),
            *[pltpu.VMEM((tokens, HEAD), F32)] * 3,
            pltpu.VMEM((rows, 2 * rows), F32),
            *[pltpu.VMEM((dim // n_kv * rows, 2 * rows), BF16)] * 2,
            *[pltpu.VMEM((steps, rows, 2 * HEAD), F32)] * 3,
            pltpu.VMEM((4, 2, dim // 8, EARLY), F32),
            pltpu.VMEM((4, dim // 8, EARLY), F32),
            *[pltpu.VMEM((n_early, 2) + k + (shard // 2, EARLY), F32) for k in ((2, 2, 2), (2, 2), (2,))],
            dma((6 * n_kv // HEAD + 5 + 2 * len(SLIM),)), dma((6,)), dma((2, steps)), *[dma((4, 3, 3))] * 4,
            *[dma((4,))] * 4, *[dma((n_seq + 1,))] * 2, *[dma((steps,))] * 2,
            *[dma((n_early,))] * 2, *[dma((n_early, 2, 2))] * 2, pltpu.SemaphoreType.REGULAR,
        ],
        compiler_params=pltpu.CompilerParams(collective_id=2, has_side_effects=True, vmem_limit_bytes=67043328),
        cost_estimate=pl.CostEstimate(flops=2 * tokens * dim * (2 * dim + 2 * n_kv), bytes_accessed=40 * 2 ** 20,
                                      transcendentals=0),
    )(x, dy, wq, wk, wv, wo, gain[None], pos, freq)


def solution(mesh):
    cp_size = mesh.shape['cp']

    def shard_fn(hidden, tok_pos, grad_out, norm_gain, w_query, w_key, w_value, w_out):
        n_seq, rows, dim = hidden.shape
        tokens = n_seq * rows
        n_q = w_query.shape[1]
        n_kv = w_key.shape[1]
        groups = n_kv // HEAD
        x16 = hidden.reshape(tokens, dim)
        dy = grad_out.reshape(tokens, dim)
        r, o, dq, w_kv, w_a, w_b, w_o, gain, dkv, part = gather_project(
            x16, dy, w_query, w_key, w_value, w_out, norm_gain, tok_pos)
        w_a, w_b, w_kv, w_o = (w.reshape(dim, -1) for w in (w_a, w_b, w_kv, w_o))
        g_wq, g_wk, g_wv, g_wo, gg, result, grad_hidden = wgrad(o, dy, r, dq, dkv, x16, w_o, w_a, w_b, w_kv, gain, part)
        shard = lax.axis_index('fsdp') * cp_size + lax.axis_index('cp')
        g_gain = lax.dynamic_slice(gg[0], (shard * norm_gain.shape[0],), norm_gain.shape)
        return result.reshape(hidden.shape), grad_hidden.reshape(hidden.shape), g_wq, g_wk, g_wv, g_wo, g_gain

    row = P('fsdp', 'cp', None)
    pos_spec = P('fsdp', 'cp')
    w = P(AXES, None)
    g = P(AXES)
    return jax.shard_map(shard_fn, mesh=mesh, in_specs=(row, pos_spec, row, g, w, w, w, w),
                         out_specs=(row, row, w, w, w, w, g), check_vma=False)
```
